64 devices in a mesh: data: 4 (over x, y), expert: 16 (over z, core).
Axes of the slice: x: 2, y: 2, z: 8, core: 2. Of those that a mesh axis runs over, the one named last changes fastest.
The devices are a block of a 4x4x8 slice.
Arguments:
- token_rows: bfloat16 [131072, 512], P(('data', 'expert')), parts along dimension 0
- expert_ids: int32 [131072, 2], P(('data', 'expert')), parts along dimension 0
- gate_weights: float32 [131072, 2], P(('data', 'expert')), parts along dimension 0
- w_in: bfloat16 [512, 512, 1024], P('expert')
- w_out: bfloat16 [512, 1024, 512], P('expert')
Outputs:
- output: bfloat16 [131072, 512], P(('data', 'expert')), parts along dimension 0
There are 4 independent parts. The reference program is written for one: setup_inputs(seed, part) draws one part's arguments, and reference() takes and returns one part's arrays. A program takes and returns all parts, laid end to end along the dimension named above; an argument that names none is the same for every part.
All inputs are finite; a program needn't handle non-finite values.
Results may differ from the reference program's by a relative error of at most 0.001.
Values are sent between devices in bfloat16 or wider.
A program may use at most 768 MiB of HBM per device.

```python
import math
import jax
import jax.numpy as jnp
from jax import lax

TOKENS_DEV = 2048
GROUP_DEVS = 16
MODEL_DIM = 512
HIDDEN_DIM = 1024
EXPERTS = 512
TOP_K = 2

TOKENS = TOKENS_DEV * GROUP_DEVS
MEAN_LOAD = TOKENS_DEV * TOP_K // EXPERTS
CAPACITY = TOKENS * TOP_K // EXPERTS
POP_SPREAD = MEAN_LOAD // 2
DEV_SPREAD = MEAN_LOAD // 4


def draw_routing(key):
    key_order, key_pop, key_dev, key_tok, key_col = jax.random.split(key, 5)
    expert_order = jax.random.permutation(key_order, EXPERTS)
    pop_bias = jax.random.randint(key_pop, (EXPERTS,), 0, POP_SPREAD + 1)
    pop_bias = pop_bias.at[0].set(POP_SPREAD).at[1].set(0)
    dev_bias = jax.random.randint(key_dev, (GROUP_DEVS, EXPERTS), 0, DEV_SPREAD + 1)
    dev_bias = dev_bias.at[:, 0].set(DEV_SPREAD).at[:, 1].set(0)
    pair_load = MEAN_LOAD + (pop_bias - jnp.roll(pop_bias, -1))[None, :] + dev_bias - jnp.roll(dev_bias, -1, axis=1)
    run_ends = jnp.cumsum(pair_load, axis=1)
    positions = jnp.arange(TOKENS_DEV * TOP_K, dtype=jnp.int32)

    def find_run(row_ends):
        return jnp.searchsorted(row_ends, positions, side="right")

    run_index = jax.vmap(find_run)(run_ends)
    labels = expert_order[run_index].reshape(GROUP_DEVS, TOP_K, TOKENS_DEV)
    choices = jnp.swapaxes(labels, 1, 2)

    def token_order(sub_key):
        return jax.random.permutation(sub_key, TOKENS_DEV)

    tok_perm = jax.vmap(token_order)(jax.random.split(key_tok, GROUP_DEVS))
    choices = jnp.take_along_axis(choices, tok_perm[:, :, None], axis=1)
    choices = jax.random.permutation(key_col, choices, axis=2, independent=True)
    return choices.reshape(TOKENS, TOP_K).astype(jnp.int32)


def draw_matrices(key, fan_in, fan_out):
    def one_matrix(sub_key):
        return (jax.random.normal(sub_key, (fan_in, fan_out), jnp.float32) / math.sqrt(fan_in)).astype(jnp.bfloat16)
    return lax.map(one_matrix, jax.random.split(key, EXPERTS))


def setup_inputs(seed: int = 0, part: int = 0) -> dict:
    root = jax.random.key(seed)
    part_key = jax.random.fold_in(root, part)
    key_route, key_rows, key_gate = jax.random.split(part_key, 3)
    key_up, key_down = jax.random.split(jax.random.fold_in(root, 1000003), 2)
    token_rows = jax.random.normal(key_rows, (TOKENS, MODEL_DIM), jnp.float32).astype(jnp.bfloat16)
    gate_weights = jax.random.uniform(key_gate, (TOKENS, TOP_K), jnp.float32, 0.5, 1.5) / math.sqrt(TOP_K)
    return {"token_rows": token_rows, "expert_ids": draw_routing(key_route), "gate_weights": gate_weights, "w_in": draw_matrices(key_up, MODEL_DIM, HIDDEN_DIM), "w_out": draw_matrices(key_down, HIDDEN_DIM, MODEL_DIM)}


def expert_ffn(operands):
    rows, up_weight, down_weight = operands
    hidden = jax.nn.gelu(jnp.dot(rows, up_weight, preferred_element_type=jnp.float32)).astype(jnp.bfloat16)
    return jnp.dot(hidden, down_weight, preferred_element_type=jnp.float32).astype(jnp.bfloat16)


def reference(token_rows, expert_ids, gate_weights, w_in, w_out):
    pairs = TOP_K * TOKENS
    flat_ids = expert_ids.T.reshape(pairs)
    sort_order = jnp.argsort(flat_ids, stable=True)
    position = jnp.zeros((pairs,), jnp.int32).at[sort_order].set(jnp.arange(pairs, dtype=jnp.int32))
    counts = jnp.bincount(flat_ids, length=EXPERTS)
    seg_start = jnp.cumsum(counts) - counts
    slot = position - seg_start[flat_ids]
    keep = slot < CAPACITY
    slot_safe = jnp.where(keep, slot, CAPACITY)
    buffer = jnp.zeros((EXPERTS, CAPACITY, MODEL_DIM), token_rows.dtype).at[flat_ids, slot_safe].set(jnp.tile(token_rows, (TOP_K, 1)), mode="drop")
    outputs = lax.map(expert_ffn, (buffer, w_in, w_out))
    weight = jnp.where(keep, gate_weights.T.reshape(pairs), 0.0).reshape(TOP_K, TOKENS)
    slot_read = jnp.minimum(slot, CAPACITY - 1).reshape(TOP_K, TOKENS)

    def add_choice(total, pieces):
        choice_weight, choice_ids, choice_slot = pieces
        return total + choice_weight[:, None] * outputs[choice_ids, choice_slot].astype(jnp.float32), None

    mixed, _ = lax.scan(add_choice, token_rows.astype(jnp.float32), (weight, flat_ids.reshape(TOP_K, TOKENS), slot_read))
    return mixed.astype(jnp.bfloat16)
```

```python
import functools

import jax
import jax.numpy as jnp
from jax import lax
from jax.experimental import pallas as pl
from jax.experimental.pallas import tpu as pltpu
from jax.sharding import PartitionSpec as P

MESH = pl.DeviceIdType.MESH
VMEM = pltpu.VMEM
F32, BF16, I32 = jnp.float32, jnp.bfloat16, jnp.int32
WIN = 32
ALIGN = 16
TOKEN_BLOCK = 256


def iota(shape, dim):
    return lax.broadcasted_iota(I32, shape, dim)


def peer(me, step, groups):
    chips = groups // 2
    half = step // 2
    away = (half + 1) // 2
    sign = 1 - 2 * ((half + 1) % 2)
    chip = lax.rem(me // 2 + sign * away + chips, chips)
    core = lax.rem(me + step, 2)
    return chip * 2 + core


def source_of(me, step, groups):
    chips = groups // 2
    half = step // 2
    away = (half + 1) // 2
    sign = 1 - 2 * ((half + 1) % 2)
    chip = lax.rem(me // 2 - sign * away + chips, chips)
    core = lax.rem(me + step, 2)
    return chip * 2 + core


def enter(me, groups):
    barrier = pltpu.get_barrier_semaphore()

    @pl.loop(1, groups)
    def _(step):
        pl.semaphore_signal(barrier, inc=1, device_id={"expert": lax.rem(me + step, groups)}, device_id_type=MESH)

    pl.semaphore_wait(barrier, groups - 1)


def route_kernel(groups, capacity, stride, local, ids_ref, pos_ref, slot_ref, start_ref, load_ref, cnt, carry, rank, rows, send_sem, recv_sem):
    me = lax.axis_index("expert")
    tokens = ids_ref.shape[1]
    experts = local * groups
    blocks = tokens // TOKEN_BLOCK
    enter(me, groups)

    expert_rows = iota((experts, TOKEN_BLOCK), 0)
    upper = (iota((TOKEN_BLOCK, TOKEN_BLOCK), 0) <= iota((TOKEN_BLOCK, TOKEN_BLOCK), 1)).astype(BF16)
    ones = jnp.ones((TOKEN_BLOCK, TOKEN_BLOCK), BF16)
    for j in range(2):
        carry[...] = jnp.zeros_like(carry)

        def count_block(b, row):
            cols = pl.ds(pl.multiple_of(b * TOKEN_BLOCK, TOKEN_BLOCK), TOKEN_BLOCK)
            hot = expert_rows == ids_ref[j : j + 1, cols]
            hot16 = jnp.where(hot, 1.0, 0.0).astype(BF16)
            run = jnp.dot(hot16, upper, preferred_element_type=F32) + carry[...]
            rank[j : j + 1, cols] = jnp.sum(jnp.where(hot, run, 0.0), axis=0, keepdims=True) - 1.0
            carry[...] += jnp.dot(hot16, ones, preferred_element_type=F32)
            return row + lax.dot_general(ones[:8], hot16, (((1,), (1,)), ((), ())), preferred_element_type=F32)

        row = lax.fori_loop(0, blocks, count_block, jnp.zeros((8, experts), F32))
        cnt[me, j : j + 1, :] = row[:1]

    def send(step):
        to = lax.rem(me + step, groups)
        return pltpu.make_async_remote_copy(src_ref=cnt.at[me], dst_ref=cnt.at[me], send_sem=send_sem.at[step], recv_sem=recv_sem.at[step], device_id={"expert": to}, device_id_type=MESH)

    def arrive(step):
        origin = lax.rem(me - step + groups, groups)
        return pltpu.make_async_remote_copy(src_ref=cnt.at[origin], dst_ref=cnt.at[origin], send_sem=send_sem.at[step], recv_sem=recv_sem.at[step], device_id={"expert": origin}, device_id_type=MESH)

    @pl.loop(1, groups)
    def _(step):
        send(step).start()

    @pl.loop(1, groups)
    def _(step):
        arrive(step).wait_recv()

    @pl.loop(1, groups)
    def _(step):
        send(step).wait_send()

    first, second = cnt[:, 0, :], cnt[:, 1, :]
    earlier = (iota((groups, groups), 1) < iota((groups, groups), 0)).astype(BF16)
    before0 = jnp.dot(earlier, first.astype(BF16), preferred_element_type=F32)
    before1 = jnp.dot(earlier, second.astype(BF16), preferred_element_type=F32)
    total0 = jnp.sum(first, axis=0, keepdims=True)
    keep0 = jnp.clip(capacity - before0, 0.0, first)
    keep1 = jnp.clip(capacity - total0 - before1, 0.0, second)
    keep = keep0 + keep1
    keep16 = keep.astype(BF16)
    er, ec = iota((experts, experts), 0), iota((experts, experts), 1)
    inside = ((er < ec) & (er // local == ec // local)).astype(BF16)
    offset = jnp.dot(keep16, inside, preferred_element_type=F32)
    load = jnp.dot(keep16, (iota((experts, 128), 0) // local == iota((experts, 128), 1)).astype(BF16), preferred_element_type=F32)
    load_ref[...] = jnp.broadcast_to(jnp.max(jnp.max(load, axis=1, keepdims=True), axis=0, keepdims=True), load_ref.shape).astype(I32)
    high = jnp.floor(offset * (1.0 / ALIGN))
    low = offset - high * ALIGN

    rows[0], rows[1], rows[2], rows[3] = high, low, keep0, keep1
    table = jnp.concatenate([rows[i, pl.ds(me, 1), :] for i in range(4)] + [jnp.zeros((4, experts), F32)], axis=0).astype(BF16)
    for j in range(2):

        def place_block(b, _):
            cols = pl.ds(pl.multiple_of(b * TOKEN_BLOCK, TOKEN_BLOCK), TOKEN_BLOCK)
            ids = ids_ref[j : j + 1, cols]
            hot16 = jnp.where(expert_rows == ids, 1.0, 0.0).astype(BF16)
            found = jnp.dot(table, hot16, preferred_element_type=F32)
            start = found[0:1] * ALIGN + found[1:2]
            if j == 1:
                start = start + found[2:3]
            rk = rank[j : j + 1, cols]
            spot = (start + rk).astype(I32) + (ids // local) * stride
            pos_ref[j : j + 1, cols] = jnp.where(rk < found[2 + j : 3 + j], spot, -1)
            return 0

        lax.fori_loop(0, blocks, place_block, 0)

    mine = (iota((local, experts), 1) == iota((local, experts), 0) + me * local).astype(BF16)

    def pick(values):
        return lax.dot_general(mine, values.astype(BF16), (((1,), (1,)), ((), ())), preferred_element_type=F32)

    ahead = jnp.dot(earlier, keep16, preferred_element_type=F32)
    start_ref[...] = (pick(high) * ALIGN).astype(I32)
    lanes = groups * WIN
    spread = (iota((groups, lanes), 1) // WIN == iota((groups, lanes), 0)).astype(BF16)

    def widen(values):
        return jnp.dot(pick(values).astype(BF16), spread, preferred_element_type=F32)

    lo, kept, base = widen(low), widen(keep), widen(ahead)
    lane = (iota((local, lanes), 1) % WIN).astype(F32)
    valid = (lane >= lo) & (lane < lo + kept)
    slot_ref[...] = jnp.where(valid, base + lane - lo, -1.0).astype(I32)


def dispatch_kernel(groups, cap, stride, pos_ref, x_ref, got_ref, buf, send_sem, recv_sem):
    me = lax.axis_index("expert")
    tokens = x_ref.shape[0]
    enter(me, groups)

    def push(step):
        to = peer(me, step, groups)
        return pltpu.make_async_remote_copy(src_ref=buf.at[to], dst_ref=got_ref.at[pl.ds(me * cap, cap)], send_sem=send_sem.at[step], recv_sem=recv_sem.at[step], device_id={"expert": to}, device_id_type=MESH)

    def land(step):
        origin = source_of(me, step, groups)
        return pltpu.make_async_remote_copy(src_ref=buf.at[origin], dst_ref=got_ref.at[pl.ds(origin * cap, cap)], send_sem=send_sem.at[step], recv_sem=recv_sem.at[step], device_id={"expert": origin}, device_id_type=MESH)

    @pl.loop(0, groups)
    def _(index):
        step = groups - 1 - index
        to = peer(me, step, groups)
        spots = pos_ref[...] - to * stride
        line = iota((cap, tokens), 0)
        hot = (line == spots[0:1]) | (line == spots[1:2])
        buf[to] = jnp.dot(jnp.where(hot, 1.0, 0.0).astype(BF16), x_ref[...], preferred_element_type=F32).astype(BF16)

        @pl.when(step > 0)
        def _():
            push(step).start()

    own = pltpu.make_async_copy(buf.at[me], got_ref.at[pl.ds(me * cap, cap)], recv_sem.at[0])
    own.start()

    @pl.loop(1, groups)
    def _(step):
        land(step).wait_recv()

    @pl.loop(1, groups)
    def _(step):
        push(step).wait_send()

    own.wait()


def expert_kernel(groups, cap, local, start_ref, slot_ref, got_ref, w_in_ref, w_out_ref, out_ref, rows, outs, win, load_sem, store_sem):
    e = pl.program_id(0)
    total = groups * cap
    fetch = pltpu.make_async_copy(got_ref, rows.at[pl.ds(0, total)], load_sem)

    @pl.when(e == 0)
    def _():
        fetch.start()
        rows[pl.ds(total, WIN), :] = jnp.zeros((WIN, rows.shape[1]), BF16)
        outs[...] = jnp.zeros_like(outs)
        fetch.wait()

    def window(s):
        return pl.ds(pl.multiple_of(s * cap + start_ref[e, s], ALIGN), WIN)

    for s in range(groups):
        win[s * WIN : (s + 1) * WIN, :] = rows[window(s), :]
    slots = slot_ref.shape[1] // 4
    hot = jnp.where(iota((slots, groups * WIN), 0) == slot_ref[pl.ds(e, 1), :], 1.0, 0.0).astype(BF16)
    x = jnp.dot(hot, win[...], preferred_element_type=F32).astype(BF16)
    h = jax.nn.gelu(jnp.dot(x, w_in_ref[0], preferred_element_type=F32)).astype(BF16)
    o = jnp.dot(h, w_out_ref[0], preferred_element_type=F32).astype(BF16)
    back = lax.dot_general(hot, o, (((0,), (0,)), ((), ())), preferred_element_type=F32).astype(BF16)
    for s in range(groups):
        outs[window(s), :] += back[s * WIN : (s + 1) * WIN, :]

    @pl.when(e == local - 1)
    def _():
        store = pltpu.make_async_copy(outs.at[pl.ds(0, total)], out_ref, store_sem)
        store.start()
        store.wait()


def combine_kernel(groups, cap, stride, sent_ref, pos_ref, gate_ref, x_ref, out_ref, got, spots, acc, send_sem, recv_sem):
    me = lax.axis_index("expert")
    tokens = x_ref.shape[0]
    enter(me, groups)

    def push(step):
        to = peer(me, step, groups)
        return pltpu.make_async_remote_copy(src_ref=sent_ref.at[pl.ds(to * cap, cap)], dst_ref=got.at[me], send_sem=send_sem.at[step], recv_sem=recv_sem.at[step], device_id={"expert": to}, device_id_type=MESH)

    def land(step):
        origin = source_of(me, step, groups)
        return pltpu.make_async_remote_copy(src_ref=sent_ref.at[pl.ds(origin * cap, cap)], dst_ref=got.at[origin], send_sem=send_sem.at[step], recv_sem=recv_sem.at[step], device_id={"expert": origin}, device_id_type=MESH)

    own = pltpu.make_async_copy(sent_ref.at[pl.ds(me * cap, cap)], got.at[me], recv_sem.at[0])
    own.start()

    @pl.loop(0, groups - 1)
    def _(index):
        push(groups - 1 - index).start()

    for j in range(2):
        spots[j] = jnp.broadcast_to(pos_ref[:, j : j + 1], (tokens, 128))
    acc[...] = jnp.zeros_like(acc)

    def add(origin):
        @pl.loop(0, tokens // TOKEN_BLOCK)
        def _(b):
            at = pl.ds(pl.multiple_of(b * TOKEN_BLOCK, TOKEN_BLOCK), TOKEN_BLOCK)
            lane = iota((TOKEN_BLOCK, 128), 1)
            for j in range(2):
                spot = spots[j, at, :] - origin * stride
                hot = jnp.concatenate([jnp.where(spot - k == lane, 1.0, 0.0).astype(BF16) for k in range(0, cap, 128)], axis=1)
                acc[j, at, :] += jnp.dot(hot[:, :cap], got[origin], preferred_element_type=F32)

    own.wait()
    add(me)

    @pl.loop(1, groups)
    def _(step):
        land(step).wait_recv()
        add(source_of(me, step, groups))

    @pl.loop(0, tokens // TOKEN_BLOCK)
    def _(b):
        at = pl.ds(pl.multiple_of(b * TOKEN_BLOCK, TOKEN_BLOCK), TOKEN_BLOCK)
        mixed = x_ref[at, :].astype(F32) + gate_ref[at, 0:1] * acc[0, at, :]
        out_ref[at, :] = (mixed + gate_ref[at, 1:2] * acc[1, at, :]).astype(BF16)

    @pl.loop(1, groups)
    def _(step):
        push(step).wait_send()


def solution(mesh):
    groups = mesh.shape["expert"]
    row_spec = P(("data", "expert"), None)
    weight_spec = P("expert", None, None)

    def device_step(token_rows, expert_ids, gate_weights, w_in, w_out):
        tokens, top_k = expert_ids.shape
        local, dim, hidden = w_in.shape
        experts = local * groups
        mean_load = tokens * top_k // experts
        capacity = groups * mean_load
        worst = local * (7 * mean_load // 4)
        stride = 2 * local * mean_load
        lanes = groups * WIN
        vmem = pl.BlockSpec(memory_space=VMEM)
        anywhere = pl.BlockSpec(memory_space=pl.ANY)

        def params(collective_id):
            return pltpu.CompilerParams(collective_id=collective_id, has_side_effects=True, vmem_limit_bytes=60 * 1024 * 1024)

        pair_sems = [pltpu.SemaphoreType.DMA((groups,)), pltpu.SemaphoreType.DMA((groups,))]
        pos, slot, start, load = pl.pallas_call(
            functools.partial(route_kernel, groups, capacity, stride, local),
            out_shape=[
                jax.ShapeDtypeStruct((top_k, tokens), I32),
                jax.ShapeDtypeStruct((local, lanes), I32),
                jax.ShapeDtypeStruct((local, groups), I32),
                jax.ShapeDtypeStruct((8, 128), I32),
            ],
            in_specs=[vmem],
            out_specs=[vmem] * 4,
            scratch_shapes=[
                VMEM((groups, top_k, experts), F32),
                VMEM((experts, TOKEN_BLOCK), F32),
                VMEM((top_k, tokens), F32),
                VMEM((4, groups, experts), F32),
            ]
            + pair_sems,
            compiler_params=params(0),
            name="route",
        )(expert_ids.T)
        pos_cols = pos.T

        def exchange(cap):
            def run():
                got = pl.pallas_call(
                    functools.partial(dispatch_kernel, groups, cap, stride),
                    out_shape=jax.ShapeDtypeStruct((groups * cap, dim), BF16),
                    in_specs=[vmem, vmem],
                    out_specs=anywhere,
                    scratch_shapes=[VMEM((groups, cap, dim), BF16)] + pair_sems,
                    compiler_params=params(1),
                    name="dispatch",
                )(pos, token_rows)
                sent = pl.pallas_call(
                    functools.partial(expert_kernel, groups, cap, local),
                    out_shape=jax.ShapeDtypeStruct((groups * cap, dim), BF16),
                    grid_spec=pltpu.PrefetchScalarGridSpec(
                        num_scalar_prefetch=1,
                        grid=(local,),
                        in_specs=[
                            pl.BlockSpec((local, lanes), lambda e, _: (0, 0)),
                            anywhere,
                            pl.BlockSpec((1, dim, hidden), lambda e, _: (e, 0, 0)),
                            pl.BlockSpec((1, hidden, dim), lambda e, _: (e, 0, 0)),
                        ],
                        out_specs=anywhere,
                        scratch_shapes=[
                            VMEM((groups * cap + WIN, dim), BF16),
                            VMEM((groups * cap + WIN, dim), BF16),
                            VMEM((lanes, dim), BF16),
                            pltpu.SemaphoreType.DMA(()),
                            pltpu.SemaphoreType.DMA(()),
                        ],
                    ),
                    compiler_params=pltpu.CompilerParams(vmem_limit_bytes=60 * 1024 * 1024),
                    name="experts",
                )(start, slot, got, w_in, w_out)
                return pl.pallas_call(
                    functools.partial(combine_kernel, groups, cap, stride),
                    out_shape=jax.ShapeDtypeStruct((tokens, dim), BF16),
                    in_specs=[anywhere, vmem, vmem, vmem],
                    out_specs=vmem,
                    scratch_shapes=[
                        VMEM((groups, cap, dim), BF16),
                        VMEM((top_k, tokens, 128), I32),
                        VMEM((top_k, tokens, dim), F32),
                    ]
                    + pair_sems,
                    compiler_params=params(2),
                    name="combine",
                )(sent, pos_cols, gate_weights, token_rows)

            return run

        sizes = [worst - worst // 3 // 16 * 16, worst]
        return lax.cond(load[0, 0] <= sizes[0], exchange(sizes[0]), exchange(sizes[1]))

    return jax.shard_map(device_step, mesh=mesh, in_specs=(row_spec, row_spec, row_spec, weight_spec, weight_spec), out_specs=row_spec, check_vma=False)
```

```python
import functools

import jax
import jax.numpy as jnp
from jax import lax
from jax.experimental import pallas as pl
from jax.experimental.pallas import tpu as pltpu
from jax.sharding import PartitionSpec as P

MESH = pl.DeviceIdType.MESH
VMEM = pltpu.VMEM
F32, BF16, I32 = jnp.float32, jnp.bfloat16, jnp.int32
WIN = 32
ALIGN = 16
TOKEN_BLOCK = 256


def iota(shape, dim):
    return lax.broadcasted_iota(I32, shape, dim)


def peer(me, step, groups):
    chips = groups // 2
    half = step // 2
    away = (half + 1) // 2
    sign = 1 - 2 * ((half + 1) % 2)
    chip = lax.rem(me // 2 + sign * away + chips, chips)
    core = lax.rem(me + step, 2)
    return chip * 2 + core


def source_of(me, step, groups):
    chips = groups // 2
    half = step // 2
    away = (half + 1) // 2
    sign = 1 - 2 * ((half + 1) % 2)
    chip = lax.rem(me // 2 - sign * away + chips, chips)
    core = lax.rem(me + step, 2)
    return chip * 2 + core


def enter(me, groups):
    barrier = pltpu.get_barrier_semaphore()

    @pl.loop(1, groups)
    def _(step):
        pl.semaphore_signal(barrier, inc=1, device_id={"expert": lax.rem(me + step, groups)}, device_id_type=MESH)

    pl.semaphore_wait(barrier, groups - 1)


def route_kernel(groups, capacity, stride, local, near, ids_ref, pos_ref, slot_ref, start_ref, place_ref, load_ref, cnt, carry, rank, rows, send_sem, recv_sem):
    me = lax.axis_index("expert")
    tokens = ids_ref.shape[1]
    experts = local * groups
    blocks = tokens // TOKEN_BLOCK
    enter(me, groups)

    expert_rows = iota((experts, TOKEN_BLOCK), 0)
    upper = (iota((TOKEN_BLOCK, TOKEN_BLOCK), 0) <= iota((TOKEN_BLOCK, TOKEN_BLOCK), 1)).astype(BF16)
    ones = jnp.ones((TOKEN_BLOCK, TOKEN_BLOCK), BF16)
    for j in range(2):
        carry[...] = jnp.zeros_like(carry)

        def count_block(b, row):
            cols = pl.ds(pl.multiple_of(b * TOKEN_BLOCK, TOKEN_BLOCK), TOKEN_BLOCK)
            hot = expert_rows == ids_ref[j : j + 1, cols]
            hot16 = jnp.where(hot, 1.0, 0.0).astype(BF16)
            run = jnp.dot(hot16, upper, preferred_element_type=F32) + carry[...]
            rank[j : j + 1, cols] = jnp.sum(jnp.where(hot, run, 0.0), axis=0, keepdims=True) - 1.0
            carry[...] += jnp.dot(hot16, ones, preferred_element_type=F32)
            return row + lax.dot_general(ones[:8], hot16, (((1,), (1,)), ((), ())), preferred_element_type=F32)

        row = lax.fori_loop(0, blocks, count_block, jnp.zeros((8, experts), F32))
        cnt[me, j : j + 1, :] = row[:1]

    def send(step):
        to = lax.rem(me + step, groups)
        return pltpu.make_async_remote_copy(src_ref=cnt.at[me], dst_ref=cnt.at[me], send_sem=send_sem.at[step], recv_sem=recv_sem.at[step], device_id={"expert": to}, device_id_type=MESH)

    def arrive(step):
        origin = lax.rem(me - step + groups, groups)
        return pltpu.make_async_remote_copy(src_ref=cnt.at[origin], dst_ref=cnt.at[origin], send_sem=send_sem.at[step], recv_sem=recv_sem.at[step], device_id={"expert": origin}, device_id_type=MESH)

    @pl.loop(1, groups)
    def _(step):
        send(step).start()

    @pl.loop(1, groups)
    def _(step):
        arrive(step).wait_recv()

    @pl.loop(1, groups)
    def _(step):
        send(step).wait_send()

    first, second = cnt[:, 0, :], cnt[:, 1, :]
    earlier = (iota((groups, groups), 1) < iota((groups, groups), 0)).astype(BF16)
    before0 = jnp.dot(earlier, first.astype(BF16), preferred_element_type=F32)
    before1 = jnp.dot(earlier, second.astype(BF16), preferred_element_type=F32)
    total0 = jnp.sum(first, axis=0, keepdims=True)
    keep0 = jnp.clip(capacity - before0, 0.0, first)
    keep1 = jnp.clip(capacity - total0 - before1, 0.0, second)
    keep = keep0 + keep1
    keep16 = keep.astype(BF16)
    er, ec = iota((experts, experts), 0), iota((experts, experts), 1)
    inside = ((er < ec) & (er // local == ec // local)).astype(BF16)
    offset = jnp.dot(keep16, inside, preferred_element_type=F32)
    load = jnp.dot(keep16, (iota((experts, 128), 0) // local == iota((experts, 128), 1)).astype(BF16), preferred_element_type=F32)
    load_ref[...] = jnp.broadcast_to(jnp.max(jnp.max(load, axis=1, keepdims=True), axis=0, keepdims=True), load_ref.shape).astype(I32)
    high = jnp.floor(offset * (1.0 / ALIGN))
    low = offset - high * ALIGN

    rows[0], rows[1], rows[2], rows[3] = high, low, keep0, keep1
    table = jnp.concatenate([rows[i, pl.ds(me, 1), :] for i in range(4)] + [jnp.zeros((4, experts), F32)], axis=0).astype(BF16)
    for j in range(2):

        def place_block(b, _):
            cols = pl.ds(pl.multiple_of(b * TOKEN_BLOCK, TOKEN_BLOCK), TOKEN_BLOCK)
            ids = ids_ref[j : j + 1, cols]
            hot16 = jnp.where(expert_rows == ids, 1.0, 0.0).astype(BF16)
            found = jnp.dot(table, hot16, preferred_element_type=F32)
            start = found[0:1] * ALIGN + found[1:2]
            if j == 1:
                start = start + found[2:3]
            rk = rank[j : j + 1, cols]
            spot = (start + rk).astype(I32) + (ids // local) * stride
            pos_ref[j : j + 1, cols] = jnp.where(rk < found[2 + j : 3 + j], spot, -1)
            return 0

        lax.fori_loop(0, blocks, place_block, 0)

    mine = (iota((local, experts), 1) == iota((local, experts), 0) + me * local).astype(BF16)

    def pick(values):
        return lax.dot_general(mine, values.astype(BF16), (((1,), (1,)), ((), ())), preferred_element_type=F32)

    from_step = (source_of(me, iota((groups, groups), 0), groups) == iota((groups, groups), 1)).astype(BF16)
    older, newer = iota((groups, groups), 1), iota((groups, groups), 0)
    ahead_of = ((older < newer) & ((older < near) == (newer < near))).astype(BF16)

    def by_step(values):
        return jnp.dot(from_step, values.astype(BF16), preferred_element_type=F32)

    kept = by_step(keep)
    ahead = pick(jnp.dot(ahead_of, kept.astype(BF16), preferred_element_type=F32))
    high, low, kept = pick(by_step(high)), pick(by_step(low)), pick(kept)
    start_ref[...] = high.astype(I32)
    lanes = groups * WIN
    spread = (iota((groups, lanes), 1) // WIN == iota((groups, lanes), 0)).astype(BF16)

    def widen(values):
        return jnp.dot(values.astype(BF16), spread, preferred_element_type=F32)

    wide_low, wide_kept, wide_ahead = widen(low), widen(kept), widen(ahead)
    lane = (iota((local, lanes), 1) % WIN).astype(F32)
    valid = (lane >= wide_low) & (lane < wide_low + wide_kept)
    slot_ref[...] = jnp.where(valid, wide_ahead + lane - wide_low, -1.0).astype(I32)
    seat = iota((local, capacity), 1).astype(F32)
    goals = [jnp.full((local, capacity), -1.0, F32) for _ in range(2)]
    for step in range(groups):
        begin, count = ahead[:, step : step + 1], kept[:, step : step + 1]
        spot = high[:, step : step + 1] * ALIGN + low[:, step : step + 1] + step * stride
        part = int(step >= near)
        goals[part] = jnp.where((seat >= begin) & (seat < begin + count), seat - begin + spot, goals[part])
    for part in range(2):
        place_ref[part] = goals[part].astype(I32)


def moe_kernel(groups, cap, stride, local, near, start_ref, slot_ref, place_ref, pos_ref, cols_ref, gate_ref, x_ref, w_in_hbm, w_out_hbm, out_ref, buf, got_a, got_b, outs, ret, w_in, w_out, win, obuf, spots, acc, w_sem, send_sem, recv_sem, back_send, back_recv):
    me = lax.axis_index("expert")
    tokens, dim = x_ref.shape
    depth = w_in.shape[0]
    enter(me, groups)

    def fetch(visit):
        e, place = lax.rem(visit, local), lax.rem(visit, depth)
        return (
            pltpu.make_async_copy(w_in_hbm.at[e], w_in.at[place], w_sem.at[0, place]),
            pltpu.make_async_copy(w_out_hbm.at[e], w_out.at[place], w_sem.at[1, place]),
        )

    for visit in range(depth):
        for copy in fetch(visit):
            copy.start()

    def push(step, got, first):
        return pltpu.make_async_remote_copy(src_ref=buf.at[step], dst_ref=got.at[pl.ds((step - first) * (cap // ALIGN), cap // ALIGN)], send_sem=send_sem.at[step], recv_sem=recv_sem.at[step], device_id={"expert": peer(me, step, groups)}, device_id_type=MESH)

    def give(step):
        return pltpu.make_async_remote_copy(src_ref=outs.at[step], dst_ref=ret.at[step], send_sem=back_send.at[step], recv_sem=back_recv.at[step], device_id={"expert": source_of(me, step, groups)}, device_id_type=MESH)

    def pack(step):
        spot = pos_ref[...] - peer(me, step, groups) * stride
        line = iota((cap, tokens), 0)
        hot = (line == spot[0:1]) | (line == spot[1:2])
        rows = jnp.dot(jnp.where(hot, 1.0, 0.0).astype(BF16), x_ref[...], preferred_element_type=F32).astype(BF16)
        return rows.reshape(cap // ALIGN, ALIGN, dim)

    @pl.loop(1, near)
    def _(step):
        buf[step] = pack(step)
        push(step, got_a, 0).start()

    @pl.loop(near, groups)
    def _(step):
        buf[step] = pack(step)
        push(step, got_b, near).start()

    tail = WIN // ALIGN
    got_a[pl.ds(0, cap // ALIGN)] = pack(0)
    got_a[pl.ds(near * cap // ALIGN, tail)] = jnp.zeros((tail, ALIGN, dim), BF16)
    got_b[pl.ds((groups - near) * cap // ALIGN, tail)] = jnp.zeros((tail, ALIGN, dim), BF16)
    for j in range(2):
        spots[j] = jnp.broadcast_to(cols_ref[:, j : j + 1], (tokens, 128))

    @pl.loop(0, groups)
    def _(step):
        outs[step] = jnp.zeros((cap, dim), BF16)

    @pl.loop(0, tokens // TOKEN_BLOCK)
    def _(b):
        for j in range(2):
            acc[j, pl.ds(pl.multiple_of(b * TOKEN_BLOCK, TOKEN_BLOCK), TOKEN_BLOCK), :] = jnp.zeros((TOKEN_BLOCK, dim), F32)

    def experts(got, first, last, done):
        lanes = (last - first) * WIN

        @pl.loop(0, local // 2)
        def _(pair):
            for k in range(2):
                e = pair * 2 + k
                for step in range(first, last):
                    row = (step - first) * (cap // ALIGN) + start_ref[e, step]
                    for half in range(WIN // ALIGN):
                        at = (step - first) * WIN + half * ALIGN
                        win[k, at : at + ALIGN, :] = got[row + half]
            for k in range(2):
                e = pair * 2 + k
                visit = done + e
                place = lax.rem(visit, depth)
                for copy in fetch(visit):
                    copy.wait()
                slot = slot_ref[pl.ds(e, 1), :][:, first * WIN : last * WIN]
                hot = jnp.where(iota((128, lanes), 0) == slot, 1.0, 0.0).astype(BF16)
                x = jnp.dot(hot, win[k, :lanes, :], preferred_element_type=F32).astype(BF16)
                h = jax.nn.gelu(jnp.dot(x, w_in[place], preferred_element_type=F32)).astype(BF16)
                obuf[k * 128 : (k + 1) * 128, :] = jnp.dot(h, w_out[place], preferred_element_type=F32).astype(BF16)
            for k in range(2):
                visit = done + pair * 2 + k + depth

                @pl.when(visit < 2 * local)
                def _():
                    for copy in fetch(visit):
                        copy.start()

            part = 0 if first == 0 else 1
            goal = jnp.concatenate([place_ref[part, pl.ds(pair * 2 + k, 1), :] for k in range(2)], axis=1)

            @pl.loop(first, last)
            def _(step):
                hot = jnp.where(iota((cap, 256), 0) == goal - step * stride, 1.0, 0.0).astype(BF16)
                outs[step] += jnp.dot(hot, obuf[...], preferred_element_type=F32).astype(BF16)

    def add(returned, step):
        base = peer(me, step, groups) * stride

        @pl.loop(0, tokens // TOKEN_BLOCK)
        def _(b):
            at = pl.ds(pl.multiple_of(b * TOKEN_BLOCK, TOKEN_BLOCK), TOKEN_BLOCK)
            lane = iota((TOKEN_BLOCK, 128), 1)
            for j in range(2):
                spot = spots[j, at, :] - base
                hot = jnp.concatenate([jnp.where(spot - k == lane, 1.0, 0.0).astype(BF16) for k in range(0, cap, 128)], axis=1)
                acc[j, at, :] += jnp.dot(hot[:, :cap], returned[step], preferred_element_type=F32)

    @pl.loop(1, near)
    def _(step):
        push(step, got_a, 0).wait_recv()

    experts(got_a, 0, near, 0)

    @pl.loop(1, near)
    def _(step):
        give(step).start()

    add(outs, 0)

    @pl.loop(near, groups)
    def _(step):
        push(step, got_b, near).wait_recv()

    experts(got_b, near, groups, local)

    @pl.loop(near, groups)
    def _(step):
        give(step).start()

    @pl.loop(1, groups)
    def _(step):
        give(step).wait_recv()
        add(ret, step)

    @pl.loop(0, tokens // TOKEN_BLOCK)
    def _(b):
        at = pl.ds(pl.multiple_of(b * TOKEN_BLOCK, TOKEN_BLOCK), TOKEN_BLOCK)
        mixed = x_ref[at, :].astype(F32) + gate_ref[at, 0:1] * acc[0, at, :]
        out_ref[at, :] = (mixed + gate_ref[at, 1:2] * acc[1, at, :]).astype(BF16)

    @pl.loop(1, near)
    def _(step):
        push(step, got_a, 0).wait_send()

    @pl.loop(near, groups)
    def _(step):
        push(step, got_b, near).wait_send()

    @pl.loop(1, groups)
    def _(step):
        give(step).wait_send()


def solution(mesh):
    groups = mesh.shape["expert"]
    row_spec = P(("data", "expert"), None)
    weight_spec = P("expert", None, None)

    def device_step(token_rows, expert_ids, gate_weights, w_in, w_out):
        tokens, top_k = expert_ids.shape
        local, dim, hidden = w_in.shape
        experts = local * groups
        mean_load = tokens * top_k // experts
        capacity = groups * mean_load
        worst = local * (7 * mean_load // 4)
        stride = 2 * local * mean_load
        lanes = groups * WIN
        vmem = pl.BlockSpec(memory_space=VMEM)
        anywhere = pl.BlockSpec(memory_space=pl.ANY)

        def params(collective_id):
            return pltpu.CompilerParams(collective_id=collective_id, has_side_effects=True, vmem_limit_bytes=60 * 1024 * 1024)

        near = groups - 6
        pair_sems = [pltpu.SemaphoreType.DMA((groups,)), pltpu.SemaphoreType.DMA((groups,))]
        pos, slot, start, place, load = pl.pallas_call(
            functools.partial(route_kernel, groups, capacity, stride, local, near),
            out_shape=[
                jax.ShapeDtypeStruct((top_k, tokens), I32),
                jax.ShapeDtypeStruct((local, lanes), I32),
                jax.ShapeDtypeStruct((local, groups), I32),
                jax.ShapeDtypeStruct((2, local, capacity), I32),
                jax.ShapeDtypeStruct((8, 128), I32),
            ],
            in_specs=[vmem],
            out_specs=[vmem] * 5,
            scratch_shapes=[
                VMEM((groups, top_k, experts), F32),
                VMEM((experts, TOKEN_BLOCK), F32),
                VMEM((top_k, tokens), F32),
                VMEM((4, groups, experts), F32),
            ]
            + pair_sems,
            compiler_params=params(0),
            name="route",
        )(expert_ids.T)
        pos_cols = pos.T
        depth = 4

        def exchange(cap, collective_id):
            def run():
                return pl.pallas_call(
                    functools.partial(moe_kernel, groups, cap, stride, local, near),
                    out_shape=jax.ShapeDtypeStruct((tokens, dim), BF16),
                    in_specs=[pl.BlockSpec(memory_space=pltpu.SMEM)] + [vmem] * 6 + [anywhere] * 2,
                    out_specs=vmem,
                    scratch_shapes=[
                        VMEM((groups, cap // ALIGN, ALIGN, dim), BF16),
                        VMEM(((near * cap + WIN) // ALIGN, ALIGN, dim), BF16),
                        VMEM((((groups - near) * cap + WIN) // ALIGN, ALIGN, dim), BF16),
                        VMEM((groups, cap, dim), BF16),
                        VMEM((groups, cap, dim), BF16),
                        VMEM((depth, dim, hidden), BF16),
                        VMEM((depth, hidden, dim), BF16),
                        VMEM((2, near * WIN, dim), BF16),
                        VMEM((2 * capacity, dim), BF16),
                        VMEM((top_k, tokens, 128), I32),
                        VMEM((top_k, tokens, dim), F32),
                        pltpu.SemaphoreType.DMA((2, depth)),
                    ]
                    + pair_sems
                    + pair_sems,
                    compiler_params=params(collective_id),
                    name="experts",
                )(start, slot, place, pos, pos_cols, gate_weights, token_rows, w_in, w_out)

            return run

        sizes = [worst - worst // 3 // 16 * 16, worst]
        return lax.cond(load[0, 0] <= sizes[0], exchange(sizes[0], 1), exchange(sizes[1], 2))

    return jax.shard_map(device_step, mesh=mesh, in_specs=(row_spec, row_spec, row_spec, weight_spec, weight_spec), out_specs=row_spec, check_vma=False)
```

```python
import functools

import jax
import jax.numpy as jnp
from jax import lax
from jax.experimental import pallas as pl
from jax.experimental.pallas import tpu as pltpu
from jax.sharding import PartitionSpec as P

MESH = pl.DeviceIdType.MESH
VMEM = pltpu.VMEM
F32, BF16, I32 = jnp.float32, jnp.bfloat16, jnp.int32
WIN = 32
ALIGN = 16
TAIL = 48
TOKEN_BLOCK = 256


def iota(shape, dim):
    return lax.broadcasted_iota(I32, shape, dim)


def peer(me, step, groups):
    chips = groups // 2
    half = step // 2
    away = (half + 1) // 2
    sign = 1 - 2 * ((half + 1) % 2)
    chip = lax.rem(me // 2 + sign * away + chips, chips)
    core = lax.rem(me + step, 2)
    return chip * 2 + core


def source_of(me, step, groups):
    chips = groups // 2
    half = step // 2
    away = (half + 1) // 2
    sign = 1 - 2 * ((half + 1) % 2)
    chip = lax.rem(me // 2 - sign * away + chips, chips)
    core = lax.rem(me + step, 2)
    return chip * 2 + core


def announce(me, groups):
    barrier = pltpu.get_barrier_semaphore()

    @pl.loop(1, groups)
    def _(step):
        pl.semaphore_signal(barrier, inc=1, device_id={"expert": lax.rem(me + step, groups)}, device_id_type=MESH)

    return barrier


def route_kernel(groups, capacity, cap, worst, stride, local, near, ids_ref, pos_ref, slot_ref, start_ref, place_ref, fits_ref, cnt, carry, rank, rows, send_sem, recv_sem):
    me = lax.axis_index("expert")
    tokens = ids_ref.shape[1]
    experts = local * groups
    blocks = tokens // TOKEN_BLOCK
    barrier = announce(me, groups)

    expert_rows = iota((experts, TOKEN_BLOCK), 0)
    upper = (iota((TOKEN_BLOCK, TOKEN_BLOCK), 0) <= iota((TOKEN_BLOCK, TOKEN_BLOCK), 1)).astype(BF16)
    ones = jnp.ones((TOKEN_BLOCK, TOKEN_BLOCK), BF16)
    for j in range(2):
        carry[...] = jnp.zeros_like(carry)

        def count_block(b, row):
            cols = pl.ds(pl.multiple_of(b * TOKEN_BLOCK, TOKEN_BLOCK), TOKEN_BLOCK)
            hot = expert_rows == ids_ref[j : j + 1, cols]
            hot16 = jnp.where(hot, 1.0, 0.0).astype(BF16)
            run = jnp.dot(hot16, upper, preferred_element_type=F32) + carry[...]
            rank[j : j + 1, cols] = jnp.sum(jnp.where(hot, run, 0.0), axis=0, keepdims=True) - 1.0
            carry[...] += jnp.dot(hot16, ones, preferred_element_type=F32)
            return row + lax.dot_general(ones[:8], hot16, (((1,), (1,)), ((), ())), preferred_element_type=F32)

        row = lax.fori_loop(0, blocks, count_block, jnp.zeros((8, experts), F32))
        cnt[me, j : j + 1, :] = row[:1]

    def send(step):
        to = lax.rem(me + step, groups)
        return pltpu.make_async_remote_copy(src_ref=cnt.at[me], dst_ref=cnt.at[me], send_sem=send_sem.at[step], recv_sem=recv_sem.at[step], device_id={"expert": to}, device_id_type=MESH)

    def arrive(step):
        origin = lax.rem(me - step + groups, groups)
        return pltpu.make_async_remote_copy(src_ref=cnt.at[origin], dst_ref=cnt.at[origin], send_sem=send_sem.at[step], recv_sem=recv_sem.at[step], device_id={"expert": origin}, device_id_type=MESH)

    pl.semaphore_wait(barrier, groups - 1)

    @pl.loop(1, groups)
    def _(step):
        send(step).start()

    @pl.loop(1, groups)
    def _(step):
        arrive(step).wait_recv()

    @pl.loop(1, groups)
    def _(step):
        send(step).wait_send()

    first, second = cnt[:, 0, :], cnt[:, 1, :]
    earlier = (iota((groups, groups), 1) < iota((groups, groups), 0)).astype(BF16)
    before0 = jnp.dot(earlier, first.astype(BF16), preferred_element_type=F32)
    before1 = jnp.dot(earlier, second.astype(BF16), preferred_element_type=F32)
    total0 = jnp.sum(first, axis=0, keepdims=True)
    keep0 = jnp.clip(capacity - before0, 0.0, first)
    keep1 = jnp.clip(capacity - total0 - before1, 0.0, second)
    keep = keep0 + keep1
    keep16 = keep.astype(BF16)
    er, ec = iota((experts, experts), 0), iota((experts, experts), 1)
    mate = er // local - ec // local + 2 * (ec // local % 2)
    same = er // local == ec // local
    load = jnp.dot(keep16, same.astype(BF16), preferred_element_type=F32)
    mate_load = jnp.dot(keep16, (mate == 1).astype(BF16), preferred_element_type=F32)
    inside = jnp.dot(keep16, (same & (er < ec)).astype(BF16), preferred_element_type=F32)
    over = jnp.maximum(load - cap, 0.0)
    bad = (over > TAIL) | ((over > 0.0) & (mate_load + over > cap))
    worse = jnp.max(jnp.max(jnp.where(bad, 1.0, 0.0), axis=1, keepdims=True), axis=0, keepdims=True)
    fits_ref[...] = jnp.broadcast_to(1.0 - worse, fits_ref.shape).astype(I32)
    over = jnp.where(worse > 0.0, 0.0, over)
    size = jnp.where(worse > 0.0, float(worst), float(cap))
    offset = TAIL - over + inside
    high = jnp.floor(offset * (1.0 / ALIGN))
    low = offset - high * ALIGN

    rows[0], rows[1], rows[2], rows[3] = high, low, keep0, keep1
    table = jnp.concatenate([rows[i, pl.ds(me, 1), :] for i in range(4)] + [jnp.zeros((4, experts), F32)], axis=0).astype(BF16)
    side = lax.rem(me, 2)
    for j in range(2):

        def place_block(b, _):
            cols = pl.ds(pl.multiple_of(b * TOKEN_BLOCK, TOKEN_BLOCK), TOKEN_BLOCK)
            ids = ids_ref[j : j + 1, cols]
            hot16 = jnp.where(expert_rows == ids, 1.0, 0.0).astype(BF16)
            found = jnp.dot(table, hot16, preferred_element_type=F32)
            rk = rank[j : j + 1, cols]
            spot = found[0:1] * ALIGN + found[1:2] + rk
            if j == 1:
                spot = spot + found[2:3]
            owner = ids // local
            half = ((owner + side) % 2).astype(F32)
            direct = spot >= TAIL
            row = jnp.where(direct, half * size + spot - TAIL, (2.0 - half) * size + spot - TAIL)
            key = row.astype(I32) + (owner // 2) * (2 * stride)
            pos_ref[j : j + 1, cols] = jnp.where(rk < found[2 + j : 3 + j], key, -1)
            return 0

        lax.fori_loop(0, blocks, place_block, 0)

    mine = (iota((local, experts), 1) == iota((local, experts), 0) + me * local).astype(BF16)

    def pick(values):
        return lax.dot_general(mine, values.astype(BF16), (((1,), (1,)), ((), ())), preferred_element_type=F32)

    from_step = (source_of(me, iota((groups, groups), 0), groups) == iota((groups, groups), 1)).astype(BF16)
    older, newer = iota((groups, groups), 1), iota((groups, groups), 0)
    ahead_of = ((older < newer) & ((older < near) == (newer < near))).astype(BF16)

    def by_step(values):
        return jnp.dot(from_step, values.astype(BF16), preferred_element_type=F32)

    kept = by_step(keep)
    ahead = pick(jnp.dot(ahead_of, kept.astype(BF16), preferred_element_type=F32))
    high, low, kept = pick(by_step(high)), pick(by_step(low)), pick(kept)
    start_ref[...] = high.astype(I32)
    lanes = groups * WIN
    spread = (iota((groups, lanes), 1) // WIN == iota((groups, lanes), 0)).astype(BF16)

    def widen(values):
        return jnp.dot(values.astype(BF16), spread, preferred_element_type=F32)

    wide_low, wide_kept, wide_ahead = widen(low), widen(kept), widen(ahead)
    lane = (iota((local, lanes), 1) % WIN).astype(F32)
    valid = (lane >= wide_low) & (lane < wide_low + wide_kept)
    slot_ref[...] = jnp.where(valid, wide_ahead + lane - wide_low, -1.0).astype(I32)
    seat = iota((local, capacity), 1).astype(F32)
    goals = [jnp.full((local, capacity), -1.0, F32) for _ in range(2)]
    for step in range(groups):
        begin, count = ahead[:, step : step + 1], kept[:, step : step + 1]
        spot = high[:, step : step + 1] * ALIGN + low[:, step : step + 1] + step * stride
        part = int(step >= near)
        goals[part] = jnp.where((seat >= begin) & (seat < begin + count), seat - begin + spot, goals[part])
    for part in range(2):
        place_ref[part] = goals[part].astype(I32)


def moe_kernel(groups, cap, stride, local, near, start_ref, slot_ref, place_ref, pos_ref, gate_ref, x_ref, w_in_hbm, w_out_hbm, out_ref, buf, got_a, got_b, outs, tails, ret, w_in, w_out, win, obuf, spots, gates, acc, w_sem, send_sem, recv_sem, back_send, back_recv, tail_send, tail_recv, pass_send, pass_recv, own_sem):
    me = lax.axis_index("expert")
    tokens, dim = x_ref.shape
    depth = w_in.shape[0]
    full = cap + TAIL
    full_blocks, cap_blocks, tail_blocks = full // ALIGN, cap // ALIGN, TAIL // ALIGN
    token_blocks = tokens // TOKEN_BLOCK
    sibling = {"expert": me + 1 - 2 * lax.rem(me, 2)}
    barrier = announce(me, groups)

    def fetch(visit):
        e, place = lax.rem(visit, local), lax.rem(visit, depth)
        return (
            pltpu.make_async_copy(w_in_hbm.at[e], w_in.at[place], w_sem.at[0, place]),
            pltpu.make_async_copy(w_out_hbm.at[e], w_out.at[place], w_sem.at[1, place]),
        )

    for visit in range(depth):
        for copy in fetch(visit):
            copy.start()

    def mate_of(step):
        return step + 1 - 2 * lax.rem(step, 2)

    def push(step, got, first):
        return pltpu.make_async_remote_copy(src_ref=buf.at[step], dst_ref=got.at[pl.ds((step - first) * full_blocks + tail_blocks, cap_blocks)], send_sem=send_sem.at[step], recv_sem=recv_sem.at[step], device_id={"expert": peer(me, step, groups)}, device_id_type=MESH)

    def tail_over(step, got, first):
        return pltpu.make_async_remote_copy(src_ref=got.at[pl.ds((step - first) * full_blocks + cap_blocks, tail_blocks)], dst_ref=got.at[pl.ds((mate_of(step) - first) * full_blocks, tail_blocks)], send_sem=tail_send.at[step], recv_sem=tail_recv.at[mate_of(step)], device_id=sibling, device_id_type=MESH)

    def tail_in(step, got, first):
        return pltpu.make_async_remote_copy(src_ref=got.at[pl.ds((mate_of(step) - first) * full_blocks + cap_blocks, tail_blocks)], dst_ref=got.at[pl.ds((step - first) * full_blocks, tail_blocks)], send_sem=tail_send.at[mate_of(step)], recv_sem=tail_recv.at[step], device_id=sibling, device_id_type=MESH)

    def pass_over(step):
        return pltpu.make_async_remote_copy(src_ref=outs.at[step, pl.ds(0, TAIL)], dst_ref=tails.at[mate_of(step)], send_sem=pass_send.at[step], recv_sem=pass_recv.at[mate_of(step)], device_id=sibling, device_id_type=MESH)

    def pass_in(step):
        return pltpu.make_async_remote_copy(src_ref=outs.at[mate_of(step), pl.ds(0, TAIL)], dst_ref=tails.at[step], send_sem=pass_send.at[mate_of(step)], recv_sem=pass_recv.at[step], device_id=sibling, device_id_type=MESH)

    def give(step):
        return pltpu.make_async_remote_copy(src_ref=outs.at[step, pl.ds(TAIL, cap)], dst_ref=ret.at[step], send_sem=back_send.at[step], recv_sem=back_recv.at[step], device_id={"expert": source_of(me, step, groups)}, device_id_type=MESH)

    def pack(step):
        base = peer(me, step, groups) // 2 * (2 * stride) + lax.rem(step, 2) * cap
        spot = pos_ref[...] - base
        line = iota((cap, tokens), 0)
        hot = (line == spot[0:1]) | (line == spot[1:2])
        rows = jnp.dot(jnp.where(hot, 1.0, 0.0).astype(BF16), x_ref[...], preferred_element_type=F32).astype(BF16)
        buf[step] = rows.reshape(cap_blocks, ALIGN, dim)

    pl.semaphore_wait(barrier, groups - 1)

    @pl.loop(1, groups + 1)
    def _(index):
        step = lax.rem(index, groups)
        pack(step)

        @pl.when((step > 0) & (step < near))
        def _():
            push(step, got_a, 0).start()

        @pl.when(step >= near)
        def _():
            push(step, got_b, near).start()

    mine = pltpu.make_async_copy(buf.at[0], got_a.at[pl.ds(tail_blocks, cap_blocks)], own_sem.at[0])
    mine.start()
    pad = WIN // ALIGN
    got_a[pl.ds(near * full_blocks, pad)] = jnp.zeros((pad, ALIGN, dim), BF16)
    got_b[pl.ds((groups - near) * full_blocks, pad)] = jnp.zeros((pad, ALIGN, dim), BF16)

    @pl.loop(0, groups)
    def _(step):
        outs[step] = jnp.zeros((full, dim), BF16)

    @pl.loop(0, tokens // 128)
    def _(b):
        at = pl.ds(pl.multiple_of(b * 128, 128), 128)
        for j in range(2):
            spots[j, at, :] = jnp.broadcast_to(pos_ref[j : j + 1, at], (128, 128)).T
            gates[j, at, :] = jnp.broadcast_to(gate_ref[j : j + 1, at], (128, 128)).T
            acc[j, at, :] = jnp.zeros((128, dim), BF16)

    def experts(got, first, last, done):
        lanes = (last - first) * WIN

        @pl.loop(0, local // 2)
        def _(pair):
            for k in range(2):
                e = pair * 2 + k
                for step in range(first, last):
                    row = (step - first) * full_blocks + start_ref[e, step]
                    for half in range(WIN // ALIGN):
                        at = (step - first) * WIN + half * ALIGN
                        win[k, at : at + ALIGN, :] = got[row + half]
            for k in range(2):
                e = pair * 2 + k
                visit = done + e
                place = lax.rem(visit, depth)
                for copy in fetch(visit):
                    copy.wait()
                slot = slot_ref[pl.ds(e, 1), :][:, first * WIN : last * WIN]
                hot = jnp.where(iota((128, lanes), 0) == slot, 1.0, 0.0).astype(BF16)
                x = jnp.dot(hot, win[k, :lanes, :], preferred_element_type=F32).astype(BF16)
                h = jax.nn.gelu(jnp.dot(x, w_in[place], preferred_element_type=F32)).astype(BF16)
                obuf[k * 128 : (k + 1) * 128, :] = jnp.dot(h, w_out[place], preferred_element_type=F32).astype(BF16)
            for k in range(2):
                visit = done + pair * 2 + k + depth

                @pl.when(visit < 2 * local)
                def _():
                    for copy in fetch(visit):
                        copy.start()

            part = 0 if first == 0 else 1
            goal = jnp.concatenate([place_ref[part, pl.ds(pair * 2 + k, 1), :] for k in range(2)], axis=1)

            @pl.loop(first, last)
            def _(step):
                hot = jnp.where(iota((full, 256), 0) == goal - step * stride, 1.0, 0.0).astype(BF16)
                outs[step] += jnp.dot(hot, obuf[...], preferred_element_type=F32).astype(BF16)

    def send_back(first, last):
        @pl.loop(first, last)
        def _(step):
            pass_over(step).start()

        @pl.loop(first, last)
        def _(step):
            pass_in(step).wait_recv()
            outs[step, cap:, :] += tails[step]

            @pl.when(step > 0)
            def _():
                give(step).start()

    def add(half):
        base = peer(me, half * 2, groups) // 2 * (2 * stride)
        returned = ret[pl.ds(half * 2, 2)].reshape(2 * cap, dim)

        @pl.loop(0, token_blocks)
        def _(b):
            at = pl.ds(pl.multiple_of(b * TOKEN_BLOCK, TOKEN_BLOCK), TOKEN_BLOCK)
            lane = iota((TOKEN_BLOCK, 128), 1)
            for j in range(2):
                spot = spots[j, at, :] - base
                hot = jnp.concatenate([jnp.where(spot - k == lane, 1.0, 0.0).astype(BF16) for k in range(0, 2 * cap, 128)], axis=1)
                acc[j, at, :] += jnp.dot(hot[:, : 2 * cap], returned, preferred_element_type=F32).astype(BF16)

    mine.wait()
    tail_over(0, got_a, 0).start()

    @pl.loop(1, near)
    def _(step):
        push(step, got_a, 0).wait_recv()
        tail_over(step, got_a, 0).start()

    @pl.loop(0, near)
    def _(step):
        tail_in(step, got_a, 0).wait_recv()

    experts(got_a, 0, near, 0)
    send_back(0, near)
    back = pltpu.make_async_copy(outs.at[0, pl.ds(TAIL, cap)], ret.at[0], own_sem.at[1])
    back.start()

    @pl.loop(near, groups)
    def _(step):
        push(step, got_b, near).wait_recv()
        tail_over(step, got_b, near).start()

    @pl.loop(near, groups)
    def _(step):
        tail_in(step, got_b, near).wait_recv()

    experts(got_b, near, groups, local)
    send_back(near, groups)
    back.wait()

    @pl.loop(0, groups // 2)
    def _(half):
        @pl.when(half > 0)
        def _():
            give(half * 2).wait_recv()

        give(half * 2 + 1).wait_recv()
        add(half)

    @pl.loop(0, token_blocks)
    def _(b):
        at = pl.ds(pl.multiple_of(b * TOKEN_BLOCK, TOKEN_BLOCK), TOKEN_BLOCK)
        for c in range(0, dim, 128):
            mixed = x_ref[at, c : c + 128].astype(F32) + gates[0, at, :] * acc[0, at, c : c + 128].astype(F32)
            out_ref[at, c : c + 128] = (mixed + gates[1, at, :] * acc[1, at, c : c + 128].astype(F32)).astype(BF16)

    @pl.loop(1, near)
    def _(step):
        push(step, got_a, 0).wait_send()

    @pl.loop(near, groups)
    def _(step):
        push(step, got_b, near).wait_send()

    @pl.loop(0, near)
    def _(step):
        tail_over(step, got_a, 0).wait_send()

    @pl.loop(near, groups)
    def _(step):
        tail_over(step, got_b, near).wait_send()

    @pl.loop(0, groups)
    def _(step):
        pass_over(step).wait_send()

    @pl.loop(1, groups)
    def _(step):
        give(step).wait_send()


def solution(mesh):
    groups = mesh.shape["expert"]
    row_spec = P(("data", "expert"), None)
    weight_spec = P("expert", None, None)

    def device_step(token_rows, expert_ids, gate_weights, w_in, w_out):
        tokens, top_k = expert_ids.shape
        local, dim, hidden = w_in.shape
        experts = local * groups
        mean_load = tokens * top_k // experts
        capacity = groups * mean_load
        worst = local * (7 * mean_load // 4)
        usual = local * mean_load * 9 // 8
        stride = 2 * local * mean_load
        lanes = groups * WIN
        near = groups - 6
        depth = 4
        vmem = pl.BlockSpec(memory_space=VMEM)
        anywhere = pl.BlockSpec(memory_space=pl.ANY)

        def params(collective_id):
            return pltpu.CompilerParams(collective_id=collective_id, has_side_effects=True, vmem_limit_bytes=61 * 1024 * 1024)

        pair_sems = [pltpu.SemaphoreType.DMA((groups,)), pltpu.SemaphoreType.DMA((groups,))]
        pos, slot, start, place, fits = pl.pallas_call(
            functools.partial(route_kernel, groups, capacity, usual, worst, stride, local, near),
            out_shape=[
                jax.ShapeDtypeStruct((top_k, tokens), I32),
                jax.ShapeDtypeStruct((local, lanes), I32),
                jax.ShapeDtypeStruct((local, groups), I32),
                jax.ShapeDtypeStruct((2, local, capacity), I32),
                jax.ShapeDtypeStruct((1, 1), I32),
            ],
            in_specs=[vmem],
            out_specs=[vmem] * 5,
            scratch_shapes=[
                VMEM((groups, top_k, experts), F32),
                VMEM((experts, TOKEN_BLOCK), F32),
                VMEM((top_k, tokens), F32),
                VMEM((4, groups, experts), F32),
            ]
            + pair_sems,
            compiler_params=params(0),
            name="route",
        )(expert_ids.T)

        def exchange(cap, collective_id):
            def run():
                return pl.pallas_call(
                    functools.partial(moe_kernel, groups, cap, stride, local, near),
                    out_shape=jax.ShapeDtypeStruct((tokens, dim), BF16),
                    in_specs=[pl.BlockSpec(memory_space=pltpu.SMEM)] + [vmem] * 5 + [anywhere] * 2,
                    out_specs=vmem,
                    scratch_shapes=[
                        VMEM((groups, cap // ALIGN, ALIGN, dim), BF16),
                        VMEM(((near * (cap + TAIL) + WIN) // ALIGN, ALIGN, dim), BF16),
                        VMEM((((groups - near) * (cap + TAIL) + WIN) // ALIGN, ALIGN, dim), BF16),
                        VMEM((groups, cap + TAIL, dim), BF16),
                        VMEM((groups, TAIL, dim), BF16),
                        VMEM((groups, cap, dim), BF16),
                        VMEM((depth, dim, hidden), BF16),
                        VMEM((depth, hidden, dim), BF16),
                        VMEM((2, near * WIN, dim), BF16),
                        VMEM((2 * capacity, dim), BF16),
                        VMEM((top_k, tokens, 128), I32),
                        VMEM((top_k, tokens, 128), F32),
                        VMEM((top_k, tokens, dim), BF16),
                        pltpu.SemaphoreType.DMA((2, depth)),
                    ]
                    + pair_sems * 4
                    + [pltpu.SemaphoreType.DMA((2,))],
                    compiler_params=params(collective_id),
                    name="experts",
                )(start, slot, place, pos, gate_weights.T, token_rows, w_in, w_out)

            return run

        return lax.cond(fits.reshape(()) > 0, exchange(usual, 1), exchange(worst, 2))

    return jax.shard_map(device_step, mesh=mesh, in_specs=(row_spec, row_spec, row_spec, weight_spec, weight_spec), out_specs=row_spec, check_vma=False)
```

```python
import functools

import jax
import jax.numpy as jnp
from jax import lax
from jax.experimental import pallas as pl
from jax.experimental.pallas import tpu as pltpu
from jax.sharding import PartitionSpec as P

MESH = pl.DeviceIdType.MESH
VMEM = pltpu.VMEM
F32, BF16, I32 = jnp.float32, jnp.bfloat16, jnp.int32
WIN = 32
ALIGN = 16
TAIL = 48
TOKEN_BLOCK = 256


def iota(shape, dim):
    return lax.broadcasted_iota(I32, shape, dim)


def chips_away(step, chips):
    half = step // 2
    return lax.rem(2 * half + 3 * (half // (chips // 2)), chips)


def peer(me, step, groups):
    chips = groups // 2
    chip = lax.rem(me // 2 + chips_away(step, chips), chips)
    return chip * 2 + lax.rem(me + step, 2)


def source_of(me, step, groups):
    chips = groups // 2
    chip = lax.rem(me // 2 - chips_away(step, chips) + chips, chips)
    return chip * 2 + lax.rem(me + step, 2)


def announce(me, groups):
    barrier = pltpu.get_barrier_semaphore()

    @pl.loop(1, groups)
    def _(step):
        pl.semaphore_signal(barrier, inc=1, device_id={"expert": lax.rem(me + step, groups)}, device_id_type=MESH)

    return barrier


def route_kernel(groups, capacity, cap, worst, stride, local, near, ids_ref, pos_ref, slot_ref, start_ref, place_ref, fits_ref, cnt, carry, rank, rows, send_sem, recv_sem):
    me = lax.axis_index("expert")
    tokens = ids_ref.shape[1]
    experts = local * groups
    blocks = tokens // TOKEN_BLOCK
    barrier = announce(me, groups)

    expert_rows = iota((experts, TOKEN_BLOCK), 0)
    upper = (iota((TOKEN_BLOCK, TOKEN_BLOCK), 0) <= iota((TOKEN_BLOCK, TOKEN_BLOCK), 1)).astype(BF16)
    ones = jnp.ones((TOKEN_BLOCK, TOKEN_BLOCK), BF16)
    for j in range(2):
        carry[...] = jnp.zeros_like(carry)

        def count_block(b, row):
            cols = pl.ds(pl.multiple_of(b * TOKEN_BLOCK, TOKEN_BLOCK), TOKEN_BLOCK)
            hot = expert_rows == ids_ref[j : j + 1, cols]
            hot16 = jnp.where(hot, 1.0, 0.0).astype(BF16)
            run = jnp.dot(hot16, upper, preferred_element_type=F32) + carry[...]
            rank[j : j + 1, cols] = jnp.sum(jnp.where(hot, run, 0.0), axis=0, keepdims=True) - 1.0
            carry[...] += jnp.dot(hot16, ones, preferred_element_type=F32)
            return row + lax.dot_general(ones[:8], hot16, (((1,), (1,)), ((), ())), preferred_element_type=F32)

        row = lax.fori_loop(0, blocks, count_block, jnp.zeros((8, experts), F32))
        cnt[me, j : j + 1, :] = row[:1]

    def send(step):
        to = lax.rem(me + step, groups)
        return pltpu.make_async_remote_copy(src_ref=cnt.at[me], dst_ref=cnt.at[me], send_sem=send_sem.at[step], recv_sem=recv_sem.at[step], device_id={"expert": to}, device_id_type=MESH)

    def arrive(step):
        origin = lax.rem(me - step + groups, groups)
        return pltpu.make_async_remote_copy(src_ref=cnt.at[origin], dst_ref=cnt.at[origin], send_sem=send_sem.at[step], recv_sem=recv_sem.at[step], device_id={"expert": origin}, device_id_type=MESH)

    pl.semaphore_wait(barrier, groups - 1)

    @pl.loop(1, groups)
    def _(step):
        send(step).start()

    @pl.loop(1, groups)
    def _(step):
        arrive(step).wait_recv()

    @pl.loop(1, groups)
    def _(step):
        send(step).wait_send()

    first, second = cnt[:, 0, :], cnt[:, 1, :]
    earlier = (iota((groups, groups), 1) < iota((groups, groups), 0)).astype(BF16)
    before0 = jnp.dot(earlier, first.astype(BF16), preferred_element_type=F32)
    before1 = jnp.dot(earlier, second.astype(BF16), preferred_element_type=F32)
    total0 = jnp.sum(first, axis=0, keepdims=True)
    keep0 = jnp.clip(capacity - before0, 0.0, first)
    keep1 = jnp.clip(capacity - total0 - before1, 0.0, second)
    keep = keep0 + keep1
    keep16 = keep.astype(BF16)
    er, ec = iota((experts, experts), 0), iota((experts, experts), 1)
    mate = er // local - ec // local + 2 * (ec // local % 2)
    same = er // local == ec // local
    load = jnp.dot(keep16, same.astype(BF16), preferred_element_type=F32)
    mate_load = jnp.dot(keep16, (mate == 1).astype(BF16), preferred_element_type=F32)
    inside = jnp.dot(keep16, (same & (er < ec)).astype(BF16), preferred_element_type=F32)
    over = jnp.maximum(load - cap, 0.0)
    bad = (over > TAIL) | ((over > 0.0) & (mate_load + over > cap))
    worse = jnp.max(jnp.max(jnp.where(bad, 1.0, 0.0), axis=1, keepdims=True), axis=0, keepdims=True)
    fits_ref[...] = jnp.broadcast_to(1.0 - worse, fits_ref.shape).astype(I32)
    over = jnp.where(worse > 0.0, 0.0, over)
    size = jnp.where(worse > 0.0, float(worst), float(cap))
    offset = TAIL - over + inside
    high = jnp.floor(offset * (1.0 / ALIGN))
    low = offset - high * ALIGN

    rows[0], rows[1], rows[2], rows[3] = high, low, keep0, keep1
    table = jnp.concatenate([rows[i, pl.ds(me, 1), :] for i in range(4)] + [jnp.zeros((4, experts), F32)], axis=0).astype(BF16)
    side = lax.rem(me, 2)
    for j in range(2):

        def place_block(b, _):
            cols = pl.ds(pl.multiple_of(b * TOKEN_BLOCK, TOKEN_BLOCK), TOKEN_BLOCK)
            ids = ids_ref[j : j + 1, cols]
            hot16 = jnp.where(expert_rows == ids, 1.0, 0.0).astype(BF16)
            found = jnp.dot(table, hot16, preferred_element_type=F32)
            rk = rank[j : j + 1, cols]
            spot = found[0:1] * ALIGN + found[1:2] + rk
            if j == 1:
                spot = spot + found[2:3]
            owner = ids // local
            half = ((owner + side) % 2).astype(F32)
            direct = spot >= TAIL
            row = jnp.where(direct, half * size + spot - TAIL, (2.0 - half) * size + spot - TAIL)
            key = row.astype(I32) + (owner // 2) * (2 * stride)
            pos_ref[j : j + 1, cols] = jnp.where(rk < found[2 + j : 3 + j], key, -1)
            return 0

        lax.fori_loop(0, blocks, place_block, 0)

    mine = (iota((local, experts), 1) == iota((local, experts), 0) + me * local).astype(BF16)

    def pick(values):
        return lax.dot_general(mine, values.astype(BF16), (((1,), (1,)), ((), ())), preferred_element_type=F32)

    from_step = (source_of(me, iota((groups, groups), 0), groups) == iota((groups, groups), 1)).astype(BF16)
    older, newer = iota((groups, groups), 1), iota((groups, groups), 0)
    ahead_of = ((older < newer) & ((older < near) == (newer < near))).astype(BF16)

    def by_step(values):
        return jnp.dot(from_step, values.astype(BF16), preferred_element_type=F32)

    kept = by_step(keep)
    ahead = pick(jnp.dot(ahead_of, kept.astype(BF16), preferred_element_type=F32))
    high, low, kept = pick(by_step(high)), pick(by_step(low)), pick(kept)
    start_ref[...] = high.astype(I32)
    lanes = groups * WIN
    spread = (iota((groups, lanes), 1) // WIN == iota((groups, lanes), 0)).astype(BF16)

    def widen(values):
        return jnp.dot(values.astype(BF16), spread, preferred_element_type=F32)

    wide_low, wide_kept, wide_ahead = widen(low), widen(kept), widen(ahead)
    lane = (iota((local, lanes), 1) % WIN).astype(F32)
    valid = (lane >= wide_low) & (lane < wide_low + wide_kept)
    slot_ref[...] = jnp.where(valid, wide_ahead + lane - wide_low, -1.0).astype(I32)
    seat = iota((local, capacity), 1).astype(F32)
    goals = [jnp.full((local, capacity), -1.0, F32) for _ in range(2)]
    for step in range(groups):
        begin, count = ahead[:, step : step + 1], kept[:, step : step + 1]
        spot = high[:, step : step + 1] * ALIGN + low[:, step : step + 1] + step * stride
        part = int(step >= near)
        goals[part] = jnp.where((seat >= begin) & (seat < begin + count), seat - begin + spot, goals[part])
    for part in range(2):
        place_ref[part] = goals[part].astype(I32)


def moe_kernel(groups, cap, stride, local, near, start_ref, slot_ref, place_ref, pos_ref, gate_ref, x_ref, w_in_hbm, w_out_hbm, out_ref, buf, got_a, got_b, outs, tails, ret, w_in, w_out, win, obuf, spots, gates, acc, w_sem, send_sem, recv_sem, back_send, back_recv, tail_send, tail_recv, pass_send, pass_recv, own_sem):
    me = lax.axis_index("expert")
    tokens, dim = x_ref.shape
    depth = w_in.shape[0]
    full = cap + TAIL
    full_blocks, cap_blocks, tail_blocks = full // ALIGN, cap // ALIGN, TAIL // ALIGN
    token_blocks = tokens // TOKEN_BLOCK
    sibling = {"expert": me + 1 - 2 * lax.rem(me, 2)}
    barrier = announce(me, groups)

    def fetch(visit):
        e, place = lax.rem(visit, local), lax.rem(visit, depth)
        return (
            pltpu.make_async_copy(w_in_hbm.at[e], w_in.at[place], w_sem.at[0, place]),
            pltpu.make_async_copy(w_out_hbm.at[e], w_out.at[place], w_sem.at[1, place]),
        )

    for visit in range(depth):
        for copy in fetch(visit):
            copy.start()

    def mate_of(step):
        return step + 1 - 2 * lax.rem(step, 2)

    def push(step, got, first):
        return pltpu.make_async_remote_copy(src_ref=buf.at[step], dst_ref=got.at[pl.ds((step - first) * full_blocks + tail_blocks, cap_blocks)], send_sem=send_sem.at[step], recv_sem=recv_sem.at[step], device_id={"expert": peer(me, step, groups)}, device_id_type=MESH)

    def tail_over(step, got, first):
        return pltpu.make_async_remote_copy(src_ref=got.at[pl.ds((step - first) * full_blocks + cap_blocks, tail_blocks)], dst_ref=got.at[pl.ds((mate_of(step) - first) * full_blocks, tail_blocks)], send_sem=tail_send.at[step], recv_sem=tail_recv.at[mate_of(step)], device_id=sibling, device_id_type=MESH)

    def tail_in(step, got, first):
        return pltpu.make_async_remote_copy(src_ref=got.at[pl.ds((mate_of(step) - first) * full_blocks + cap_blocks, tail_blocks)], dst_ref=got.at[pl.ds((step - first) * full_blocks, tail_blocks)], send_sem=tail_send.at[mate_of(step)], recv_sem=tail_recv.at[step], device_id=sibling, device_id_type=MESH)

    def pass_over(step):
        return pltpu.make_async_remote_copy(src_ref=outs.at[step, pl.ds(0, TAIL)], dst_ref=tails.at[mate_of(step)], send_sem=pass_send.at[step], recv_sem=pass_recv.at[mate_of(step)], device_id=sibling, device_id_type=MESH)

    def pass_in(step):
        return pltpu.make_async_remote_copy(src_ref=outs.at[mate_of(step), pl.ds(0, TAIL)], dst_ref=tails.at[step], send_sem=pass_send.at[mate_of(step)], recv_sem=pass_recv.at[step], device_id=sibling, device_id_type=MESH)

    def give(step):
        return pltpu.make_async_remote_copy(src_ref=outs.at[step, pl.ds(TAIL, cap)], dst_ref=ret.at[step], send_sem=back_send.at[step], recv_sem=back_recv.at[step], device_id={"expert": source_of(me, step, groups)}, device_id_type=MESH)

    def pack(step):
        base = peer(me, step, groups) // 2 * (2 * stride) + lax.rem(step, 2) * cap
        spot = pos_ref[...] - base
        line = iota((cap, tokens), 0)
        hot = (line == spot[0:1]) | (line == spot[1:2])
        rows = jnp.dot(jnp.where(hot, 1.0, 0.0).astype(BF16), x_ref[...], preferred_element_type=F32).astype(BF16)
        buf[step] = rows.reshape(cap_blocks, ALIGN, dim)

    pack(0)
    pl.semaphore_wait(barrier, groups - 1)

    @pl.loop(1, groups)
    def _(step):
        pack(step)

        @pl.when(step < near)
        def _():
            push(step, got_a, 0).start()

        @pl.when(step >= near)
        def _():
            push(step, got_b, near).start()

    mine = pltpu.make_async_copy(buf.at[0], got_a.at[pl.ds(tail_blocks, cap_blocks)], own_sem.at[0])
    mine.start()
    pad = WIN // ALIGN
    got_a[pl.ds(near * full_blocks, pad)] = jnp.zeros((pad, ALIGN, dim), BF16)
    got_b[pl.ds((groups - near) * full_blocks, pad)] = jnp.zeros((pad, ALIGN, dim), BF16)

    @pl.loop(0, groups)
    def _(step):
        outs[step] = jnp.zeros((full, dim), BF16)

    @pl.loop(0, tokens // 128)
    def _(b):
        at = pl.ds(pl.multiple_of(b * 128, 128), 128)
        for j in range(2):
            spots[j, at, :] = jnp.broadcast_to(pos_ref[j : j + 1, at], (128, 128)).T
            gates[j, at, :] = jnp.broadcast_to(gate_ref[j : j + 1, at], (128, 128)).T
            acc[j, at, :] = jnp.zeros((128, dim), BF16)

    def experts(got, first, last, done):
        lanes = (last - first) * WIN

        @pl.loop(0, local // 4)
        def _(quad):
            @pl.loop(0, 2)
            def _(twin):
                pair = quad * 2 + twin
                for k in range(2):
                    e = pair * 2 + k
                    for step in range(first, last):
                        row = (step - first) * full_blocks + start_ref[e, step]
                        for half in range(WIN // ALIGN):
                            at = (step - first) * WIN + half * ALIGN
                            win[k, at : at + ALIGN, :] = got[row + half]
                for k in range(2):
                    e = pair * 2 + k
                    visit = done + e
                    place = lax.rem(visit, depth)
                    for copy in fetch(visit):
                        copy.wait()
                    slot = slot_ref[pl.ds(e, 1), :][:, first * WIN : last * WIN]
                    hot = jnp.where(iota((128, lanes), 0) == slot, 1.0, 0.0).astype(BF16)
                    x = jnp.dot(hot, win[k, :lanes, :], preferred_element_type=F32).astype(BF16)
                    h = jax.nn.gelu(jnp.dot(x, w_in[place], preferred_element_type=F32)).astype(BF16)
                    o = jnp.dot(h, w_out[place], preferred_element_type=F32).astype(BF16)
                    obuf[pl.ds(pl.multiple_of(twin * 256 + k * 128, 128), 128), :] = o
                for k in range(2):
                    visit = done + pair * 2 + k + depth

                    @pl.when(visit < 2 * local)
                    def _():
                        for copy in fetch(visit):
                            copy.start()

            part = 0 if first == 0 else 1
            goal = jnp.concatenate([place_ref[part, pl.ds(quad * 4 + k, 1), :] for k in range(4)], axis=1)

            @pl.loop(first, last)
            def _(step):
                hot = jnp.where(iota((full, 512), 0) == goal - step * stride, 1.0, 0.0).astype(BF16)
                outs[step] += jnp.dot(hot, obuf[...], preferred_element_type=F32).astype(BF16)

    def send_back(first, last):
        @pl.loop(first, last)
        def _(step):
            pass_over(step).start()

        @pl.loop(first, last)
        def _(step):
            pass_in(step).wait_recv()
            outs[step, cap:, :] += tails[step]

            @pl.when(step > 0)
            def _():
                give(step).start()

    def add(half):
        base = peer(me, half * 2, groups) // 2 * (2 * stride)
        returned = ret[pl.ds(half * 2, 2)].reshape(2 * cap, dim)

        @pl.loop(0, token_blocks)
        def _(b):
            at = pl.ds(pl.multiple_of(b * TOKEN_BLOCK, TOKEN_BLOCK), TOKEN_BLOCK)
            lane = iota((TOKEN_BLOCK, 128), 1)
            for j in range(2):
                spot = spots[j, at, :] - base
                hot = jnp.concatenate([jnp.where(spot - k == lane, 1.0, 0.0).astype(BF16) for k in range(0, 2 * cap, 128)], axis=1)
                acc[j, at, :] += jnp.dot(hot[:, : 2 * cap], returned, preferred_element_type=F32).astype(BF16)

    mine.wait()
    tail_over(0, got_a, 0).start()

    @pl.loop(1, near)
    def _(step):
        push(step, got_a, 0).wait_recv()
        tail_over(step, got_a, 0).start()

    @pl.loop(0, near)
    def _(step):
        tail_in(step, got_a, 0).wait_recv()

    experts(got_a, 0, near, 0)
    send_back(0, near)
    back = pltpu.make_async_copy(outs.at[0, pl.ds(TAIL, cap)], ret.at[0], own_sem.at[1])
    back.start()

    @pl.loop(near, groups)
    def _(step):
        push(step, got_b, near).wait_recv()
        tail_over(step, got_b, near).start()

    @pl.loop(near, groups)
    def _(step):
        tail_in(step, got_b, near).wait_recv()

    experts(got_b, near, groups, local)
    send_back(near, groups)
    back.wait()

    @pl.loop(0, groups // 2)
    def _(half):
        @pl.when(half > 0)
        def _():
            give(half * 2).wait_recv()

        give(half * 2 + 1).wait_recv()
        add(half)

    @pl.loop(0, token_blocks)
    def _(b):
        at = pl.ds(pl.multiple_of(b * TOKEN_BLOCK, TOKEN_BLOCK), TOKEN_BLOCK)
        for c in range(0, dim, 128):
            mixed = x_ref[at, c : c + 128].astype(F32) + gates[0, at, :] * acc[0, at, c : c + 128].astype(F32)
            out_ref[at, c : c + 128] = (mixed + gates[1, at, :] * acc[1, at, c : c + 128].astype(F32)).astype(BF16)

    @pl.loop(1, near)
    def _(step):
        push(step, got_a, 0).wait_send()

    @pl.loop(near, groups)
    def _(step):
        push(step, got_b, near).wait_send()

    @pl.loop(0, near)
    def _(step):
        tail_over(step, got_a, 0).wait_send()

    @pl.loop(near, groups)
    def _(step):
        tail_over(step, got_b, near).wait_send()

    @pl.loop(0, groups)
    def _(step):
        pass_over(step).wait_send()

    @pl.loop(1, groups)
    def _(step):
        give(step).wait_send()


def solution(mesh):
    groups = mesh.shape["expert"]
    row_spec = P(("data", "expert"), None)
    weight_spec = P("expert", None, None)

    def device_step(token_rows, expert_ids, gate_weights, w_in, w_out):
        tokens, top_k = expert_ids.shape
        local, dim, hidden = w_in.shape
        experts = local * groups
        mean_load = tokens * top_k // experts
        capacity = groups * mean_load
        worst = local * (7 * mean_load // 4)
        usual = local * mean_load * 9 // 8
        stride = 2 * local * mean_load
        lanes = groups * WIN
        near = groups // 2
        depth = 4
        vmem = pl.BlockSpec(memory_space=VMEM)
        anywhere = pl.BlockSpec(memory_space=pl.ANY)

        def params(collective_id):
            return pltpu.CompilerParams(collective_id=collective_id, has_side_effects=True, vmem_limit_bytes=61 * 1024 * 1024)

        pair_sems = [pltpu.SemaphoreType.DMA((groups,)), pltpu.SemaphoreType.DMA((groups,))]
        pos, slot, start, place, fits = pl.pallas_call(
            functools.partial(route_kernel, groups, capacity, usual, worst, stride, local, near),
            out_shape=[
                jax.ShapeDtypeStruct((top_k, tokens), I32),
                jax.ShapeDtypeStruct((local, lanes), I32),
                jax.ShapeDtypeStruct((local, groups), I32),
                jax.ShapeDtypeStruct((2, local, capacity), I32),
                jax.ShapeDtypeStruct((1, 1), I32),
            ],
            in_specs=[vmem],
            out_specs=[vmem] * 5,
            scratch_shapes=[
                VMEM((groups, top_k, experts), F32),
                VMEM((experts, TOKEN_BLOCK), F32),
                VMEM((top_k, tokens), F32),
                VMEM((4, groups, experts), F32),
            ]
            + pair_sems,
            compiler_params=params(0),
            name="route",
        )(expert_ids.T)

        def exchange(cap, collective_id):
            def run():
                return pl.pallas_call(
                    functools.partial(moe_kernel, groups, cap, stride, local, near),
                    out_shape=jax.ShapeDtypeStruct((tokens, dim), BF16),
                    in_specs=[pl.BlockSpec(memory_space=pltpu.SMEM)] + [vmem] * 5 + [anywhere] * 2,
                    out_specs=vmem,
                    scratch_shapes=[
                        VMEM((groups, cap // ALIGN, ALIGN, dim), BF16),
                        VMEM(((near * (cap + TAIL) + WIN) // ALIGN, ALIGN, dim), BF16),
                        VMEM((((groups - near) * (cap + TAIL) + WIN) // ALIGN, ALIGN, dim), BF16),
                        VMEM((groups, cap + TAIL, dim), BF16),
                        VMEM((groups, TAIL, dim), BF16),
                        VMEM((groups, cap, dim), BF16),
                        VMEM((depth, dim, hidden), BF16),
                        VMEM((depth, hidden, dim), BF16),
                        VMEM((2, near * WIN, dim), BF16),
                        VMEM((4 * capacity, dim), BF16),
                        VMEM((top_k, tokens, 128), I32),
                        VMEM((top_k, tokens, 128), F32),
                        VMEM((top_k, tokens, dim), BF16),
                        pltpu.SemaphoreType.DMA((2, depth)),
                    ]
                    + pair_sems * 4
                    + [pltpu.SemaphoreType.DMA((2,))],
                    compiler_params=params(collective_id),
                    name="experts",
                )(start, slot, place, pos, gate_weights.T, token_rows, w_in, w_out)

            return run

        return lax.cond(fits.reshape(()) > 0, exchange(usual, 1), exchange(worst, 2))

    return jax.shard_map(device_step, mesh=mesh, in_specs=(row_spec, row_spec, row_spec, weight_spec, weight_spec), out_specs=row_spec, check_vma=False)
```

```python
import functools

import jax
import jax.numpy as jnp
from jax import lax
from jax.experimental import pallas as pl
from jax.experimental.pallas import tpu as pltpu
from jax.sharding import PartitionSpec as P

MESH = pl.DeviceIdType.MESH
VMEM = pltpu.VMEM
F32, BF16, I32 = jnp.float32, jnp.bfloat16, jnp.int32
WIN = 32
ALIGN = 16
TAIL = 48
TOKEN_BLOCK = 256


def iota(shape, dim):
    return lax.broadcasted_iota(I32, shape, dim)


def chips_away(step, chips):
    half = step // 2
    return lax.rem(2 * half + 3 * (half // (chips // 2)), chips)


def peer(me, step, groups):
    chips = groups // 2
    chip = lax.rem(me // 2 + chips_away(step, chips), chips)
    return chip * 2 + lax.rem(me + step, 2)


def source_of(me, step, groups):
    chips = groups // 2
    chip = lax.rem(me // 2 - chips_away(step, chips) + chips, chips)
    return chip * 2 + lax.rem(me + step, 2)


def announce(me, groups):
    barrier = pltpu.get_barrier_semaphore()

    @pl.loop(1, groups)
    def _(step):
        pl.semaphore_signal(barrier, inc=1, device_id={"expert": lax.rem(me + step, groups)}, device_id_type=MESH)

    return barrier


def route_kernel(groups, capacity, cap, worst, stride, local, near, ids_ref, pos_ref, slot_ref, start_ref, place_ref, fits_ref, cnt, carry, rank, rows, send_sem, recv_sem):
    me = lax.axis_index("expert")
    tokens = ids_ref.shape[1]
    experts = local * groups
    blocks = tokens // TOKEN_BLOCK
    barrier = announce(me, groups)

    expert_rows = iota((experts, TOKEN_BLOCK), 0)
    upper = (iota((TOKEN_BLOCK, TOKEN_BLOCK), 0) <= iota((TOKEN_BLOCK, TOKEN_BLOCK), 1)).astype(BF16)
    carry[...] = jnp.zeros_like(carry)

    @pl.loop(0, blocks)
    def _(b):
        cols = pl.ds(pl.multiple_of(b * TOKEN_BLOCK, TOKEN_BLOCK), TOKEN_BLOCK)
        for j in range(2):
            hot = expert_rows == ids_ref[j : j + 1, cols]
            run = jnp.dot(jnp.where(hot, 1.0, 0.0).astype(BF16), upper, preferred_element_type=F32)
            run = run + jnp.concatenate([carry[j]] * (TOKEN_BLOCK // 128), axis=1)
            rank[j : j + 1, cols] = jnp.sum(jnp.where(hot, run, 0.0), axis=0, keepdims=True) - 1.0
            carry[j] = jnp.broadcast_to(run[:, TOKEN_BLOCK - 1 :], (experts, 128))

    for j in range(2):
        row = jnp.concatenate([carry[j, k : k + 128, :].T[:1] for k in range(0, experts, 128)], axis=1)
        cnt[me, j : j + 1, :] = row

    def send(step):
        to = lax.rem(me + step, groups)
        return pltpu.make_async_remote_copy(src_ref=cnt.at[me], dst_ref=cnt.at[me], send_sem=send_sem.at[step], recv_sem=recv_sem.at[step], device_id={"expert": to}, device_id_type=MESH)

    def arrive(step):
        origin = lax.rem(me - step + groups, groups)
        return pltpu.make_async_remote_copy(src_ref=cnt.at[origin], dst_ref=cnt.at[origin], send_sem=send_sem.at[step], recv_sem=recv_sem.at[step], device_id={"expert": origin}, device_id_type=MESH)

    pl.semaphore_wait(barrier, groups - 1)

    @pl.loop(1, groups)
    def _(step):
        send(step).start()

    @pl.loop(1, groups)
    def _(step):
        arrive(step).wait_recv()

    @pl.loop(1, groups)
    def _(step):
        send(step).wait_send()

    first, second = cnt[:, 0, :], cnt[:, 1, :]
    earlier = (iota((groups, groups), 1) < iota((groups, groups), 0)).astype(BF16)
    before0 = jnp.dot(earlier, first.astype(BF16), preferred_element_type=F32)
    before1 = jnp.dot(earlier, second.astype(BF16), preferred_element_type=F32)
    total0 = jnp.sum(first, axis=0, keepdims=True)
    keep0 = jnp.clip(capacity - before0, 0.0, first)
    keep1 = jnp.clip(capacity - total0 - before1, 0.0, second)
    keep = keep0 + keep1
    keep16 = keep.astype(BF16)
    er, ec = iota((experts, experts), 0), iota((experts, experts), 1)
    mate = er // local - ec // local + 2 * (ec // local % 2)
    same = er // local == ec // local
    load = jnp.dot(keep16, same.astype(BF16), preferred_element_type=F32)
    mate_load = jnp.dot(keep16, (mate == 1).astype(BF16), preferred_element_type=F32)
    inside = jnp.dot(keep16, (same & (er < ec)).astype(BF16), preferred_element_type=F32)
    over = jnp.maximum(load - cap, 0.0)
    bad = (over > TAIL) | ((over > 0.0) & (mate_load + over > cap))
    worse = jnp.max(jnp.max(jnp.where(bad, 1.0, 0.0), axis=1, keepdims=True), axis=0, keepdims=True)
    fits_ref[...] = jnp.broadcast_to(1.0 - worse, fits_ref.shape).astype(I32)
    over = jnp.where(worse > 0.0, 0.0, over)
    size = jnp.where(worse > 0.0, float(worst), float(cap))
    offset = TAIL - over + inside
    high = jnp.floor(offset * (1.0 / ALIGN))
    low = offset - high * ALIGN

    rows[0], rows[1], rows[2], rows[3] = high, low, keep0, keep1
    table = jnp.concatenate([rows[i, pl.ds(me, 1), :] for i in range(4)] + [jnp.zeros((4, experts), F32)], axis=0).astype(BF16)
    side = lax.rem(me, 2)

    @pl.loop(0, blocks)
    def _(b):
        cols = pl.ds(pl.multiple_of(b * TOKEN_BLOCK, TOKEN_BLOCK), TOKEN_BLOCK)
        for j in range(2):
            ids = ids_ref[j : j + 1, cols]
            hot16 = jnp.where(expert_rows == ids, 1.0, 0.0).astype(BF16)
            found = jnp.dot(table, hot16, preferred_element_type=F32)
            rk = rank[j : j + 1, cols]
            spot = found[0:1] * ALIGN + found[1:2] + rk
            if j == 1:
                spot = spot + found[2:3]
            owner = ids // local
            half = ((owner + side) % 2).astype(F32)
            direct = spot >= TAIL
            row = jnp.where(direct, half * size + spot - TAIL, (2.0 - half) * size + spot - TAIL)
            key = row.astype(I32) + (owner // 2) * (2 * stride)
            pos_ref[j : j + 1, cols] = jnp.where(rk < found[2 + j : 3 + j], key, -1)

    mine = (iota((local, experts), 1) == iota((local, experts), 0) + me * local).astype(BF16)

    def pick(values):
        return lax.dot_general(mine, values.astype(BF16), (((1,), (1,)), ((), ())), preferred_element_type=F32)

    from_step = (source_of(me, iota((groups, groups), 0), groups) == iota((groups, groups), 1)).astype(BF16)
    older, newer = iota((groups, groups), 1), iota((groups, groups), 0)
    ahead_of = ((older < newer) & ((older < near) == (newer < near))).astype(BF16)

    def by_step(values):
        return jnp.dot(from_step, values.astype(BF16), preferred_element_type=F32)

    kept = by_step(keep)
    ahead = pick(jnp.dot(ahead_of, kept.astype(BF16), preferred_element_type=F32))
    high, low, kept = pick(by_step(high)), pick(by_step(low)), pick(kept)
    start_ref[...] = high.astype(I32)
    lanes = groups * WIN
    spread = (iota((groups, lanes), 1) // WIN == iota((groups, lanes), 0)).astype(BF16)

    def widen(values):
        return jnp.dot(values.astype(BF16), spread, preferred_element_type=F32)

    wide_low, wide_kept, wide_ahead = widen(low), widen(kept), widen(ahead)
    lane = (iota((local, lanes), 1) % WIN).astype(F32)
    valid = (lane >= wide_low) & (lane < wide_low + wide_kept)
    slot_ref[...] = jnp.where(valid, wide_ahead + lane - wide_low, -1.0).astype(I32)
    seat = iota((local, capacity), 1).astype(F32)
    goals = [jnp.full((local, capacity), -1.0, F32) for _ in range(2)]
    for step in range(groups):
        begin, count = ahead[:, step : step + 1], kept[:, step : step + 1]
        spot = high[:, step : step + 1] * ALIGN + low[:, step : step + 1] + step * stride
        part = int(step >= near)
        goals[part] = jnp.where((seat >= begin) & (seat < begin + count), seat - begin + spot, goals[part])
    for part in range(2):
        place_ref[part] = goals[part].astype(I32)


def moe_kernel(groups, cap, stride, local, near, start_ref, slot_ref, place_ref, pos_ref, gate_ref, x_hbm, w_in_hbm, w_out_hbm, out_ref, x_ref, buf, got_a, got_b, outs, tails, ret, w_in, w_out, win, obuf, spots, gates, acc, w_sem, send_sem, recv_sem, back_send, back_recv, tail_send, tail_recv, pass_send, pass_recv, own_sem):
    me = lax.axis_index("expert")
    tokens, dim = x_ref.shape
    depth = w_in.shape[0]
    x_copy = pltpu.make_async_copy(x_hbm, x_ref, own_sem.at[2])
    x_copy.start()
    full = cap + TAIL
    full_blocks, cap_blocks, tail_blocks = full // ALIGN, cap // ALIGN, TAIL // ALIGN
    token_blocks = tokens // TOKEN_BLOCK
    sibling = {"expert": me + 1 - 2 * lax.rem(me, 2)}
    barrier = announce(me, groups)

    def fetch(visit):
        e, place = lax.rem(visit, local), lax.rem(visit, depth)
        return (
            pltpu.make_async_copy(w_in_hbm.at[e], w_in.at[place], w_sem.at[0, place]),
            pltpu.make_async_copy(w_out_hbm.at[e], w_out.at[place], w_sem.at[1, place]),
        )

    for visit in range(depth):
        for copy in fetch(visit):
            copy.start()

    def mate_of(step):
        return step + 1 - 2 * lax.rem(step, 2)

    def push(step, got, first):
        return pltpu.make_async_remote_copy(src_ref=buf.at[step], dst_ref=got.at[pl.ds((step - first) * full_blocks + tail_blocks, cap_blocks)], send_sem=send_sem.at[step], recv_sem=recv_sem.at[step], device_id={"expert": peer(me, step, groups)}, device_id_type=MESH)

    def tail_over(step, got, first):
        return pltpu.make_async_remote_copy(src_ref=got.at[pl.ds((step - first) * full_blocks + cap_blocks, tail_blocks)], dst_ref=got.at[pl.ds((mate_of(step) - first) * full_blocks, tail_blocks)], send_sem=tail_send.at[step], recv_sem=tail_recv.at[mate_of(step)], device_id=sibling, device_id_type=MESH)

    def tail_in(step, got, first):
        return pltpu.make_async_remote_copy(src_ref=got.at[pl.ds((mate_of(step) - first) * full_blocks + cap_blocks, tail_blocks)], dst_ref=got.at[pl.ds((step - first) * full_blocks, tail_blocks)], send_sem=tail_send.at[mate_of(step)], recv_sem=tail_recv.at[step], device_id=sibling, device_id_type=MESH)

    def pass_over(step):
        return pltpu.make_async_remote_copy(src_ref=outs.at[step, pl.ds(0, TAIL)], dst_ref=tails.at[mate_of(step)], send_sem=pass_send.at[step], recv_sem=pass_recv.at[mate_of(step)], device_id=sibling, device_id_type=MESH)

    def pass_in(step):
        return pltpu.make_async_remote_copy(src_ref=outs.at[mate_of(step), pl.ds(0, TAIL)], dst_ref=tails.at[step], send_sem=pass_send.at[mate_of(step)], recv_sem=pass_recv.at[step], device_id=sibling, device_id_type=MESH)

    def berth(step):
        rest = step - (groups - 4)
        return step + step // (groups - 4) * (rest % 2 * 2 + rest // 2 - rest)

    def give(step):
        return pltpu.make_async_remote_copy(src_ref=outs.at[step, pl.ds(TAIL, cap)], dst_ref=ret.at[berth(step)], send_sem=back_send.at[step], recv_sem=back_recv.at[step], device_id={"expert": source_of(me, step, groups)}, device_id_type=MESH)

    def pack(step):
        base = peer(me, step, groups) // 2 * (2 * stride) + lax.rem(step, 2) * cap
        spot = pos_ref[...] - base
        line = iota((cap, tokens), 0)
        hot = (line == spot[0:1]) | (line == spot[1:2])
        rows = jnp.dot(jnp.where(hot, 1.0, 0.0).astype(BF16), x_ref[...], preferred_element_type=F32).astype(BF16)
        buf[step] = rows.reshape(cap_blocks, ALIGN, dim)

    x_copy.wait()
    pack(0)
    pl.semaphore_wait(barrier, groups - 1)

    @pl.loop(1, groups)
    def _(step):
        pack(step)

        @pl.when(step < near)
        def _():
            push(step, got_a, 0).start()

        @pl.when(step >= near)
        def _():
            push(step, got_b, near).start()

    mine = pltpu.make_async_copy(buf.at[0], got_a.at[pl.ds(tail_blocks, cap_blocks)], own_sem.at[0])
    mine.start()
    pad = WIN // ALIGN
    got_a[pl.ds(near * full_blocks, pad)] = jnp.zeros((pad, ALIGN, dim), BF16)
    got_b[pl.ds((groups - near) * full_blocks, pad)] = jnp.zeros((pad, ALIGN, dim), BF16)

    @pl.loop(0, groups)
    def _(step):
        outs[step] = jnp.zeros((full, dim), BF16)

    @pl.loop(0, tokens // 128)
    def _(b):
        at = pl.ds(pl.multiple_of(b * 128, 128), 128)
        for j in range(2):
            spots[j, at, :] = jnp.broadcast_to(pos_ref[j : j + 1, at], (128, 128)).T
            gates[j, at, :] = jnp.broadcast_to(gate_ref[j : j + 1, at], (128, 128)).T
            acc[j, at, :] = jnp.zeros((128, dim), BF16)

    def experts(got, first, last, done):
        lanes = (last - first) * WIN

        @pl.loop(0, local // 4)
        def _(quad):
            @pl.loop(0, 2)
            def _(twin):
                pair = quad * 2 + twin
                for k in range(2):
                    e = pair * 2 + k
                    for step in range(first, last):
                        row = (step - first) * full_blocks + start_ref[e, step]
                        for half in range(WIN // ALIGN):
                            at = (step - first) * WIN + half * ALIGN
                            win[k, at : at + ALIGN, :] = got[row + half]
                for k in range(2):
                    e = pair * 2 + k
                    visit = done + e
                    place = lax.rem(visit, depth)
                    for copy in fetch(visit):
                        copy.wait()
                    slot = slot_ref[pl.ds(e, 1), :][:, first * WIN : last * WIN]
                    hot = jnp.where(iota((128, lanes), 0) == slot, 1.0, 0.0).astype(BF16)
                    x = jnp.dot(hot, win[k, :lanes, :], preferred_element_type=F32).astype(BF16)
                    h = jax.nn.gelu(jnp.dot(x, w_in[place], preferred_element_type=F32)).astype(BF16)
                    o = jnp.dot(h, w_out[place], preferred_element_type=F32).astype(BF16)
                    obuf[pl.ds(pl.multiple_of(twin * 256 + k * 128, 128), 128), :] = o
                for k in range(2):
                    visit = done + pair * 2 + k + depth

                    @pl.when(visit < 2 * local)
                    def _():
                        for copy in fetch(visit):
                            copy.start()

            part = 0 if first == 0 else 1
            goal = jnp.concatenate([place_ref[part, pl.ds(quad * 4 + k, 1), :] for k in range(4)], axis=1)

            @pl.loop(first, last)
            def _(step):
                hot = jnp.where(iota((full, 512), 0) == goal - step * stride, 1.0, 0.0).astype(BF16)
                outs[step] += jnp.dot(hot, obuf[...], preferred_element_type=F32).astype(BF16)

    def send_back(first, last):
        @pl.loop(first, last)
        def _(step):
            pass_over(step).start()

        @pl.loop(first, last)
        def _(step):
            pass_in(step).wait_recv()
            outs[step, cap:, :] += tails[step]

            @pl.when(step > 0)
            def _():
                give(step).start()

    def chip_base(step):
        return peer(me, step, groups) // 2 * (2 * stride)

    def picked(at, returned, lines):
        lane = iota((TOKEN_BLOCK, 128), 1)
        for j in range(2):
            line = lines(spots[j, at, :])
            hot = jnp.concatenate([jnp.where(line - k == lane, 1.0, 0.0).astype(BF16) for k in range(0, 2 * cap, 128)], axis=1)
            yield j, acc[j, at, :] + jnp.dot(hot[:, : 2 * cap], returned, preferred_element_type=F32).astype(BF16)

    def add(first, lines, finish):
        returned = ret[pl.ds(first, 2)].reshape(2 * cap, dim)

        @pl.loop(0, token_blocks)
        def _(b):
            at = pl.ds(pl.multiple_of(b * TOKEN_BLOCK, TOKEN_BLOCK), TOKEN_BLOCK)
            sums = [value for _, value in picked(at, returned, lines)]
            if not finish:
                for j in range(2):
                    acc[j, at, :] = sums[j]
                return
            for c in range(0, dim, 128):
                mixed = x_ref[at, c : c + 128].astype(F32) + gates[0, at, :] * sums[0][:, c : c + 128].astype(F32)
                out_ref[at, c : c + 128] = (mixed + gates[1, at, :] * sums[1][:, c : c + 128].astype(F32)).astype(BF16)

    mine.wait()
    tail_over(0, got_a, 0).start()

    @pl.loop(1, near)
    def _(step):
        push(step, got_a, 0).wait_recv()
        tail_over(step, got_a, 0).start()

    @pl.loop(0, near)
    def _(step):
        tail_in(step, got_a, 0).wait_recv()

    experts(got_a, 0, near, 0)
    send_back(0, near)
    back = pltpu.make_async_copy(outs.at[0, pl.ds(TAIL, cap)], ret.at[0], own_sem.at[1])
    back.start()

    @pl.loop(near, groups)
    def _(step):
        push(step, got_b, near).wait_recv()
        tail_over(step, got_b, near).start()

    @pl.loop(near, groups)
    def _(step):
        tail_in(step, got_b, near).wait_recv()

    experts(got_b, near, groups, local)
    send_back(near, groups)
    back.wait()

    @pl.loop(0, groups // 2 - 2)
    def _(half):
        @pl.when(half > 0)
        def _():
            give(half * 2).wait_recv()

        give(half * 2 + 1).wait_recv()
        base = chip_base(half * 2)
        add(half * 2, lambda spot: spot - base, False)

    for core in range(2):
        steps = [groups - 4 + core, groups - 2 + core]
        for step in steps:
            give(step).wait_recv()
        bases = [chip_base(step) + core * cap for step in steps]

        def lines(spot):
            near_by, other = spot - bases[0], spot - bases[1]
            other = jnp.where((other >= 0) & (other < cap), other + cap, -1)
            return jnp.where((near_by >= 0) & (near_by < cap), near_by, other)

        add(groups - 4 + 2 * core, lines, core == 1)

    @pl.loop(1, near)
    def _(step):
        push(step, got_a, 0).wait_send()

    @pl.loop(near, groups)
    def _(step):
        push(step, got_b, near).wait_send()

    @pl.loop(0, near)
    def _(step):
        tail_over(step, got_a, 0).wait_send()

    @pl.loop(near, groups)
    def _(step):
        tail_over(step, got_b, near).wait_send()

    @pl.loop(0, groups)
    def _(step):
        pass_over(step).wait_send()

    @pl.loop(1, groups)
    def _(step):
        give(step).wait_send()


def solution(mesh):
    groups = mesh.shape["expert"]
    row_spec = P(("data", "expert"), None)
    weight_spec = P("expert", None, None)

    def device_step(token_rows, expert_ids, gate_weights, w_in, w_out):
        tokens, top_k = expert_ids.shape
        local, dim, hidden = w_in.shape
        experts = local * groups
        mean_load = tokens * top_k // experts
        capacity = groups * mean_load
        worst = local * (7 * mean_load // 4)
        usual = local * mean_load * 9 // 8
        stride = 2 * local * mean_load
        lanes = groups * WIN
        near = groups // 2
        depth = 4
        vmem = pl.BlockSpec(memory_space=VMEM)
        anywhere = pl.BlockSpec(memory_space=pl.ANY)

        def params(collective_id):
            return pltpu.CompilerParams(collective_id=collective_id, has_side_effects=True, vmem_limit_bytes=61 * 1024 * 1024)

        pair_sems = [pltpu.SemaphoreType.DMA((groups,)), pltpu.SemaphoreType.DMA((groups,))]
        pos, slot, start, place, fits = pl.pallas_call(
            functools.partial(route_kernel, groups, capacity, usual, worst, stride, local, near),
            out_shape=[
                jax.ShapeDtypeStruct((top_k, tokens), I32),
                jax.ShapeDtypeStruct((local, lanes), I32),
                jax.ShapeDtypeStruct((local, groups), I32),
                jax.ShapeDtypeStruct((2, local, capacity), I32),
                jax.ShapeDtypeStruct((1, 1), I32),
            ],
            in_specs=[vmem],
            out_specs=[vmem] * 5,
            scratch_shapes=[
                VMEM((groups, top_k, experts), F32),
                VMEM((top_k, experts, 128), F32),
                VMEM((top_k, tokens), F32),
                VMEM((4, groups, experts), F32),
            ]
            + pair_sems,
            compiler_params=params(0),
            name="route",
        )(expert_ids.T)

        def exchange(cap, collective_id):
            def run():
                return pl.pallas_call(
                    functools.partial(moe_kernel, groups, cap, stride, local, near),
                    out_shape=jax.ShapeDtypeStruct((tokens, dim), BF16),
                    in_specs=[pl.BlockSpec(memory_space=pltpu.SMEM)] + [vmem] * 4 + [anywhere] * 3,
                    out_specs=vmem,
                    scratch_shapes=[
                        VMEM((tokens, dim), BF16),
                        VMEM((groups, cap // ALIGN, ALIGN, dim), BF16),
                        VMEM(((near * (cap + TAIL) + WIN) // ALIGN, ALIGN, dim), BF16),
                        VMEM((((groups - near) * (cap + TAIL) + WIN) // ALIGN, ALIGN, dim), BF16),
                        VMEM((groups, cap + TAIL, dim), BF16),
                        VMEM((groups, TAIL, dim), BF16),
                        VMEM((groups, cap, dim), BF16),
                        VMEM((depth, dim, hidden), BF16),
                        VMEM((depth, hidden, dim), BF16),
                        VMEM((2, near * WIN, dim), BF16),
                        VMEM((4 * capacity, dim), BF16),
                        VMEM((top_k, tokens, 128), I32),
                        VMEM((top_k, tokens, 128), F32),
                        VMEM((top_k, tokens, dim), BF16),
                        pltpu.SemaphoreType.DMA((2, depth)),
                    ]
                    + pair_sems * 4
                    + [pltpu.SemaphoreType.DMA((3,))],
                    compiler_params=params(collective_id),
                    name="experts",
                )(start, slot, place, pos, gate_weights.T, token_rows, w_in, w_out)

            return run

        return lax.cond(fits.reshape(()) > 0, exchange(usual, 1), exchange(worst, 2))

    return jax.shard_map(device_step, mesh=mesh, in_specs=(row_spec, row_spec, row_spec, weight_spec, weight_spec), out_specs=row_spec, check_vma=False)
```

```python
import functools

import jax
import jax.numpy as jnp
from jax import lax
from jax.experimental import pallas as pl
from jax.experimental.pallas import tpu as pltpu
from jax.sharding import PartitionSpec as P

MESH = pl.DeviceIdType.MESH
VMEM = pltpu.VMEM
F32, BF16, I32 = jnp.float32, jnp.bfloat16, jnp.int32
WIN = 32
ALIGN = 16
TAIL = 48
TOKEN_BLOCK = 256


def iota(shape, dim):
    return lax.broadcasted_iota(I32, shape, dim)


def chips_away(step, chips):
    half = step // 2
    return lax.rem(2 * half + 3 * (half // (chips // 2)), chips)


def peer(me, step, groups):
    chips = groups // 2
    chip = lax.rem(me // 2 + chips_away(step, chips), chips)
    return chip * 2 + lax.rem(me + step, 2)


def source_of(me, step, groups):
    chips = groups // 2
    chip = lax.rem(me // 2 - chips_away(step, chips) + chips, chips)
    return chip * 2 + lax.rem(me + step, 2)


def announce(me, groups):
    barrier = pltpu.get_barrier_semaphore()

    @pl.loop(1, groups)
    def _(step):
        pl.semaphore_signal(barrier, inc=1, device_id={"expert": lax.rem(me + step, groups)}, device_id_type=MESH)

    return barrier


def route_kernel(groups, capacity, sizes, stride, local, near, ids_ref, pos_ref, slot_ref, start_ref, place_ref, rung_ref, cnt, carry, rank, rows, send_sem, recv_sem):
    me = lax.axis_index("expert")
    tokens = ids_ref.shape[1]
    experts = local * groups
    blocks = tokens // TOKEN_BLOCK
    barrier = announce(me, groups)

    expert_rows = iota((experts, TOKEN_BLOCK), 0)
    upper = (iota((TOKEN_BLOCK, TOKEN_BLOCK), 0) <= iota((TOKEN_BLOCK, TOKEN_BLOCK), 1)).astype(BF16)
    carry[...] = jnp.zeros_like(carry)

    @pl.loop(0, blocks)
    def _(b):
        cols = pl.ds(pl.multiple_of(b * TOKEN_BLOCK, TOKEN_BLOCK), TOKEN_BLOCK)
        for j in range(2):
            hot = expert_rows == ids_ref[j : j + 1, cols]
            run = jnp.dot(jnp.where(hot, 1.0, 0.0).astype(BF16), upper, preferred_element_type=F32)
            run = run + jnp.concatenate([carry[j]] * (TOKEN_BLOCK // 128), axis=1)
            rank[j : j + 1, cols] = jnp.sum(jnp.where(hot, run, 0.0), axis=0, keepdims=True) - 1.0
            carry[j] = jnp.broadcast_to(run[:, TOKEN_BLOCK - 1 :], (experts, 128))

    for j in range(2):
        row = jnp.concatenate([carry[j, k : k + 128, :].T[:1] for k in range(0, experts, 128)], axis=1)
        cnt[me, j : j + 1, :] = row

    def send(step):
        to = lax.rem(me + step, groups)
        return pltpu.make_async_remote_copy(src_ref=cnt.at[me], dst_ref=cnt.at[me], send_sem=send_sem.at[step], recv_sem=recv_sem.at[step], device_id={"expert": to}, device_id_type=MESH)

    def arrive(step):
        origin = lax.rem(me - step + groups, groups)
        return pltpu.make_async_remote_copy(src_ref=cnt.at[origin], dst_ref=cnt.at[origin], send_sem=send_sem.at[step], recv_sem=recv_sem.at[step], device_id={"expert": origin}, device_id_type=MESH)

    pl.semaphore_wait(barrier, groups - 1)

    @pl.loop(1, groups)
    def _(step):
        send(step).start()

    @pl.loop(1, groups)
    def _(step):
        arrive(step).wait_recv()

    @pl.loop(1, groups)
    def _(step):
        send(step).wait_send()

    first, second = cnt[:, 0, :], cnt[:, 1, :]
    earlier = (iota((groups, groups), 1) < iota((groups, groups), 0)).astype(BF16)
    before0 = jnp.dot(earlier, first.astype(BF16), preferred_element_type=F32)
    before1 = jnp.dot(earlier, second.astype(BF16), preferred_element_type=F32)
    total0 = jnp.sum(first, axis=0, keepdims=True)
    keep0 = jnp.clip(capacity - before0, 0.0, first)
    keep1 = jnp.clip(capacity - total0 - before1, 0.0, second)
    keep = keep0 + keep1
    keep16 = keep.astype(BF16)
    er, ec = iota((experts, experts), 0), iota((experts, experts), 1)
    mate = er // local - ec // local + 2 * (ec // local % 2)
    same = er // local == ec // local
    load = jnp.dot(keep16, same.astype(BF16), preferred_element_type=F32)
    mate_load = jnp.dot(keep16, (mate == 1).astype(BF16), preferred_element_type=F32)
    inside = jnp.dot(keep16, (same & (er < ec)).astype(BF16), preferred_element_type=F32)
    rung = jnp.zeros((1, 1), F32)
    over = jnp.zeros_like(load)
    size = jnp.full((1, 1), float(sizes[-1]), F32)
    for cap in reversed(sizes[:-1]):
        spill = jnp.maximum(load - cap, 0.0)
        bad = (spill > TAIL) | ((spill > 0.0) & (mate_load + spill > cap))
        good = jnp.max(jnp.max(jnp.where(bad, 1.0, 0.0), axis=1, keepdims=True), axis=0, keepdims=True) == 0.0
        over = jnp.where(good, spill, over)
        size = jnp.where(good, float(cap), size)
        rung = jnp.where(good, rung, rung + 1.0)
    rung_ref[...] = rung.astype(I32)
    offset = TAIL - over + inside
    high = jnp.floor(offset * (1.0 / ALIGN))
    low = offset - high * ALIGN

    rows[0], rows[1], rows[2], rows[3] = high, low, keep0, keep1
    table = jnp.concatenate([rows[i, pl.ds(me, 1), :] for i in range(4)] + [jnp.zeros((4, experts), F32)], axis=0).astype(BF16)
    side = lax.rem(me, 2)

    @pl.loop(0, blocks)
    def _(b):
        cols = pl.ds(pl.multiple_of(b * TOKEN_BLOCK, TOKEN_BLOCK), TOKEN_BLOCK)
        for j in range(2):
            ids = ids_ref[j : j + 1, cols]
            hot16 = jnp.where(expert_rows == ids, 1.0, 0.0).astype(BF16)
            found = jnp.dot(table, hot16, preferred_element_type=F32)
            rk = rank[j : j + 1, cols]
            spot = found[0:1] * ALIGN + found[1:2] + rk
            if j == 1:
                spot = spot + found[2:3]
            owner = ids // local
            half = ((owner + side) % 2).astype(F32)
            direct = spot >= TAIL
            row = jnp.where(direct, half * size + spot - TAIL, (2.0 - half) * size + spot - TAIL)
            key = row.astype(I32) + (owner // 2) * (2 * stride)
            pos_ref[j : j + 1, cols] = jnp.where(rk < found[2 + j : 3 + j], key, -1)

    mine = (iota((local, experts), 1) == iota((local, experts), 0) + me * local).astype(BF16)

    def pick(values):
        return lax.dot_general(mine, values.astype(BF16), (((1,), (1,)), ((), ())), preferred_element_type=F32)

    from_step = (source_of(me, iota((groups, groups), 0), groups) == iota((groups, groups), 1)).astype(BF16)
    older, newer = iota((groups, groups), 1), iota((groups, groups), 0)
    ahead_of = ((older < newer) & ((older < near) == (newer < near))).astype(BF16)

    def by_step(values):
        return jnp.dot(from_step, values.astype(BF16), preferred_element_type=F32)

    kept = by_step(keep)
    ahead = pick(jnp.dot(ahead_of, kept.astype(BF16), preferred_element_type=F32))
    high, low, kept = pick(by_step(high)), pick(by_step(low)), pick(kept)
    start_ref[...] = high.astype(I32)
    lanes = groups * WIN
    spread = (iota((groups, lanes), 1) // WIN == iota((groups, lanes), 0)).astype(BF16)

    def widen(values):
        return jnp.dot(values.astype(BF16), spread, preferred_element_type=F32)

    wide_low, wide_kept, wide_ahead = widen(low), widen(kept), widen(ahead)
    lane = (iota((local, lanes), 1) % WIN).astype(F32)
    valid = (lane >= wide_low) & (lane < wide_low + wide_kept)
    slot_ref[...] = jnp.where(valid, wide_ahead + lane - wide_low, -1.0).astype(I32)
    seat = iota((local, capacity), 1).astype(F32)
    goals = [jnp.full((local, capacity), -1.0, F32) for _ in range(2)]
    for step in range(groups):
        begin, count = ahead[:, step : step + 1], kept[:, step : step + 1]
        spot = high[:, step : step + 1] * ALIGN + low[:, step : step + 1] + step * stride
        part = int(step >= near)
        goals[part] = jnp.where((seat >= begin) & (seat < begin + count), seat - begin + spot, goals[part])
    for part in range(2):
        place_ref[part] = goals[part].astype(I32)


def moe_kernel(groups, cap, stride, local, near, start_ref, slot_ref, place_ref, pos_ref, gate_ref, x_hbm, w_in_hbm, w_out_hbm, out_ref, x_ref, buf, got_a, got_b, outs, tails, ret, w_in, w_out, win, obuf, spots, gates, acc, w_sem, send_sem, recv_sem, back_send, back_recv, tail_send, tail_recv, pass_send, pass_recv, own_sem):
    me = lax.axis_index("expert")
    tokens, dim = x_ref.shape
    depth = w_in.shape[0]
    x_copy = pltpu.make_async_copy(x_hbm, x_ref, own_sem.at[2])
    x_copy.start()
    full = cap + TAIL
    full_blocks, cap_blocks, tail_blocks = full // ALIGN, cap // ALIGN, TAIL // ALIGN
    token_blocks = tokens // TOKEN_BLOCK
    sibling = {"expert": me + 1 - 2 * lax.rem(me, 2)}
    barrier = announce(me, groups)

    def fetch(visit):
        e, place = lax.rem(visit, local), lax.rem(visit, depth)
        return (
            pltpu.make_async_copy(w_in_hbm.at[e], w_in.at[place], w_sem.at[0, place]),
            pltpu.make_async_copy(w_out_hbm.at[e], w_out.at[place], w_sem.at[1, place]),
        )

    for visit in range(depth):
        for copy in fetch(visit):
            copy.start()

    def mate_of(step):
        return step + 1 - 2 * lax.rem(step, 2)

    def push(step, got, first):
        return pltpu.make_async_remote_copy(src_ref=buf.at[step], dst_ref=got.at[pl.ds((step - first) * full_blocks + tail_blocks, cap_blocks)], send_sem=send_sem.at[step], recv_sem=recv_sem.at[step], device_id={"expert": peer(me, step, groups)}, device_id_type=MESH)

    def tail_over(step, got, first):
        return pltpu.make_async_remote_copy(src_ref=got.at[pl.ds((step - first) * full_blocks + cap_blocks, tail_blocks)], dst_ref=got.at[pl.ds((mate_of(step) - first) * full_blocks, tail_blocks)], send_sem=tail_send.at[step], recv_sem=tail_recv.at[mate_of(step)], device_id=sibling, device_id_type=MESH)

    def tail_in(step, got, first):
        return pltpu.make_async_remote_copy(src_ref=got.at[pl.ds((mate_of(step) - first) * full_blocks + cap_blocks, tail_blocks)], dst_ref=got.at[pl.ds((step - first) * full_blocks, tail_blocks)], send_sem=tail_send.at[mate_of(step)], recv_sem=tail_recv.at[step], device_id=sibling, device_id_type=MESH)

    def pass_over(step):
        return pltpu.make_async_remote_copy(src_ref=outs.at[step, pl.ds(0, TAIL)], dst_ref=tails.at[mate_of(step)], send_sem=pass_send.at[step], recv_sem=pass_recv.at[mate_of(step)], device_id=sibling, device_id_type=MESH)

    def pass_in(step):
        return pltpu.make_async_remote_copy(src_ref=outs.at[mate_of(step), pl.ds(0, TAIL)], dst_ref=tails.at[step], send_sem=pass_send.at[mate_of(step)], recv_sem=pass_recv.at[step], device_id=sibling, device_id_type=MESH)

    def berth(step):
        rest = step - (groups - 4)
        return step + step // (groups - 4) * (rest % 2 * 2 + rest // 2 - rest)

    def give(step):
        return pltpu.make_async_remote_copy(src_ref=outs.at[step, pl.ds(TAIL, cap)], dst_ref=ret.at[berth(step)], send_sem=back_send.at[step], recv_sem=back_recv.at[step], device_id={"expert": source_of(me, step, groups)}, device_id_type=MESH)

    def pack(step):
        base = peer(me, step, groups) // 2 * (2 * stride) + lax.rem(step, 2) * cap
        spot = pos_ref[...] - base
        line = iota((cap, tokens), 0)
        hot = (line == spot[0:1]) | (line == spot[1:2])
        rows = jnp.dot(jnp.where(hot, 1.0, 0.0).astype(BF16), x_ref[...], preferred_element_type=F32).astype(BF16)
        buf[step] = rows.reshape(cap_blocks, ALIGN, dim)

    def turn(index):
        start = 1 - (index + groups - 4) // groups
        later = (index + groups - 6) // groups
        last = (index + 2) // groups
        return index + start * (2 + index % 2 * 4 + index // 2 - index) + 2 * later - groups * last

    x_copy.wait()
    pack(2)
    pl.semaphore_wait(barrier, groups - 1)
    push(2, got_a, 0).start()

    @pl.loop(1, groups)
    def _(index):
        step = turn(index)
        pack(step)

        @pl.when((step > 0) & (step < near))
        def _():
            push(step, got_a, 0).start()

        @pl.when(step >= near)
        def _():
            push(step, got_b, near).start()

    mine = pltpu.make_async_copy(buf.at[0], got_a.at[pl.ds(tail_blocks, cap_blocks)], own_sem.at[0])
    mine.start()
    pad = WIN // ALIGN
    got_a[pl.ds(near * full_blocks, pad)] = jnp.zeros((pad, ALIGN, dim), BF16)
    got_b[pl.ds((groups - near) * full_blocks, pad)] = jnp.zeros((pad, ALIGN, dim), BF16)

    @pl.loop(0, groups)
    def _(step):
        outs[step] = jnp.zeros((full, dim), BF16)

    @pl.loop(0, tokens // 128)
    def _(b):
        at = pl.ds(pl.multiple_of(b * 128, 128), 128)
        for j in range(2):
            spots[j, at, :] = jnp.broadcast_to(pos_ref[j : j + 1, at], (128, 128)).T
            gates[j, at, :] = jnp.broadcast_to(gate_ref[j : j + 1, at], (128, 128)).T
            acc[j, at, :] = jnp.zeros((128, dim), BF16)

    def experts(got, first, last, done):
        lanes = (last - first) * WIN

        @pl.loop(0, local // 4)
        def _(quad):
            @pl.loop(0, 2)
            def _(twin):
                pair = quad * 2 + twin
                for k in range(2):
                    e = pair * 2 + k
                    for step in range(first, last):
                        row = (step - first) * full_blocks + start_ref[e, step]
                        for half in range(WIN // ALIGN):
                            at = (step - first) * WIN + half * ALIGN
                            win[k, at : at + ALIGN, :] = got[row + half]
                for k in range(2):
                    e = pair * 2 + k
                    visit = done + e
                    place = lax.rem(visit, depth)
                    for copy in fetch(visit):
                        copy.wait()
                    slot = slot_ref[pl.ds(e, 1), :][:, first * WIN : last * WIN]
                    hot = jnp.where(iota((128, lanes), 0) == slot, 1.0, 0.0).astype(BF16)
                    x = jnp.dot(hot, win[k, :lanes, :], preferred_element_type=F32).astype(BF16)
                    h = jax.nn.gelu(jnp.dot(x, w_in[place], preferred_element_type=F32)).astype(BF16)
                    o = jnp.dot(h, w_out[place], preferred_element_type=F32).astype(BF16)
                    obuf[pl.ds(pl.multiple_of(twin * 256 + k * 128, 128), 128), :] = o
                for k in range(2):
                    visit = done + pair * 2 + k + depth

                    @pl.when(visit < 2 * local)
                    def _():
                        for copy in fetch(visit):
                            copy.start()

            part = 0 if first == 0 else 1
            goal = jnp.concatenate([place_ref[part, pl.ds(quad * 4 + k, 1), :] for k in range(4)], axis=1)

            @pl.loop(first, last)
            def _(step):
                hot = jnp.where(iota((full, 512), 0) == goal - step * stride, 1.0, 0.0).astype(BF16)
                outs[step] += jnp.dot(hot, obuf[...], preferred_element_type=F32).astype(BF16)

    def send_back(first, last):
        @pl.loop(first, last)
        def _(step):
            pass_over(step).start()

        @pl.loop(first, last)
        def _(step):
            pass_in(step).wait_recv()
            outs[step, cap:, :] += tails[step]

            @pl.when(step > 0)
            def _():
                give(step).start()

    def chip_base(step):
        return peer(me, step, groups) // 2 * (2 * stride)

    def picked(at, returned, lines):
        lane = iota((TOKEN_BLOCK, 128), 1)
        for j in range(2):
            line = lines(spots[j, at, :])
            hot = jnp.concatenate([jnp.where(line - k == lane, 1.0, 0.0).astype(BF16) for k in range(0, 2 * cap, 128)], axis=1)
            yield j, acc[j, at, :] + jnp.dot(hot[:, : 2 * cap], returned, preferred_element_type=F32).astype(BF16)

    def add(first, lines, finish):
        returned = ret[pl.ds(first, 2)].reshape(2 * cap, dim)

        @pl.loop(0, token_blocks)
        def _(b):
            at = pl.ds(pl.multiple_of(b * TOKEN_BLOCK, TOKEN_BLOCK), TOKEN_BLOCK)
            sums = [value for _, value in picked(at, returned, lines)]
            if not finish:
                for j in range(2):
                    acc[j, at, :] = sums[j]
                return
            for c in range(0, dim, 128):
                mixed = x_ref[at, c : c + 128].astype(F32) + gates[0, at, :] * sums[0][:, c : c + 128].astype(F32)
                out_ref[at, c : c + 128] = (mixed + gates[1, at, :] * sums[1][:, c : c + 128].astype(F32)).astype(BF16)

    mine.wait()
    tail_over(0, got_a, 0).start()

    @pl.loop(1, near)
    def _(step):
        push(step, got_a, 0).wait_recv()
        tail_over(step, got_a, 0).start()

    @pl.loop(0, near)
    def _(step):
        tail_in(step, got_a, 0).wait_recv()

    experts(got_a, 0, near, 0)
    send_back(0, near)
    back = pltpu.make_async_copy(outs.at[0, pl.ds(TAIL, cap)], ret.at[0], own_sem.at[1])
    back.start()

    @pl.loop(near, groups)
    def _(step):
        push(step, got_b, near).wait_recv()
        tail_over(step, got_b, near).start()

    @pl.loop(near, groups)
    def _(step):
        tail_in(step, got_b, near).wait_recv()

    experts(got_b, near, groups, local)
    send_back(near, groups)
    back.wait()

    @pl.loop(0, groups // 2 - 2)
    def _(half):
        @pl.when(half > 0)
        def _():
            give(half * 2).wait_recv()

        give(half * 2 + 1).wait_recv()
        base = chip_base(half * 2)
        add(half * 2, lambda spot: spot - base, False)

    for core in range(2):
        steps = [groups - 4 + core, groups - 2 + core]
        for step in steps:
            give(step).wait_recv()
        bases = [chip_base(step) + core * cap for step in steps]

        def lines(spot):
            near_by, other = spot - bases[0], spot - bases[1]
            other = jnp.where((other >= 0) & (other < cap), other + cap, -1)
            return jnp.where((near_by >= 0) & (near_by < cap), near_by, other)

        add(groups - 4 + 2 * core, lines, core == 1)

    @pl.loop(1, near)
    def _(step):
        push(step, got_a, 0).wait_send()

    @pl.loop(near, groups)
    def _(step):
        push(step, got_b, near).wait_send()

    @pl.loop(0, near)
    def _(step):
        tail_over(step, got_a, 0).wait_send()

    @pl.loop(near, groups)
    def _(step):
        tail_over(step, got_b, near).wait_send()

    @pl.loop(0, groups)
    def _(step):
        pass_over(step).wait_send()

    @pl.loop(1, groups)
    def _(step):
        give(step).wait_send()


def solution(mesh):
    groups = mesh.shape["expert"]
    row_spec = P(("data", "expert"), None)
    weight_spec = P("expert", None, None)

    def device_step(token_rows, expert_ids, gate_weights, w_in, w_out):
        tokens, top_k = expert_ids.shape
        local, dim, hidden = w_in.shape
        experts = local * groups
        mean_load = tokens * top_k // experts
        capacity = groups * mean_load
        worst = local * (7 * mean_load // 4)
        sizes = [local * mean_load * 18 // 16, local * mean_load * 19 // 16, worst]
        stride = 2 * local * mean_load
        lanes = groups * WIN
        near = groups // 2
        depth = 4
        vmem = pl.BlockSpec(memory_space=VMEM)
        anywhere = pl.BlockSpec(memory_space=pl.ANY)

        def params(collective_id):
            return pltpu.CompilerParams(collective_id=collective_id, has_side_effects=True, vmem_limit_bytes=61 * 1024 * 1024)

        pair_sems = [pltpu.SemaphoreType.DMA((groups,)), pltpu.SemaphoreType.DMA((groups,))]
        pos, slot, start, place, rung = pl.pallas_call(
            functools.partial(route_kernel, groups, capacity, sizes, stride, local, near),
            out_shape=[
                jax.ShapeDtypeStruct((top_k, tokens), I32),
                jax.ShapeDtypeStruct((local, lanes), I32),
                jax.ShapeDtypeStruct((local, groups), I32),
                jax.ShapeDtypeStruct((2, local, capacity), I32),
                jax.ShapeDtypeStruct((1, 1), I32),
            ],
            in_specs=[vmem],
            out_specs=[vmem] * 5,
            scratch_shapes=[
                VMEM((groups, top_k, experts), F32),
                VMEM((top_k, experts, 128), F32),
                VMEM((top_k, tokens), F32),
                VMEM((4, groups, experts), F32),
            ]
            + pair_sems,
            compiler_params=params(0),
            name="route",
        )(expert_ids.T)

        def exchange(cap, collective_id):
            def run():
                return pl.pallas_call(
                    functools.partial(moe_kernel, groups, cap, stride, local, near),
                    out_shape=jax.ShapeDtypeStruct((tokens, dim), BF16),
                    in_specs=[pl.BlockSpec(memory_space=pltpu.SMEM)] + [vmem] * 4 + [anywhere] * 3,
                    out_specs=vmem,
                    scratch_shapes=[
                        VMEM((tokens, dim), BF16),
                        VMEM((groups, cap // ALIGN, ALIGN, dim), BF16),
                        VMEM(((near * (cap + TAIL) + WIN) // ALIGN, ALIGN, dim), BF16),
                        VMEM((((groups - near) * (cap + TAIL) + WIN) // ALIGN, ALIGN, dim), BF16),
                        VMEM((groups, cap + TAIL, dim), BF16),
                        VMEM((groups, TAIL, dim), BF16),
                        VMEM((groups, cap, dim), BF16),
                        VMEM((depth, dim, hidden), BF16),
                        VMEM((depth, hidden, dim), BF16),
                        VMEM((2, near * WIN, dim), BF16),
                        VMEM((4 * capacity, dim), BF16),
                        VMEM((top_k, tokens, 128), I32),
                        VMEM((top_k, tokens, 128), F32),
                        VMEM((top_k, tokens, dim), BF16),
                        pltpu.SemaphoreType.DMA((2, depth)),
                    ]
                    + pair_sems * 4
                    + [pltpu.SemaphoreType.DMA((3,))],
                    compiler_params=params(collective_id),
                    name="experts",
                )(start, slot, place, pos, gate_weights.T, token_rows, w_in, w_out)

            return run

        return lax.switch(rung.reshape(()), [exchange(cap, 1 + i) for i, cap in enumerate(sizes)])

    return jax.shard_map(device_step, mesh=mesh, in_specs=(row_spec, row_spec, row_spec, weight_spec, weight_spec), out_specs=row_spec, check_vma=False)
```

```python
import functools

import jax
import jax.numpy as jnp
from jax import lax
from jax.experimental import pallas as pl
from jax.experimental.pallas import tpu as pltpu
from jax.sharding import PartitionSpec as P

MESH = pl.DeviceIdType.MESH
VMEM = pltpu.VMEM
F32, BF16, I32 = jnp.float32, jnp.bfloat16, jnp.int32
WIN = 32
ALIGN = 16
TAIL = 48
TOKEN_BLOCK = 256


def iota(shape, dim):
    return lax.broadcasted_iota(I32, shape, dim)


def chips_away(step, chips):
    half = step // 2
    return lax.rem(2 * half + 3 * (half // (chips // 2)), chips)


def peer(me, step, groups):
    chips = groups // 2
    chip = lax.rem(me // 2 + chips_away(step, chips), chips)
    return chip * 2 + lax.rem(me + step, 2)


def source_of(me, step, groups):
    chips = groups // 2
    chip = lax.rem(me // 2 - chips_away(step, chips) + chips, chips)
    return chip * 2 + lax.rem(me + step, 2)


def announce(me, groups):
    barrier = pltpu.get_barrier_semaphore()

    @pl.loop(1, groups)
    def _(step):
        pl.semaphore_signal(barrier, inc=1, device_id={"expert": lax.rem(me + step, groups)}, device_id_type=MESH)

    return barrier


def route_kernel(groups, capacity, sizes, stride, local, near, ids_ref, pos_ref, slot_ref, start_ref, place_ref, rung_ref, cnt, carry, rank, rows, send_sem, recv_sem):
    me = lax.axis_index("expert")
    tokens = ids_ref.shape[1]
    experts = local * groups
    blocks = tokens // TOKEN_BLOCK
    barrier = announce(me, groups)

    expert_rows = iota((experts, TOKEN_BLOCK), 0)
    upper = (iota((TOKEN_BLOCK, TOKEN_BLOCK), 0) <= iota((TOKEN_BLOCK, TOKEN_BLOCK), 1)).astype(BF16)
    carry[...] = jnp.zeros_like(carry)

    @pl.loop(0, blocks)
    def _(b):
        cols = pl.ds(pl.multiple_of(b * TOKEN_BLOCK, TOKEN_BLOCK), TOKEN_BLOCK)
        for j in range(2):
            hot = expert_rows == ids_ref[j : j + 1, cols]
            run = jnp.dot(jnp.where(hot, 1.0, 0.0).astype(BF16), upper, preferred_element_type=F32)
            run = run + jnp.concatenate([carry[j]] * (TOKEN_BLOCK // 128), axis=1)
            rank[j : j + 1, cols] = jnp.sum(jnp.where(hot, run, 0.0), axis=0, keepdims=True) - 1.0
            carry[j] = jnp.broadcast_to(run[:, TOKEN_BLOCK - 1 :], (experts, 128))

    for j in range(2):
        row = jnp.concatenate([carry[j, k : k + 128, :].T[:1] for k in range(0, experts, 128)], axis=1)
        cnt[me, j : j + 1, :] = row

    def send(step):
        to = lax.rem(me + step, groups)
        return pltpu.make_async_remote_copy(src_ref=cnt.at[me], dst_ref=cnt.at[me], send_sem=send_sem.at[step], recv_sem=recv_sem.at[step], device_id={"expert": to}, device_id_type=MESH)

    def arrive(step):
        origin = lax.rem(me - step + groups, groups)
        return pltpu.make_async_remote_copy(src_ref=cnt.at[origin], dst_ref=cnt.at[origin], send_sem=send_sem.at[step], recv_sem=recv_sem.at[step], device_id={"expert": origin}, device_id_type=MESH)

    pl.semaphore_wait(barrier, groups - 1)

    @pl.loop(1, groups)
    def _(step):
        send(step).start()

    @pl.loop(1, groups)
    def _(step):
        arrive(step).wait_recv()

    @pl.loop(1, groups)
    def _(step):
        send(step).wait_send()

    first, second = cnt[:, 0, :], cnt[:, 1, :]
    earlier = (iota((groups, groups), 1) < iota((groups, groups), 0)).astype(BF16)
    before0 = jnp.dot(earlier, first.astype(BF16), preferred_element_type=F32)
    before1 = jnp.dot(earlier, second.astype(BF16), preferred_element_type=F32)
    total0 = jnp.sum(first, axis=0, keepdims=True)
    keep0 = jnp.clip(capacity - before0, 0.0, first)
    keep1 = jnp.clip(capacity - total0 - before1, 0.0, second)
    keep = keep0 + keep1
    keep16 = keep.astype(BF16)
    er, ec = iota((experts, experts), 0), iota((experts, experts), 1)
    mate = er // local - ec // local + 2 * (ec // local % 2)
    same = er // local == ec // local
    load = jnp.dot(keep16, same.astype(BF16), preferred_element_type=F32)
    mate_load = jnp.dot(keep16, (mate == 1).astype(BF16), preferred_element_type=F32)
    inside = jnp.dot(keep16, (same & (er < ec)).astype(BF16), preferred_element_type=F32)
    rung = jnp.zeros((1, 1), F32)
    over = jnp.zeros_like(load)
    size = jnp.full((1, 1), float(sizes[-1]), F32)
    for cap in reversed(sizes[:-1]):
        spill = jnp.maximum(load - cap, 0.0)
        bad = (spill > TAIL) | ((spill > 0.0) & (mate_load + spill > cap))
        good = jnp.max(jnp.max(jnp.where(bad, 1.0, 0.0), axis=1, keepdims=True), axis=0, keepdims=True) == 0.0
        over = jnp.where(good, spill, over)
        size = jnp.where(good, float(cap), size)
        rung = jnp.where(good, rung, rung + 1.0)
    rung_ref[...] = rung.astype(I32)
    offset = TAIL - over + inside
    high = jnp.floor(offset * (1.0 / ALIGN))
    low = offset - high * ALIGN

    rows[0], rows[1], rows[2], rows[3] = high, low, keep0, keep1
    table = jnp.concatenate([rows[i, pl.ds(me, 1), :] for i in range(4)] + [jnp.zeros((4, experts), F32)], axis=0).astype(BF16)
    side = lax.rem(me, 2)

    @pl.loop(0, blocks)
    def _(b):
        cols = pl.ds(pl.multiple_of(b * TOKEN_BLOCK, TOKEN_BLOCK), TOKEN_BLOCK)
        for j in range(2):
            ids = ids_ref[j : j + 1, cols]
            hot16 = jnp.where(expert_rows == ids, 1.0, 0.0).astype(BF16)
            found = jnp.dot(table, hot16, preferred_element_type=F32)
            rk = rank[j : j + 1, cols]
            spot = found[0:1] * ALIGN + found[1:2] + rk
            if j == 1:
                spot = spot + found[2:3]
            owner = ids // local
            half = ((owner + side) % 2).astype(F32)
            direct = spot >= TAIL
            row = jnp.where(direct, half * size + spot - TAIL, (2.0 - half) * size + spot - TAIL)
            key = row.astype(I32) + (owner // 2) * (2 * stride)
            pos_ref[j : j + 1, cols] = jnp.where(rk < found[2 + j : 3 + j], key, -1)

    mine = (iota((local, experts), 1) == iota((local, experts), 0) + me * local).astype(BF16)

    def pick(values):
        return lax.dot_general(mine, values.astype(BF16), (((1,), (1,)), ((), ())), preferred_element_type=F32)

    from_step = (source_of(me, iota((groups, groups), 0), groups) == iota((groups, groups), 1)).astype(BF16)
    older, newer = iota((groups, groups), 1), iota((groups, groups), 0)
    ahead_of = ((older < newer) & ((older < near) == (newer < near))).astype(BF16)

    def by_step(values):
        return jnp.dot(from_step, values.astype(BF16), preferred_element_type=F32)

    kept = by_step(keep)
    ahead = pick(jnp.dot(ahead_of, kept.astype(BF16), preferred_element_type=F32))
    high, low, kept = pick(by_step(high)), pick(by_step(low)), pick(kept)
    start_ref[...] = high.astype(I32)
    lanes = groups * WIN
    spread = (iota((groups, lanes), 1) // WIN == iota((groups, lanes), 0)).astype(BF16)

    def widen(values):
        return jnp.dot(values.astype(BF16), spread, preferred_element_type=F32)

    wide_low, wide_kept, wide_ahead = widen(low), widen(kept), widen(ahead)
    lane = (iota((local, lanes), 1) % WIN).astype(F32)
    valid = (lane >= wide_low) & (lane < wide_low + wide_kept)
    slot_ref[...] = jnp.where(valid, wide_ahead + lane - wide_low, -1.0).astype(I32)
    seat = iota((local, capacity), 1).astype(F32)
    goals = [jnp.full((local, capacity), -1.0, F32) for _ in range(2)]
    for step in range(groups):
        begin, count = ahead[:, step : step + 1], kept[:, step : step + 1]
        spot = high[:, step : step + 1] * ALIGN + low[:, step : step + 1] + step * stride
        part = int(step >= near)
        goals[part] = jnp.where((seat >= begin) & (seat < begin + count), seat - begin + spot, goals[part])
    for part in range(2):
        place_ref[part] = goals[part].astype(I32)


def moe_kernel(groups, cap, stride, local, near, start_ref, slot_ref, place_ref, pos_ref, gate_ref, x_hbm, w_in_hbm, w_out_hbm, out_ref, x_ref, buf, got_a, got_b, outs, tails, ret, w_in, w_out, win, obuf, spots, gates, acc, w_sem, send_sem, recv_sem, back_send, back_recv, tail_send, tail_recv, pass_send, pass_recv, own_sem):
    me = lax.axis_index("expert")
    tokens, dim = x_ref.shape
    depth = w_in.shape[0]
    x_copy = pltpu.make_async_copy(x_hbm, x_ref, own_sem.at[2])
    x_copy.start()
    full = cap + TAIL
    full_blocks, cap_blocks, tail_blocks = full // ALIGN, cap // ALIGN, TAIL // ALIGN
    token_blocks = tokens // TOKEN_BLOCK
    sibling = {"expert": me + 1 - 2 * lax.rem(me, 2)}
    barrier = announce(me, groups)

    def fetch(visit):
        e, place = lax.rem(visit, local), lax.rem(visit, depth)
        return (
            pltpu.make_async_copy(w_in_hbm.at[e], w_in.at[place], w_sem.at[0, place]),
            pltpu.make_async_copy(w_out_hbm.at[e], w_out.at[place], w_sem.at[1, place]),
        )

    for visit in range(depth):
        for copy in fetch(visit):
            copy.start()

    def mate_of(step):
        return step + 1 - 2 * lax.rem(step, 2)

    def push(step, got, first):
        return pltpu.make_async_remote_copy(src_ref=buf.at[step], dst_ref=got.at[pl.ds((step - first) * full_blocks + tail_blocks, cap_blocks)], send_sem=send_sem.at[step], recv_sem=recv_sem.at[step], device_id={"expert": peer(me, step, groups)}, device_id_type=MESH)

    def tail_over(step, got, first):
        return pltpu.make_async_remote_copy(src_ref=got.at[pl.ds((step - first) * full_blocks + cap_blocks, tail_blocks)], dst_ref=got.at[pl.ds((mate_of(step) - first) * full_blocks, tail_blocks)], send_sem=tail_send.at[step], recv_sem=tail_recv.at[mate_of(step)], device_id=sibling, device_id_type=MESH)

    def tail_in(step, got, first):
        return pltpu.make_async_remote_copy(src_ref=got.at[pl.ds((mate_of(step) - first) * full_blocks + cap_blocks, tail_blocks)], dst_ref=got.at[pl.ds((step - first) * full_blocks, tail_blocks)], send_sem=tail_send.at[mate_of(step)], recv_sem=tail_recv.at[step], device_id=sibling, device_id_type=MESH)

    def pass_over(step):
        return pltpu.make_async_remote_copy(src_ref=outs.at[step, pl.ds(0, TAIL)], dst_ref=tails.at[mate_of(step)], send_sem=pass_send.at[step], recv_sem=pass_recv.at[mate_of(step)], device_id=sibling, device_id_type=MESH)

    def pass_in(step):
        return pltpu.make_async_remote_copy(src_ref=outs.at[mate_of(step), pl.ds(0, TAIL)], dst_ref=tails.at[step], send_sem=pass_send.at[mate_of(step)], recv_sem=pass_recv.at[step], device_id=sibling, device_id_type=MESH)

    def berth(step):
        rest = step - (groups - 4)
        return step + step // (groups - 4) * (rest % 2 * 2 + rest // 2 - rest)

    def give(step):
        return pltpu.make_async_remote_copy(src_ref=outs.at[step, pl.ds(TAIL, cap)], dst_ref=ret.at[berth(step)], send_sem=back_send.at[step], recv_sem=back_recv.at[step], device_id={"expert": source_of(me, step, groups)}, device_id_type=MESH)

    def pack(step):
        base = peer(me, step, groups) // 2 * (2 * stride) + lax.rem(step, 2) * cap
        spot = pos_ref[...] - base
        line = iota((cap, tokens), 0)
        hot = (line == spot[0:1]) | (line == spot[1:2])
        rows = jnp.dot(jnp.where(hot, 1.0, 0.0).astype(BF16), x_ref[...], preferred_element_type=F32).astype(BF16)
        buf[step] = rows.reshape(cap_blocks, ALIGN, dim)

    x_copy.wait()
    pack(0)
    pl.semaphore_wait(barrier, groups - 1)

    @pl.loop(1, groups)
    def _(step):
        pack(step)

        @pl.when(step < near)
        def _():
            push(step, got_a, 0).start()

        @pl.when(step >= near)
        def _():
            push(step, got_b, near).start()

    mine = pltpu.make_async_copy(buf.at[0], got_a.at[pl.ds(tail_blocks, cap_blocks)], own_sem.at[0])
    mine.start()
    pad = WIN // ALIGN
    got_a[pl.ds(near * full_blocks, pad)] = jnp.zeros((pad, ALIGN, dim), BF16)
    got_b[pl.ds((groups - near) * full_blocks, pad)] = jnp.zeros((pad, ALIGN, dim), BF16)

    @pl.loop(0, groups)
    def _(step):
        outs[step] = jnp.zeros((full, dim), BF16)

    @pl.loop(0, tokens // 128)
    def _(b):
        at = pl.ds(pl.multiple_of(b * 128, 128), 128)
        for j in range(2):
            spots[j, at, :] = jnp.broadcast_to(pos_ref[j : j + 1, at], (128, 128)).T
            gates[j, at, :] = jnp.broadcast_to(gate_ref[j : j + 1, at], (128, 128)).T
            acc[j, at, :] = jnp.zeros((128, dim), BF16)

    def experts(got, first, last, done):
        lanes = (last - first) * WIN

        @pl.loop(0, local // 4)
        def _(quad):
            @pl.loop(0, 2)
            def _(twin):
                pair = quad * 2 + twin
                for k in range(2):
                    e = pair * 2 + k
                    for step in range(first, last):
                        row = (step - first) * full_blocks + start_ref[e, step]
                        for half in range(WIN // ALIGN):
                            at = (step - first) * WIN + half * ALIGN
                            win[k, at : at + ALIGN, :] = got[row + half]
                for k in range(2):
                    e = pair * 2 + k
                    visit = done + e
                    place = lax.rem(visit, depth)
                    for copy in fetch(visit):
                        copy.wait()
                    slot = slot_ref[pl.ds(e, 1), :][:, first * WIN : last * WIN]
                    hot = jnp.where(iota((128, lanes), 0) == slot, 1.0, 0.0).astype(BF16)
                    x = jnp.dot(hot, win[k, :lanes, :], preferred_element_type=F32).astype(BF16)
                    h = jax.nn.gelu(jnp.dot(x, w_in[place], preferred_element_type=F32)).astype(BF16)
                    o = jnp.dot(h, w_out[place], preferred_element_type=F32).astype(BF16)
                    obuf[pl.ds(pl.multiple_of(twin * 256 + k * 128, 128), 128), :] = o
                for k in range(2):
                    visit = done + pair * 2 + k + depth

                    @pl.when(visit < 2 * local)
                    def _():
                        for copy in fetch(visit):
                            copy.start()

            part = 0 if first == 0 else 1
            goal = jnp.concatenate([place_ref[part, pl.ds(quad * 4 + k, 1), :] for k in range(4)], axis=1)

            @pl.loop(first, last)
            def _(step):
                hot = jnp.where(iota((full, 512), 0) == goal - step * stride, 1.0, 0.0).astype(BF16)
                outs[step] += jnp.dot(hot, obuf[...], preferred_element_type=F32).astype(BF16)

    def send_back(first, last):
        @pl.loop(first, last)
        def _(step):
            pass_over(step).start()

        @pl.loop(first, last)
        def _(step):
            pass_in(step).wait_recv()
            outs[step, cap:, :] += tails[step]

            @pl.when(step > 0)
            def _():
                give(step).start()

    def chip_base(step):
        return peer(me, step, groups) // 2 * (2 * stride)

    def picked(at, returned, lines):
        lane = iota((TOKEN_BLOCK, 128), 1)
        for j in range(2):
            line = lines(spots[j, at, :])
            hot = jnp.concatenate([jnp.where(line - k == lane, 1.0, 0.0).astype(BF16) for k in range(0, 2 * cap, 128)], axis=1)
            yield j, acc[j, at, :] + jnp.dot(hot[:, : 2 * cap], returned, preferred_element_type=F32).astype(BF16)

    def add(first, lines, finish):
        returned = ret[pl.ds(first, 2)].reshape(2 * cap, dim)

        @pl.loop(0, token_blocks)
        def _(b):
            at = pl.ds(pl.multiple_of(b * TOKEN_BLOCK, TOKEN_BLOCK), TOKEN_BLOCK)
            sums = [value for _, value in picked(at, returned, lines)]
            if not finish:
                for j in range(2):
                    acc[j, at, :] = sums[j]
                return
            for c in range(0, dim, 128):
                mixed = x_ref[at, c : c + 128].astype(F32) + gates[0, at, :] * sums[0][:, c : c + 128].astype(F32)
                out_ref[at, c : c + 128] = (mixed + gates[1, at, :] * sums[1][:, c : c + 128].astype(F32)).astype(BF16)

    mine.wait()
    tail_over(0, got_a, 0).start()

    @pl.loop(1, near)
    def _(step):
        push(step, got_a, 0).wait_recv()
        tail_over(step, got_a, 0).start()

    @pl.loop(0, near)
    def _(step):
        tail_in(step, got_a, 0).wait_recv()

    experts(got_a, 0, near, 0)
    send_back(0, near)
    back = pltpu.make_async_copy(outs.at[0, pl.ds(TAIL, cap)], ret.at[0], own_sem.at[1])
    back.start()

    @pl.loop(near, groups)
    def _(step):
        push(step, got_b, near).wait_recv()
        tail_over(step, got_b, near).start()

    @pl.loop(near, groups)
    def _(step):
        tail_in(step, got_b, near).wait_recv()

    experts(got_b, near, groups, local)
    send_back(near, groups)
    back.wait()

    @pl.loop(0, groups // 2 - 2)
    def _(half):
        @pl.when(half > 0)
        def _():
            give(half * 2).wait_recv()

        give(half * 2 + 1).wait_recv()
        base = chip_base(half * 2)
        add(half * 2, lambda spot: spot - base, False)

    for core in range(2):
        steps = [groups - 4 + core, groups - 2 + core]
        for step in steps:
            give(step).wait_recv()
        bases = [chip_base(step) + core * cap for step in steps]

        def lines(spot):
            near_by, other = spot - bases[0], spot - bases[1]
            other = jnp.where((other >= 0) & (other < cap), other + cap, -1)
            return jnp.where((near_by >= 0) & (near_by < cap), near_by, other)

        add(groups - 4 + 2 * core, lines, core == 1)

    @pl.loop(1, near)
    def _(step):
        push(step, got_a, 0).wait_send()

    @pl.loop(near, groups)
    def _(step):
        push(step, got_b, near).wait_send()

    @pl.loop(0, near)
    def _(step):
        tail_over(step, got_a, 0).wait_send()

    @pl.loop(near, groups)
    def _(step):
        tail_over(step, got_b, near).wait_send()

    @pl.loop(0, groups)
    def _(step):
        pass_over(step).wait_send()

    @pl.loop(1, groups)
    def _(step):
        give(step).wait_send()


def solution(mesh):
    groups = mesh.shape["expert"]
    row_spec = P(("data", "expert"), None)
    weight_spec = P("expert", None, None)

    def device_step(token_rows, expert_ids, gate_weights, w_in, w_out):
        tokens, top_k = expert_ids.shape
        local, dim, hidden = w_in.shape
        experts = local * groups
        mean_load = tokens * top_k // experts
        capacity = groups * mean_load
        worst = local * (7 * mean_load // 4)
        sizes = [local * mean_load * 18 // 16, local * mean_load * 19 // 16, worst]
        stride = 2 * local * mean_load
        lanes = groups * WIN
        near = groups // 2
        vmem = pl.BlockSpec(memory_space=VMEM)
        anywhere = pl.BlockSpec(memory_space=pl.ANY)

        def params(collective_id):
            return pltpu.CompilerParams(collective_id=collective_id, has_side_effects=True, vmem_limit_bytes=61 * 1024 * 1024)

        pair_sems = [pltpu.SemaphoreType.DMA((groups,)), pltpu.SemaphoreType.DMA((groups,))]
        pos, slot, start, place, rung = pl.pallas_call(
            functools.partial(route_kernel, groups, capacity, sizes, stride, local, near),
            out_shape=[
                jax.ShapeDtypeStruct((top_k, tokens), I32),
                jax.ShapeDtypeStruct((local, lanes), I32),
                jax.ShapeDtypeStruct((local, groups), I32),
                jax.ShapeDtypeStruct((2, local, capacity), I32),
                jax.ShapeDtypeStruct((1, 1), I32),
            ],
            in_specs=[vmem],
            out_specs=[vmem] * 5,
            scratch_shapes=[
                VMEM((groups, top_k, experts), F32),
                VMEM((top_k, experts, 128), F32),
                VMEM((top_k, tokens), F32),
                VMEM((4, groups, experts), F32),
            ]
            + pair_sems,
            compiler_params=params(0),
            name="route",
        )(expert_ids.T)

        def exchange(cap, collective_id):
            depth = 4 if cap == worst else 10

            def run():
                return pl.pallas_call(
                    functools.partial(moe_kernel, groups, cap, stride, local, near),
                    out_shape=jax.ShapeDtypeStruct((tokens, dim), BF16),
                    in_specs=[pl.BlockSpec(memory_space=pltpu.SMEM)] + [vmem] * 4 + [anywhere] * 3,
                    out_specs=vmem,
                    scratch_shapes=[
                        VMEM((tokens, dim), BF16),
                        VMEM((groups, cap // ALIGN, ALIGN, dim), BF16),
                        VMEM(((near * (cap + TAIL) + WIN) // ALIGN, ALIGN, dim), BF16),
                        VMEM((((groups - near) * (cap + TAIL) + WIN) // ALIGN, ALIGN, dim), BF16),
                        VMEM((groups, cap + TAIL, dim), BF16),
                        VMEM((groups, TAIL, dim), BF16),
                        VMEM((groups, cap, dim), BF16),
                        VMEM((depth, dim, hidden), BF16),
                        VMEM((depth, hidden, dim), BF16),
                        VMEM((2, near * WIN, dim), BF16),
                        VMEM((4 * capacity, dim), BF16),
                        VMEM((top_k, tokens, 128), I32),
                        VMEM((top_k, tokens, 128), F32),
                        VMEM((top_k, tokens, dim), BF16),
                        pltpu.SemaphoreType.DMA((2, depth)),
                    ]
                    + pair_sems * 4
                    + [pltpu.SemaphoreType.DMA((3,))],
                    compiler_params=params(collective_id),
                    name="experts",
                )(start, slot, place, pos, gate_weights.T, token_rows, w_in, w_out)

            return run

        return lax.switch(rung.reshape(()), [exchange(cap, 1 + i) for i, cap in enumerate(sizes)])

    return jax.shard_map(device_step, mesh=mesh, in_specs=(row_spec, row_spec, row_spec, weight_spec, weight_spec), out_specs=row_spec, check_vma=False)
```

```python
import functools

import jax
import jax.numpy as jnp
from jax import lax
from jax.experimental import pallas as pl
from jax.experimental.pallas import tpu as pltpu
from jax.sharding import PartitionSpec as P

MESH = pl.DeviceIdType.MESH
VMEM = pltpu.VMEM
F32, BF16, I32 = jnp.float32, jnp.bfloat16, jnp.int32
WIN = 32
ALIGN = 16
TAIL = 48
TOKEN_BLOCK = 256


def iota(shape, dim):
    return lax.broadcasted_iota(I32, shape, dim)


def chips_away(step, chips):
    half = step // 2
    return lax.rem(2 * half + 3 * (half // (chips // 2)), chips)


def peer(me, step, groups):
    chips = groups // 2
    chip = lax.rem(me // 2 + chips_away(step, chips), chips)
    return chip * 2 + lax.rem(me + step, 2)


def source_of(me, step, groups):
    chips = groups // 2
    chip = lax.rem(me // 2 - chips_away(step, chips) + chips, chips)
    return chip * 2 + lax.rem(me + step, 2)


def announce(me, groups):
    barrier = pltpu.get_barrier_semaphore()

    @pl.loop(1, groups)
    def _(step):
        pl.semaphore_signal(barrier, inc=1, device_id={"expert": lax.rem(me + step, groups)}, device_id_type=MESH)

    return barrier


def route_kernel(groups, capacity, sizes, stride, local, near, ids_ref, pos_ref, slot_ref, start_ref, place_ref, rung_ref, cnt, carry, rank, rows, send_sem, recv_sem):
    me = lax.axis_index("expert")
    tokens = ids_ref.shape[1]
    experts = local * groups
    blocks = tokens // TOKEN_BLOCK
    barrier = announce(me, groups)

    expert_rows = iota((experts, TOKEN_BLOCK), 0)
    upper = (iota((TOKEN_BLOCK, TOKEN_BLOCK), 0) <= iota((TOKEN_BLOCK, TOKEN_BLOCK), 1)).astype(BF16)
    carry[...] = jnp.zeros_like(carry)

    @pl.loop(0, blocks)
    def _(b):
        cols = pl.ds(pl.multiple_of(b * TOKEN_BLOCK, TOKEN_BLOCK), TOKEN_BLOCK)
        for j in range(2):
            hot = expert_rows == ids_ref[j : j + 1, cols]
            run = jnp.dot(jnp.where(hot, 1.0, 0.0).astype(BF16), upper, preferred_element_type=F32)
            run = run + jnp.concatenate([carry[j]] * (TOKEN_BLOCK // 128), axis=1)
            rank[j : j + 1, cols] = jnp.sum(jnp.where(hot, run, 0.0), axis=0, keepdims=True) - 1.0
            carry[j] = jnp.broadcast_to(run[:, TOKEN_BLOCK - 1 :], (experts, 128))

    for j in range(2):
        row = jnp.concatenate([carry[j, k : k + 128, :].T[:1] for k in range(0, experts, 128)], axis=1)
        cnt[me, j : j + 1, :] = row

    def send(step):
        to = lax.rem(me + step, groups)
        return pltpu.make_async_remote_copy(src_ref=cnt.at[me], dst_ref=cnt.at[me], send_sem=send_sem.at[step], recv_sem=recv_sem.at[step], device_id={"expert": to}, device_id_type=MESH)

    def arrive(step):
        origin = lax.rem(me - step + groups, groups)
        return pltpu.make_async_remote_copy(src_ref=cnt.at[origin], dst_ref=cnt.at[origin], send_sem=send_sem.at[step], recv_sem=recv_sem.at[step], device_id={"expert": origin}, device_id_type=MESH)

    pl.semaphore_wait(barrier, groups - 1)

    @pl.loop(1, groups)
    def _(step):
        send(step).start()

    @pl.loop(1, groups)
    def _(step):
        arrive(step).wait_recv()

    @pl.loop(1, groups)
    def _(step):
        send(step).wait_send()

    first, second = cnt[:, 0, :], cnt[:, 1, :]
    earlier = (iota((groups, groups), 1) < iota((groups, groups), 0)).astype(BF16)
    before0 = jnp.dot(earlier, first.astype(BF16), preferred_element_type=F32)
    before1 = jnp.dot(earlier, second.astype(BF16), preferred_element_type=F32)
    total0 = jnp.sum(first, axis=0, keepdims=True)
    keep0 = jnp.clip(capacity - before0, 0.0, first)
    keep1 = jnp.clip(capacity - total0 - before1, 0.0, second)
    keep = keep0 + keep1
    keep16 = keep.astype(BF16)
    er, ec = iota((experts, experts), 0), iota((experts, experts), 1)
    mate = er // local - ec // local + 2 * (ec // local % 2)
    same = er // local == ec // local
    load = jnp.dot(keep16, same.astype(BF16), preferred_element_type=F32)
    mate_load = jnp.dot(keep16, (mate == 1).astype(BF16), preferred_element_type=F32)
    inside = jnp.dot(keep16, (same & (er < ec)).astype(BF16), preferred_element_type=F32)
    rung = jnp.zeros((1, 1), F32)
    over = jnp.zeros_like(load)
    size = jnp.full((1, 1), float(sizes[-1]), F32)
    for cap in reversed(sizes[:-1]):
        spill = jnp.maximum(load - cap, 0.0)
        bad = (spill > TAIL) | ((spill > 0.0) & (mate_load + spill > cap))
        good = jnp.max(jnp.max(jnp.where(bad, 1.0, 0.0), axis=1, keepdims=True), axis=0, keepdims=True) == 0.0
        over = jnp.where(good, spill, over)
        size = jnp.where(good, float(cap), size)
        rung = jnp.where(good, rung, rung + 1.0)
    rung_ref[...] = rung.astype(I32)
    offset = TAIL - over + inside
    high = jnp.floor(offset * (1.0 / ALIGN))
    low = offset - high * ALIGN

    rows[0], rows[1], rows[2], rows[3] = high, low, keep0, keep1
    table = jnp.concatenate([rows[i, pl.ds(me, 1), :] for i in range(4)] + [jnp.zeros((4, experts), F32)], axis=0).astype(BF16)
    side = lax.rem(me, 2)

    @pl.loop(0, blocks)
    def _(b):
        cols = pl.ds(pl.multiple_of(b * TOKEN_BLOCK, TOKEN_BLOCK), TOKEN_BLOCK)
        for j in range(2):
            ids = ids_ref[j : j + 1, cols]
            hot16 = jnp.where(expert_rows == ids, 1.0, 0.0).astype(BF16)
            found = jnp.dot(table, hot16, preferred_element_type=F32)
            rk = rank[j : j + 1, cols]
            spot = found[0:1] * ALIGN + found[1:2] + rk
            if j == 1:
                spot = spot + found[2:3]
            owner = ids // local
            half = ((owner + side) % 2).astype(F32)
            direct = spot >= TAIL
            row = jnp.where(direct, half * size + spot - TAIL, (2.0 - half) * size + spot - TAIL)
            key = row.astype(I32) + (owner // 2) * (2 * stride)
            pos_ref[j : j + 1, cols] = jnp.where(rk < found[2 + j : 3 + j], key, -1)

    mine = (iota((local, experts), 1) == iota((local, experts), 0) + me * local).astype(BF16)

    def pick(values):
        return lax.dot_general(mine, values.astype(BF16), (((1,), (1,)), ((), ())), preferred_element_type=F32)

    from_step = (source_of(me, iota((groups, groups), 0), groups) == iota((groups, groups), 1)).astype(BF16)
    older, newer = iota((groups, groups), 1), iota((groups, groups), 0)
    ahead_of = ((older < newer) & ((older < near) == (newer < near))).astype(BF16)

    def by_step(values):
        return jnp.dot(from_step, values.astype(BF16), preferred_element_type=F32)

    kept = by_step(keep)
    ahead = pick(jnp.dot(ahead_of, kept.astype(BF16), preferred_element_type=F32))
    high, low, kept = pick(by_step(high)), pick(by_step(low)), pick(kept)
    start_ref[...] = high.astype(I32)
    lanes = groups * WIN
    spread = (iota((groups, lanes), 1) // WIN == iota((groups, lanes), 0)).astype(BF16)

    def widen(values):
        return jnp.dot(values.astype(BF16), spread, preferred_element_type=F32)

    wide_low, wide_kept, wide_ahead = widen(low), widen(kept), widen(ahead)
    lane = (iota((local, lanes), 1) % WIN).astype(F32)
    valid = (lane >= wide_low) & (lane < wide_low + wide_kept)
    slot_ref[...] = jnp.where(valid, wide_ahead + lane - wide_low, -1.0).astype(I32)
    seat = iota((local, capacity), 1).astype(F32)
    goals = [jnp.full((local, capacity), -1.0, F32) for _ in range(2)]
    for step in range(groups):
        begin, count = ahead[:, step : step + 1], kept[:, step : step + 1]
        spot = high[:, step : step + 1] * ALIGN + low[:, step : step + 1] + step * stride
        part = int(step >= near)
        goals[part] = jnp.where((seat >= begin) & (seat < begin + count), seat - begin + spot, goals[part])
    for part in range(2):
        place_ref[part] = goals[part].astype(I32)


def moe_kernel(groups, cap, stride, local, near, segment, start_ref, slot_ref, place_ref, pos_ref, gate_ref, x_hbm, w_in_hbm, w_out_hbm, out_ref, x_ref, buf, got_a, got_b, outs, tails, ret, w_in, w_out, win, obuf, spots, gates, acc, w_sem, send_sem, recv_sem, back_send, back_recv, tail_send, tail_recv, pass_send, pass_recv, own_sem):
    me = lax.axis_index("expert")
    tokens, dim = x_ref.shape
    depth = w_in.shape[0]
    x_copy = pltpu.make_async_copy(x_hbm, x_ref, own_sem.at[2])
    x_copy.start()
    full = cap + TAIL
    full_blocks, cap_blocks, tail_blocks = full // ALIGN, cap // ALIGN, TAIL // ALIGN
    token_blocks = tokens // TOKEN_BLOCK
    sibling = {"expert": me + 1 - 2 * lax.rem(me, 2)}
    barrier = announce(me, groups)

    def fetch(visit):
        e, place = lax.rem(visit, local), lax.rem(visit, depth)
        return (
            pltpu.make_async_copy(w_in_hbm.at[e], w_in.at[place], w_sem.at[0, place]),
            pltpu.make_async_copy(w_out_hbm.at[e], w_out.at[place], w_sem.at[1, place]),
        )

    for visit in range(depth):
        for copy in fetch(visit):
            copy.start()

    def mate_of(step):
        return step + 1 - 2 * lax.rem(step, 2)

    def push(step, got, first):
        return pltpu.make_async_remote_copy(src_ref=buf.at[step], dst_ref=got.at[pl.ds((step - first) * full_blocks + tail_blocks, cap_blocks)], send_sem=send_sem.at[step], recv_sem=recv_sem.at[step], device_id={"expert": peer(me, step, groups)}, device_id_type=MESH)

    def tail_over(step, got, first):
        return pltpu.make_async_remote_copy(src_ref=got.at[pl.ds((step - first) * full_blocks + cap_blocks, tail_blocks)], dst_ref=got.at[pl.ds((mate_of(step) - first) * full_blocks, tail_blocks)], send_sem=tail_send.at[step], recv_sem=tail_recv.at[mate_of(step)], device_id=sibling, device_id_type=MESH)

    def tail_in(step, got, first):
        return pltpu.make_async_remote_copy(src_ref=got.at[pl.ds((mate_of(step) - first) * full_blocks + cap_blocks, tail_blocks)], dst_ref=got.at[pl.ds((step - first) * full_blocks, tail_blocks)], send_sem=tail_send.at[mate_of(step)], recv_sem=tail_recv.at[step], device_id=sibling, device_id_type=MESH)

    def pass_over(step):
        return pltpu.make_async_remote_copy(src_ref=outs.at[step, pl.ds(0, TAIL)], dst_ref=tails.at[mate_of(step)], send_sem=pass_send.at[step], recv_sem=pass_recv.at[mate_of(step)], device_id=sibling, device_id_type=MESH)

    def pass_in(step):
        return pltpu.make_async_remote_copy(src_ref=outs.at[mate_of(step), pl.ds(0, TAIL)], dst_ref=tails.at[step], send_sem=pass_send.at[mate_of(step)], recv_sem=pass_recv.at[step], device_id=sibling, device_id_type=MESH)

    def berth(step):
        rest = step - (groups - 4)
        return step + step // (groups - 4) * (rest % 2 * 2 + rest // 2 - rest)

    def give(step):
        return pltpu.make_async_remote_copy(src_ref=outs.at[step, pl.ds(TAIL, cap)], dst_ref=ret.at[berth(step)], send_sem=back_send.at[step], recv_sem=back_recv.at[step], device_id={"expert": source_of(me, step, groups)}, device_id_type=MESH)

    def pack(step):
        base = peer(me, step, groups) // 2 * (2 * stride) + lax.rem(step, 2) * cap
        spot = pos_ref[...] - base
        line = iota((cap, tokens), 0)
        hot = (line == spot[0:1]) | (line == spot[1:2])
        rows = jnp.dot(jnp.where(hot, 1.0, 0.0).astype(BF16), x_ref[...], preferred_element_type=F32).astype(BF16)
        buf[step] = rows.reshape(cap_blocks, ALIGN, dim)

    def turn(index):
        third = index % 3
        early = 2 * (2 - third + 3 * (third * (third - 1) // 2)) + index // 3
        later = (index + groups - 6) // groups
        last = (index + 2) // groups
        return index + (1 - later) * (early - index) + 2 * later - groups * last

    x_copy.wait()
    pack(4)
    pl.semaphore_wait(barrier, groups - 1)
    push(4, got_a, 0).start()

    @pl.loop(1, groups)
    def _(index):
        step = turn(index)
        pack(step)

        @pl.when((step > 0) & (step < near))
        def _():
            push(step, got_a, 0).start()

        @pl.when(step >= near)
        def _():
            push(step, got_b, near).start()

    mine = pltpu.make_async_copy(buf.at[0], got_a.at[pl.ds(tail_blocks, cap_blocks)], own_sem.at[0])
    mine.start()
    pad = WIN // ALIGN
    got_a[pl.ds(near * full_blocks, pad)] = jnp.zeros((pad, ALIGN, dim), BF16)
    got_b[pl.ds((groups - near) * full_blocks, pad)] = jnp.zeros((pad, ALIGN, dim), BF16)

    @pl.loop(0, groups)
    def _(step):
        outs[step] = jnp.zeros((full, dim), BF16)

    @pl.loop(0, tokens // 128)
    def _(b):
        at = pl.ds(pl.multiple_of(b * 128, 128), 128)
        for j in range(2):
            spots[j, at, :] = jnp.broadcast_to(pos_ref[j : j + 1, at], (128, 128)).T
            gates[j, at, :] = jnp.broadcast_to(gate_ref[j : j + 1, at], (128, 128)).T
            acc[j, at, :] = jnp.zeros((128, dim), BF16)

    obuf[...] = jnp.zeros_like(obuf)

    def experts(got, first, last, done):
        lanes = (last - first) * WIN
        seats = (last - first) * segment

        @pl.loop(0, local // 4)
        def _(quad):
            @pl.loop(0, 2)
            def _(twin):
                pair = quad * 2 + twin
                for k in range(2):
                    e = pair * 2 + k
                    for step in range(first, last):
                        row = (step - first) * full_blocks + start_ref[e, step]
                        for half in range(WIN // ALIGN):
                            at = (step - first) * WIN + half * ALIGN
                            win[k, at : at + ALIGN, :] = got[row + half]
                for k in range(2):
                    e = pair * 2 + k
                    visit = done + e
                    place = lax.rem(visit, depth)
                    for copy in fetch(visit):
                        copy.wait()
                    slot = slot_ref[pl.ds(e, 1), :][:, first * WIN : last * WIN]
                    hot = jnp.where(iota((seats, lanes), 0) == slot, 1.0, 0.0).astype(BF16)
                    x = jnp.dot(hot, win[k, :lanes, :], preferred_element_type=F32).astype(BF16)
                    h = jax.nn.gelu(jnp.dot(x, w_in[place], preferred_element_type=F32)).astype(BF16)
                    o = jnp.dot(h, w_out[place], preferred_element_type=F32).astype(BF16)
                    obuf[pl.ds(pl.multiple_of(twin * 256 + k * 128, 128), seats), :] = o
                for k in range(2):
                    visit = done + pair * 2 + k + depth

                    @pl.when(visit < 2 * local)
                    def _():
                        for copy in fetch(visit):
                            copy.start()

            part = 0 if first == 0 else 1
            goal = jnp.concatenate([place_ref[part, pl.ds(quad * 4 + k, 1), :] for k in range(4)], axis=1)

            def place_rows(rows):
                @pl.loop(first, last)
                def _(step):
                    hot = jnp.where(iota((rows, 512), 0) == goal - step * stride, 1.0, 0.0).astype(BF16)
                    outs[step, :rows] += jnp.dot(hot, obuf[...], preferred_element_type=F32).astype(BF16)

            short = TAIL + 8 * segment

            @pl.when(quad < 2)
            def _():
                place_rows(short)

            @pl.when(quad >= 2)
            def _():
                place_rows(full)

    def send_back(first, last):
        @pl.loop(first, last)
        def _(step):
            pass_over(step).start()

        @pl.loop(first, last)
        def _(step):
            pass_in(step).wait_recv()
            outs[step, cap:, :] += tails[step]

            @pl.when(step > 0)
            def _():
                give(step).start()

    def chip_base(step):
        return peer(me, step, groups) // 2 * (2 * stride)

    def picked(at, returned, lines):
        lane = iota((TOKEN_BLOCK, 128), 1)
        for j in range(2):
            line = lines(spots[j, at, :])
            hot = jnp.concatenate([jnp.where(line - k == lane, 1.0, 0.0).astype(BF16) for k in range(0, 2 * cap, 128)], axis=1)
            yield j, acc[j, at, :] + jnp.dot(hot[:, : 2 * cap], returned, preferred_element_type=F32).astype(BF16)

    def add(first, lines, finish):
        returned = ret[pl.ds(first, 2)].reshape(2 * cap, dim)

        @pl.loop(0, token_blocks)
        def _(b):
            at = pl.ds(pl.multiple_of(b * TOKEN_BLOCK, TOKEN_BLOCK), TOKEN_BLOCK)
            sums = [value for _, value in picked(at, returned, lines)]
            if not finish:
                for j in range(2):
                    acc[j, at, :] = sums[j]
                return
            for c in range(0, dim, 128):
                mixed = x_ref[at, c : c + 128].astype(F32) + gates[0, at, :] * sums[0][:, c : c + 128].astype(F32)
                out_ref[at, c : c + 128] = (mixed + gates[1, at, :] * sums[1][:, c : c + 128].astype(F32)).astype(BF16)

    mine.wait()
    tail_over(0, got_a, 0).start()

    @pl.loop(1, near)
    def _(step):
        push(step, got_a, 0).wait_recv()
        tail_over(step, got_a, 0).start()

    @pl.loop(0, near)
    def _(step):
        tail_in(step, got_a, 0).wait_recv()

    experts(got_a, 0, near, 0)
    send_back(0, near)
    back = pltpu.make_async_copy(outs.at[0, pl.ds(TAIL, cap)], ret.at[0], own_sem.at[1])
    back.start()

    @pl.loop(near, groups)
    def _(step):
        push(step, got_b, near).wait_recv()
        tail_over(step, got_b, near).start()

    @pl.loop(near, groups)
    def _(step):
        tail_in(step, got_b, near).wait_recv()

    experts(got_b, near, groups, local)
    send_back(near, groups)
    back.wait()

    @pl.loop(0, groups // 2 - 2)
    def _(half):
        @pl.when(half > 0)
        def _():
            give(half * 2).wait_recv()

        give(half * 2 + 1).wait_recv()
        base = chip_base(half * 2)
        add(half * 2, lambda spot: spot - base, False)

    for core in range(2):
        steps = [groups - 4 + core, groups - 2 + core]
        for step in steps:
            give(step).wait_recv()
        bases = [chip_base(step) + core * cap for step in steps]

        def lines(spot):
            near_by, other = spot - bases[0], spot - bases[1]
            other = jnp.where((other >= 0) & (other < cap), other + cap, -1)
            return jnp.where((near_by >= 0) & (near_by < cap), near_by, other)

        add(groups - 4 + 2 * core, lines, core == 1)

    @pl.loop(1, near)
    def _(step):
        push(step, got_a, 0).wait_send()

    @pl.loop(near, groups)
    def _(step):
        push(step, got_b, near).wait_send()

    @pl.loop(0, near)
    def _(step):
        tail_over(step, got_a, 0).wait_send()

    @pl.loop(near, groups)
    def _(step):
        tail_over(step, got_b, near).wait_send()

    @pl.loop(0, groups)
    def _(step):
        pass_over(step).wait_send()

    @pl.loop(1, groups)
    def _(step):
        give(step).wait_send()


def solution(mesh):
    groups = mesh.shape["expert"]
    row_spec = P(("data", "expert"), None)
    weight_spec = P("expert", None, None)

    def device_step(token_rows, expert_ids, gate_weights, w_in, w_out):
        tokens, top_k = expert_ids.shape
        local, dim, hidden = w_in.shape
        experts = local * groups
        mean_load = tokens * top_k // experts
        capacity = groups * mean_load
        segment = 7 * mean_load // 4
        worst = local * segment
        sizes = [local * mean_load * 18 // 16, local * mean_load * 19 // 16, worst]
        stride = 2 * local * mean_load
        lanes = groups * WIN
        near = groups // 2
        vmem = pl.BlockSpec(memory_space=VMEM)
        anywhere = pl.BlockSpec(memory_space=pl.ANY)

        def params(collective_id):
            return pltpu.CompilerParams(collective_id=collective_id, has_side_effects=True, vmem_limit_bytes=61 * 1024 * 1024)

        pair_sems = [pltpu.SemaphoreType.DMA((groups,)), pltpu.SemaphoreType.DMA((groups,))]
        pos, slot, start, place, rung = pl.pallas_call(
            functools.partial(route_kernel, groups, capacity, sizes, stride, local, near),
            out_shape=[
                jax.ShapeDtypeStruct((top_k, tokens), I32),
                jax.ShapeDtypeStruct((local, lanes), I32),
                jax.ShapeDtypeStruct((local, groups), I32),
                jax.ShapeDtypeStruct((2, local, capacity), I32),
                jax.ShapeDtypeStruct((1, 1), I32),
            ],
            in_specs=[vmem],
            out_specs=[vmem] * 5,
            scratch_shapes=[
                VMEM((groups, top_k, experts), F32),
                VMEM((top_k, experts, 128), F32),
                VMEM((top_k, tokens), F32),
                VMEM((4, groups, experts), F32),
            ]
            + pair_sems,
            compiler_params=params(0),
            name="route",
        )(expert_ids.T)

        def exchange(cap, collective_id):
            depth = 4 if cap == worst else 10

            def run():
                return pl.pallas_call(
                    functools.partial(moe_kernel, groups, cap, stride, local, near, segment),
                    out_shape=jax.ShapeDtypeStruct((tokens, dim), BF16),
                    in_specs=[pl.BlockSpec(memory_space=pltpu.SMEM)] + [vmem] * 4 + [anywhere] * 3,
                    out_specs=vmem,
                    scratch_shapes=[
                        VMEM((tokens, dim), BF16),
                        VMEM((groups, cap // ALIGN, ALIGN, dim), BF16),
                        VMEM(((near * (cap + TAIL) + WIN) // ALIGN, ALIGN, dim), BF16),
                        VMEM((((groups - near) * (cap + TAIL) + WIN) // ALIGN, ALIGN, dim), BF16),
                        VMEM((groups, cap + TAIL, dim), BF16),
                        VMEM((groups, TAIL, dim), BF16),
                        VMEM((groups, cap, dim), BF16),
                        VMEM((depth, dim, hidden), BF16),
                        VMEM((depth, hidden, dim), BF16),
                        VMEM((2, near * WIN, dim), BF16),
                        VMEM((4 * capacity, dim), BF16),
                        VMEM((top_k, tokens, 128), I32),
                        VMEM((top_k, tokens, 128), F32),
                        VMEM((top_k, tokens, dim), BF16),
                        pltpu.SemaphoreType.DMA((2, depth)),
                    ]
                    + pair_sems * 4
                    + [pltpu.SemaphoreType.DMA((3,))],
                    compiler_params=params(collective_id),
                    name="experts",
                )(start, slot, place, pos, gate_weights.T, token_rows, w_in, w_out)

            return run

        return lax.switch(rung.reshape(()), [exchange(cap, 1 + i) for i, cap in enumerate(sizes)])

    return jax.shard_map(device_step, mesh=mesh, in_specs=(row_spec, row_spec, row_spec, weight_spec, weight_spec), out_specs=row_spec, check_vma=False)
```

```python
import functools

import jax
import jax.numpy as jnp
from jax import lax
from jax.experimental import pallas as pl
from jax.experimental.pallas import tpu as pltpu
from jax.sharding import PartitionSpec as P

MESH = pl.DeviceIdType.MESH
VMEM = pltpu.VMEM
F32, BF16, I32 = jnp.float32, jnp.bfloat16, jnp.int32
WIN = 32
ALIGN = 16
TAIL = 48
TOKEN_BLOCK = 256


def iota(shape, dim):
    return lax.broadcasted_iota(I32, shape, dim)


def chips_away(step, chips):
    half = step // 2
    return lax.rem(2 * half + 3 * (half // (chips // 2)), chips)


def peer(me, step, groups):
    chips = groups // 2
    chip = lax.rem(me // 2 + chips_away(step, chips), chips)
    return chip * 2 + lax.rem(me + step, 2)


def source_of(me, step, groups):
    chips = groups // 2
    chip = lax.rem(me // 2 - chips_away(step, chips) + chips, chips)
    return chip * 2 + lax.rem(me + step, 2)


def announce(me, groups):
    barrier = pltpu.get_barrier_semaphore()

    @pl.loop(1, groups)
    def _(step):
        pl.semaphore_signal(barrier, inc=1, device_id={"expert": lax.rem(me + step, groups)}, device_id_type=MESH)

    return barrier


def route_kernel(groups, capacity, sizes, stride, local, near, ids_ref, pos_ref, slot_ref, start_ref, place_ref, rung_ref, cnt, carry, rank, rows, send_sem, recv_sem):
    me = lax.axis_index("expert")
    tokens = ids_ref.shape[1]
    experts = local * groups
    blocks = tokens // TOKEN_BLOCK
    barrier = announce(me, groups)

    expert_rows = iota((experts, TOKEN_BLOCK), 0)
    upper = (iota((TOKEN_BLOCK, TOKEN_BLOCK), 0) <= iota((TOKEN_BLOCK, TOKEN_BLOCK), 1)).astype(BF16)
    carry[...] = jnp.zeros_like(carry)

    @pl.loop(0, blocks)
    def _(b):
        cols = pl.ds(pl.multiple_of(b * TOKEN_BLOCK, TOKEN_BLOCK), TOKEN_BLOCK)
        for j in range(2):
            hot = expert_rows == ids_ref[j : j + 1, cols]
            run = jnp.dot(jnp.where(hot, 1.0, 0.0).astype(BF16), upper, preferred_element_type=F32)
            run = run + jnp.concatenate([carry[j]] * (TOKEN_BLOCK // 128), axis=1)
            rank[j : j + 1, cols] = jnp.sum(jnp.where(hot, run, 0.0), axis=0, keepdims=True) - 1.0
            carry[j] = jnp.broadcast_to(run[:, TOKEN_BLOCK - 1 :], (experts, 128))

    for j in range(2):
        row = jnp.concatenate([carry[j, k : k + 128, :].T[:1] for k in range(0, experts, 128)], axis=1)
        cnt[me, j : j + 1, :] = row

    def send(step):
        to = lax.rem(me + step, groups)
        return pltpu.make_async_remote_copy(src_ref=cnt.at[me], dst_ref=cnt.at[me], send_sem=send_sem.at[step], recv_sem=recv_sem.at[step], device_id={"expert": to}, device_id_type=MESH)

    def arrive(step):
        origin = lax.rem(me - step + groups, groups)
        return pltpu.make_async_remote_copy(src_ref=cnt.at[origin], dst_ref=cnt.at[origin], send_sem=send_sem.at[step], recv_sem=recv_sem.at[step], device_id={"expert": origin}, device_id_type=MESH)

    pl.semaphore_wait(barrier, groups - 1)

    @pl.loop(1, groups)
    def _(step):
        send(step).start()

    @pl.loop(1, groups)
    def _(step):
        arrive(step).wait_recv()

    @pl.loop(1, groups)
    def _(step):
        send(step).wait_send()

    first, second = cnt[:, 0, :], cnt[:, 1, :]
    earlier = (iota((groups, groups), 1) < iota((groups, groups), 0)).astype(BF16)
    before0 = jnp.dot(earlier, first.astype(BF16), preferred_element_type=F32)
    before1 = jnp.dot(earlier, second.astype(BF16), preferred_element_type=F32)
    total0 = jnp.sum(first, axis=0, keepdims=True)
    keep0 = jnp.clip(capacity - before0, 0.0, first)
    keep1 = jnp.clip(capacity - total0 - before1, 0.0, second)
    keep = keep0 + keep1
    keep16 = keep.astype(BF16)
    er, ec = iota((experts, experts), 0), iota((experts, experts), 1)
    mate = er // local - ec // local + 2 * (ec // local % 2)
    same = er // local == ec // local
    load = jnp.dot(keep16, same.astype(BF16), preferred_element_type=F32)
    mate_load = jnp.dot(keep16, (mate == 1).astype(BF16), preferred_element_type=F32)
    inside = jnp.dot(keep16, (same & (er < ec)).astype(BF16), preferred_element_type=F32)
    rung = jnp.zeros((1, 1), F32)
    over = jnp.zeros_like(load)
    size = jnp.full((1, 1), float(sizes[-1]), F32)
    for cap in reversed(sizes[:-1]):
        spill = jnp.maximum(load - cap, 0.0)
        bad = (spill > TAIL) | ((spill > 0.0) & (mate_load + spill > cap))
        good = jnp.max(jnp.max(jnp.where(bad, 1.0, 0.0), axis=1, keepdims=True), axis=0, keepdims=True) == 0.0
        over = jnp.where(good, spill, over)
        size = jnp.where(good, float(cap), size)
        rung = jnp.where(good, rung, rung + 1.0)
    rung_ref[...] = rung.astype(I32)
    offset = TAIL - over + inside
    high = jnp.floor(offset * (1.0 / ALIGN))
    low = offset - high * ALIGN

    rows[0], rows[1], rows[2], rows[3] = high, low, keep0, keep1
    table = jnp.concatenate([rows[i, pl.ds(me, 1), :] for i in range(4)] + [jnp.zeros((4, experts), F32)], axis=0).astype(BF16)
    side = lax.rem(me, 2)

    @pl.loop(0, blocks)
    def _(b):
        cols = pl.ds(pl.multiple_of(b * TOKEN_BLOCK, TOKEN_BLOCK), TOKEN_BLOCK)
        for j in range(2):
            ids = ids_ref[j : j + 1, cols]
            hot16 = jnp.where(expert_rows == ids, 1.0, 0.0).astype(BF16)
            found = jnp.dot(table, hot16, preferred_element_type=F32)
            rk = rank[j : j + 1, cols]
            spot = found[0:1] * ALIGN + found[1:2] + rk
            if j == 1:
                spot = spot + found[2:3]
            owner = ids // local
            half = ((owner + side) % 2).astype(F32)
            direct = spot >= TAIL
            row = jnp.where(direct, half * size + spot - TAIL, (2.0 - half) * size + spot - TAIL)
            key = row.astype(I32) + (owner // 2) * (2 * stride)
            pos_ref[j : j + 1, cols] = jnp.where(rk < found[2 + j : 3 + j], key, -1)

    mine = (iota((local, experts), 1) == iota((local, experts), 0) + me * local).astype(BF16)

    def pick(values):
        return lax.dot_general(mine, values.astype(BF16), (((1,), (1,)), ((), ())), preferred_element_type=F32)

    from_step = (source_of(me, iota((groups, groups), 0), groups) == iota((groups, groups), 1)).astype(BF16)
    older, newer = iota((groups, groups), 1), iota((groups, groups), 0)
    ahead_of = ((older < newer) & ((older < near) == (newer < near))).astype(BF16)

    def by_step(values):
        return jnp.dot(from_step, values.astype(BF16), preferred_element_type=F32)

    kept = by_step(keep)
    ahead = pick(jnp.dot(ahead_of, kept.astype(BF16), preferred_element_type=F32))
    high, low, kept = pick(by_step(high)), pick(by_step(low)), pick(kept)
    start_ref[...] = high.astype(I32)
    lanes = groups * WIN
    spread = (iota((groups, lanes), 1) // WIN == iota((groups, lanes), 0)).astype(BF16)

    def widen(values):
        return jnp.dot(values.astype(BF16), spread, preferred_element_type=F32)

    wide_low, wide_kept, wide_ahead = widen(low), widen(kept), widen(ahead)
    lane = (iota((local, lanes), 1) % WIN).astype(F32)
    valid = (lane >= wide_low) & (lane < wide_low + wide_kept)
    slot_ref[...] = jnp.where(valid, wide_ahead + lane - wide_low, -1.0).astype(I32)
    seat = iota((local, capacity), 1).astype(F32)
    goals = [jnp.full((local, capacity), -1.0, F32) for _ in range(2)]
    for step in range(groups):
        begin, count = ahead[:, step : step + 1], kept[:, step : step + 1]
        spot = high[:, step : step + 1] * ALIGN + low[:, step : step + 1] + step * stride
        part = int(step >= near)
        goals[part] = jnp.where((seat >= begin) & (seat < begin + count), seat - begin + spot, goals[part])
    for part in range(2):
        place_ref[part] = goals[part].astype(I32)


def moe_kernel(groups, cap, stride, local, near, segment, start_ref, slot_ref, place_ref, pos_ref, gate_ref, x_hbm, w_in_hbm, w_out_hbm, out_ref, x_ref, buf, got_a, got_b, outs, tails, ret, w_in, w_out, win, obuf, spots, gates, acc, w_sem, send_sem, recv_sem, back_send, back_recv, tail_send, tail_recv, pass_send, pass_recv, own_sem):
    me = lax.axis_index("expert")
    tokens, dim = x_ref.shape
    depth = w_in.shape[0]
    x_copy = pltpu.make_async_copy(x_hbm, x_ref, own_sem.at[2])
    x_copy.start()
    full = cap + TAIL
    full_blocks, cap_blocks, tail_blocks = full // ALIGN, cap // ALIGN, TAIL // ALIGN
    token_blocks = tokens // TOKEN_BLOCK
    sibling = {"expert": me + 1 - 2 * lax.rem(me, 2)}
    barrier = announce(me, groups)

    def fetch(visit):
        e, place = lax.rem(visit, local), lax.rem(visit, depth)
        return (
            pltpu.make_async_copy(w_in_hbm.at[e], w_in.at[place], w_sem.at[0, place]),
            pltpu.make_async_copy(w_out_hbm.at[e], w_out.at[place], w_sem.at[1, place]),
        )

    for visit in range(depth):
        for copy in fetch(visit):
            copy.start()

    def mate_of(step):
        return step + 1 - 2 * lax.rem(step, 2)

    def push(step, got, first):
        return pltpu.make_async_remote_copy(src_ref=buf.at[step], dst_ref=got.at[pl.ds((step - first) * full_blocks + tail_blocks, cap_blocks)], send_sem=send_sem.at[step], recv_sem=recv_sem.at[step], device_id={"expert": peer(me, step, groups)}, device_id_type=MESH)

    def tail_over(step, got, first):
        return pltpu.make_async_remote_copy(src_ref=got.at[pl.ds((step - first) * full_blocks + cap_blocks, tail_blocks)], dst_ref=got.at[pl.ds((mate_of(step) - first) * full_blocks, tail_blocks)], send_sem=tail_send.at[step], recv_sem=tail_recv.at[mate_of(step)], device_id=sibling, device_id_type=MESH)

    def tail_in(step, got, first):
        return pltpu.make_async_remote_copy(src_ref=got.at[pl.ds((mate_of(step) - first) * full_blocks + cap_blocks, tail_blocks)], dst_ref=got.at[pl.ds((step - first) * full_blocks, tail_blocks)], send_sem=tail_send.at[mate_of(step)], recv_sem=tail_recv.at[step], device_id=sibling, device_id_type=MESH)

    def pass_over(step):
        return pltpu.make_async_remote_copy(src_ref=outs.at[step, pl.ds(0, TAIL)], dst_ref=tails.at[mate_of(step)], send_sem=pass_send.at[step], recv_sem=pass_recv.at[mate_of(step)], device_id=sibling, device_id_type=MESH)

    def pass_in(step):
        return pltpu.make_async_remote_copy(src_ref=outs.at[mate_of(step), pl.ds(0, TAIL)], dst_ref=tails.at[step], send_sem=pass_send.at[mate_of(step)], recv_sem=pass_recv.at[step], device_id=sibling, device_id_type=MESH)

    def berth(step):
        rest = step - (groups - 4)
        return step + step // (groups - 4) * (rest % 2 * 2 + rest // 2 - rest)

    def give(step):
        return pltpu.make_async_remote_copy(src_ref=outs.at[step, pl.ds(TAIL, cap)], dst_ref=ret.at[berth(step)], send_sem=back_send.at[step], recv_sem=back_recv.at[step], device_id={"expert": source_of(me, step, groups)}, device_id_type=MESH)

    def pack(step):
        base = peer(me, step, groups) // 2 * (2 * stride) + lax.rem(step, 2) * cap
        spot = pos_ref[...] - base
        line = iota((cap, tokens), 0)
        hot = (line == spot[0:1]) | (line == spot[1:2])
        rows = jnp.dot(jnp.where(hot, 1.0, 0.0).astype(BF16), x_ref[...], preferred_element_type=F32).astype(BF16)
        buf[step] = rows.reshape(cap_blocks, ALIGN, dim)

    def turn(index):
        third = index % 3
        early = 2 * (2 - third + 3 * (third * (third - 1) // 2)) + index // 3
        later = (index + groups - 6) // groups
        last = (index + 2) // groups
        return index + (1 - later) * (early - index) + 2 * later - groups * last

    x_copy.wait()
    pack(4)
    pl.semaphore_wait(barrier, groups - 1)
    push(4, got_a, 0).start()

    @pl.loop(1, groups)
    def _(index):
        step = turn(index)
        pack(step)

        @pl.when((step > 0) & (step < near))
        def _():
            push(step, got_a, 0).start()

        @pl.when(step >= near)
        def _():
            push(step, got_b, near).start()

    mine = pltpu.make_async_copy(buf.at[0], got_a.at[pl.ds(tail_blocks, cap_blocks)], own_sem.at[0])
    mine.start()
    pad = WIN // ALIGN
    got_a[pl.ds(near * full_blocks, pad)] = jnp.zeros((pad, ALIGN, dim), BF16)
    got_b[pl.ds((groups - near) * full_blocks, pad)] = jnp.zeros((pad, ALIGN, dim), BF16)

    @pl.loop(0, groups)
    def _(step):
        outs[step] = jnp.zeros((full, dim), BF16)

    @pl.loop(0, tokens // 128)
    def _(b):
        at = pl.ds(pl.multiple_of(b * 128, 128), 128)
        for j in range(2):
            spots[j, at, :] = jnp.broadcast_to(pos_ref[j : j + 1, at], (128, 128)).T
            gates[j, at, :] = jnp.broadcast_to(gate_ref[j : j + 1, at], (128, 128)).T
            acc[j, at, :] = jnp.zeros((128, dim), BF16)

    obuf[...] = jnp.zeros_like(obuf)

    def experts(got, first, last, done):
        lanes = (last - first) * WIN
        seats = (last - first) * segment

        quads = local // 4

        @pl.loop(0, quads)
        def _(quad):
            @pl.loop(0, 2)
            def _(twin):
                pair = quad * 2 + twin
                for k in range(2):
                    e = pair * 2 + k
                    for step in range(first, last):
                        row = (step - first) * full_blocks + start_ref[e, step]
                        for half in range(WIN // ALIGN):
                            at = (step - first) * WIN + half * ALIGN
                            win[k, at : at + ALIGN, :] = got[row + half]
                for k in range(2):
                    e = pair * 2 + k
                    visit = done + e
                    place = lax.rem(visit, depth)
                    for copy in fetch(visit):
                        copy.wait()
                    slot = slot_ref[pl.ds(e, 1), :][:, first * WIN : last * WIN]
                    hot = jnp.where(iota((seats, lanes), 0) == slot, 1.0, 0.0).astype(BF16)
                    x = jnp.dot(hot, win[k, :lanes, :], preferred_element_type=F32).astype(BF16)
                    h = jax.nn.gelu(jnp.dot(x, w_in[place], preferred_element_type=F32)).astype(BF16)
                    o = jnp.dot(h, w_out[place], preferred_element_type=F32).astype(BF16)
                    obuf[pl.ds(pl.multiple_of(twin * 256 + k * 128, 128), seats), :] = o
                for k in range(2):
                    visit = done + pair * 2 + k + depth

                    @pl.when(visit < 2 * local)
                    def _():
                        for copy in fetch(visit):
                            copy.start()

            part = 0 if first == 0 else 1
            goal = jnp.concatenate([place_ref[part, pl.ds(quad * 4 + k, 1), :] for k in range(4)], axis=1)

            def place_rows(low, high):
                @pl.loop(first, last)
                def _(step):
                    hot = jnp.where(iota((high - low, 512), 0) == goal - step * stride - low, 1.0, 0.0).astype(BF16)
                    outs[step, low:high] += jnp.dot(hot, obuf[...], preferred_element_type=F32).astype(BF16)

            quarter = TAIL + local // 4 * segment
            middle = TAIL + local // 2 * segment

            @pl.when(quad < quads // 4)
            def _():
                place_rows(0, quarter)

            @pl.when((quad >= quads // 4) & (quad < quads // 2))
            def _():
                place_rows(0, min(middle, full))

            @pl.when(quad >= quads // 2)
            def _():
                place_rows(TAIL, full)

            @pl.when(quad == quads // 2 - 1)
            def _():
                @pl.loop(first, last)
                def _(step):
                    pass_over(step).start()

    def send_back(first, last):
        @pl.loop(first, last)
        def _(step):
            pass_in(step).wait_recv()
            outs[step, cap:, :] += tails[step]

            @pl.when(step > 0)
            def _():
                give(step).start()

    def chip_base(step):
        return peer(me, step, groups) // 2 * (2 * stride)

    def picked(at, returned, lines):
        lane = iota((TOKEN_BLOCK, 128), 1)
        for j in range(2):
            line = lines(spots[j, at, :])
            hot = jnp.concatenate([jnp.where(line - k == lane, 1.0, 0.0).astype(BF16) for k in range(0, 2 * cap, 128)], axis=1)
            yield j, acc[j, at, :] + jnp.dot(hot[:, : 2 * cap], returned, preferred_element_type=F32).astype(BF16)

    def add(first, lines, finish):
        returned = ret[pl.ds(first, 2)].reshape(2 * cap, dim)

        @pl.loop(0, token_blocks)
        def _(b):
            at = pl.ds(pl.multiple_of(b * TOKEN_BLOCK, TOKEN_BLOCK), TOKEN_BLOCK)
            sums = [value for _, value in picked(at, returned, lines)]
            if not finish:
                for j in range(2):
                    acc[j, at, :] = sums[j]
                return
            for c in range(0, dim, 128):
                mixed = x_ref[at, c : c + 128].astype(F32) + gates[0, at, :] * sums[0][:, c : c + 128].astype(F32)
                out_ref[at, c : c + 128] = (mixed + gates[1, at, :] * sums[1][:, c : c + 128].astype(F32)).astype(BF16)

    mine.wait()
    tail_over(0, got_a, 0).start()

    @pl.loop(1, near)
    def _(step):
        push(step, got_a, 0).wait_recv()
        tail_over(step, got_a, 0).start()

    @pl.loop(0, near)
    def _(step):
        tail_in(step, got_a, 0).wait_recv()

    experts(got_a, 0, near, 0)
    send_back(0, near)
    back = pltpu.make_async_copy(outs.at[0, pl.ds(TAIL, cap)], ret.at[0], own_sem.at[1])
    back.start()

    @pl.loop(near, groups)
    def _(step):
        push(step, got_b, near).wait_recv()
        tail_over(step, got_b, near).start()

    @pl.loop(near, groups)
    def _(step):
        tail_in(step, got_b, near).wait_recv()

    experts(got_b, near, groups, local)
    send_back(near, groups)
    back.wait()

    @pl.loop(0, groups // 2 - 2)
    def _(half):
        @pl.when(half > 0)
        def _():
            give(half * 2).wait_recv()

        give(half * 2 + 1).wait_recv()
        base = chip_base(half * 2)
        add(half * 2, lambda spot: spot - base, False)

    for core in range(2):
        steps = [groups - 4 + core, groups - 2 + core]
        for step in steps:
            give(step).wait_recv()
        bases = [chip_base(step) + core * cap for step in steps]

        def lines(spot):
            near_by, other = spot - bases[0], spot - bases[1]
            other = jnp.where((other >= 0) & (other < cap), other + cap, -1)
            return jnp.where((near_by >= 0) & (near_by < cap), near_by, other)

        add(groups - 4 + 2 * core, lines, core == 1)

    @pl.loop(1, near)
    def _(step):
        push(step, got_a, 0).wait_send()

    @pl.loop(near, groups)
    def _(step):
        push(step, got_b, near).wait_send()

    @pl.loop(0, near)
    def _(step):
        tail_over(step, got_a, 0).wait_send()

    @pl.loop(near, groups)
    def _(step):
        tail_over(step, got_b, near).wait_send()

    @pl.loop(0, groups)
    def _(step):
        pass_over(step).wait_send()

    @pl.loop(1, groups)
    def _(step):
        give(step).wait_send()


def solution(mesh):
    groups = mesh.shape["expert"]
    row_spec = P(("data", "expert"), None)
    weight_spec = P("expert", None, None)

    def device_step(token_rows, expert_ids, gate_weights, w_in, w_out):
        tokens, top_k = expert_ids.shape
        local, dim, hidden = w_in.shape
        experts = local * groups
        mean_load = tokens * top_k // experts
        capacity = groups * mean_load
        segment = 7 * mean_load // 4
        worst = local * segment
        sizes = [local * mean_load * 18 // 16, local * mean_load * 19 // 16, worst]
        stride = 2 * local * mean_load
        lanes = groups * WIN
        near = groups // 2
        vmem = pl.BlockSpec(memory_space=VMEM)
        anywhere = pl.BlockSpec(memory_space=pl.ANY)

        def params(collective_id):
            return pltpu.CompilerParams(collective_id=collective_id, has_side_effects=True, vmem_limit_bytes=61 * 1024 * 1024)

        pair_sems = [pltpu.SemaphoreType.DMA((groups,)), pltpu.SemaphoreType.DMA((groups,))]
        pos, slot, start, place, rung = pl.pallas_call(
            functools.partial(route_kernel, groups, capacity, sizes, stride, local, near),
            out_shape=[
                jax.ShapeDtypeStruct((top_k, tokens), I32),
                jax.ShapeDtypeStruct((local, lanes), I32),
                jax.ShapeDtypeStruct((local, groups), I32),
                jax.ShapeDtypeStruct((2, local, capacity), I32),
                jax.ShapeDtypeStruct((1, 1), I32),
            ],
            in_specs=[vmem],
            out_specs=[vmem] * 5,
            scratch_shapes=[
                VMEM((groups, top_k, experts), F32),
                VMEM((top_k, experts, 128), F32),
                VMEM((top_k, tokens), F32),
                VMEM((4, groups, experts), F32),
            ]
            + pair_sems,
            compiler_params=params(0),
            name="route",
        )(expert_ids.T)

        def exchange(cap, collective_id):
            depth = 4 if cap == worst else 10

            def run():
                return pl.pallas_call(
                    functools.partial(moe_kernel, groups, cap, stride, local, near, segment),
                    out_shape=jax.ShapeDtypeStruct((tokens, dim), BF16),
                    in_specs=[pl.BlockSpec(memory_space=pltpu.SMEM)] + [vmem] * 4 + [anywhere] * 3,
                    out_specs=vmem,
                    scratch_shapes=[
                        VMEM((tokens, dim), BF16),
                        VMEM((groups, cap // ALIGN, ALIGN, dim), BF16),
                        VMEM(((near * (cap + TAIL) + WIN) // ALIGN, ALIGN, dim), BF16),
                        VMEM((((groups - near) * (cap + TAIL) + WIN) // ALIGN, ALIGN, dim), BF16),
                        VMEM((groups, cap + TAIL, dim), BF16),
                        VMEM((groups, TAIL, dim), BF16),
                        VMEM((groups, cap, dim), BF16),
                        VMEM((depth, dim, hidden), BF16),
                        VMEM((depth, hidden, dim), BF16),
                        VMEM((2, near * WIN, dim), BF16),
                        VMEM((4 * capacity, dim), BF16),
                        VMEM((top_k, tokens, 128), I32),
                        VMEM((top_k, tokens, 128), F32),
                        VMEM((top_k, tokens, dim), BF16),
                        pltpu.SemaphoreType.DMA((2, depth)),
                    ]
                    + pair_sems * 4
                    + [pltpu.SemaphoreType.DMA((3,))],
                    compiler_params=params(collective_id),
                    name="experts",
                )(start, slot, place, pos, gate_weights.T, token_rows, w_in, w_out)

            return run

        return lax.switch(rung.reshape(()), [exchange(cap, 1 + i) for i, cap in enumerate(sizes)])

    return jax.shard_map(device_step, mesh=mesh, in_specs=(row_spec, row_spec, row_spec, weight_spec, weight_spec), out_specs=row_spec, check_vma=False)
```

```python
import functools

import jax
import jax.numpy as jnp
from jax import lax
from jax.experimental import pallas as pl
from jax.experimental.pallas import tpu as pltpu
from jax.sharding import PartitionSpec as P

MESH = pl.DeviceIdType.MESH
VMEM = pltpu.VMEM
F32, BF16, I32 = jnp.float32, jnp.bfloat16, jnp.int32
WIN = 32
ALIGN = 16
TAIL = 48
TOKEN_BLOCK = 256


def iota(shape, dim):
    return lax.broadcasted_iota(I32, shape, dim)


def chips_away(step, chips):
    half = step // 2
    return lax.rem(2 * half + 3 * (half // (chips // 2)), chips)


def peer(me, step, groups):
    chips = groups // 2
    chip = lax.rem(me // 2 + chips_away(step, chips), chips)
    return chip * 2 + lax.rem(me + step, 2)


def source_of(me, step, groups):
    chips = groups // 2
    chip = lax.rem(me // 2 - chips_away(step, chips) + chips, chips)
    return chip * 2 + lax.rem(me + step, 2)


def announce(me, groups):
    barrier = pltpu.get_barrier_semaphore()

    @pl.loop(1, groups)
    def _(step):
        pl.semaphore_signal(barrier, inc=1, device_id={"expert": lax.rem(me + step, groups)}, device_id_type=MESH)

    return barrier


def route_kernel(groups, capacity, sizes, stride, local, near, ids_ref, pos_ref, slot_ref, start_ref, place_ref, rung_ref, cnt, carry, rank, rows, send_sem, recv_sem):
    me = lax.axis_index("expert")
    tokens = ids_ref.shape[1]
    experts = local * groups
    blocks = tokens // TOKEN_BLOCK
    barrier = announce(me, groups)

    expert_rows = iota((experts, TOKEN_BLOCK), 0)
    upper = (iota((TOKEN_BLOCK, TOKEN_BLOCK), 0) <= iota((TOKEN_BLOCK, TOKEN_BLOCK), 1)).astype(BF16)
    carry[...] = jnp.zeros_like(carry)

    @pl.loop(0, blocks)
    def _(b):
        cols = pl.ds(pl.multiple_of(b * TOKEN_BLOCK, TOKEN_BLOCK), TOKEN_BLOCK)
        for j in range(2):
            hot = expert_rows == ids_ref[j : j + 1, cols]
            run = jnp.dot(jnp.where(hot, 1.0, 0.0).astype(BF16), upper, preferred_element_type=F32)
            run = run + jnp.concatenate([carry[j]] * (TOKEN_BLOCK // 128), axis=1)
            rank[j : j + 1, cols] = jnp.sum(jnp.where(hot, run, 0.0), axis=0, keepdims=True) - 1.0
            carry[j] = jnp.broadcast_to(run[:, TOKEN_BLOCK - 1 :], (experts, 128))

    for j in range(2):
        row = jnp.concatenate([carry[j, k : k + 128, :].T[:1] for k in range(0, experts, 128)], axis=1)
        cnt[me, j : j + 1, :] = row

    def send(step):
        to = lax.rem(me + step, groups)
        return pltpu.make_async_remote_copy(src_ref=cnt.at[me], dst_ref=cnt.at[me], send_sem=send_sem.at[step], recv_sem=recv_sem.at[step], device_id={"expert": to}, device_id_type=MESH)

    def arrive(step):
        origin = lax.rem(me - step + groups, groups)
        return pltpu.make_async_remote_copy(src_ref=cnt.at[origin], dst_ref=cnt.at[origin], send_sem=send_sem.at[step], recv_sem=recv_sem.at[step], device_id={"expert": origin}, device_id_type=MESH)

    pl.semaphore_wait(barrier, groups - 1)

    @pl.loop(1, groups)
    def _(step):
        send(step).start()

    @pl.loop(1, groups)
    def _(step):
        arrive(step).wait_recv()

    @pl.loop(1, groups)
    def _(step):
        send(step).wait_send()

    first, second = cnt[:, 0, :], cnt[:, 1, :]
    earlier = (iota((groups, groups), 1) < iota((groups, groups), 0)).astype(BF16)
    before0 = jnp.dot(earlier, first.astype(BF16), preferred_element_type=F32)
    before1 = jnp.dot(earlier, second.astype(BF16), preferred_element_type=F32)
    total0 = jnp.sum(first, axis=0, keepdims=True)
    keep0 = jnp.clip(capacity - before0, 0.0, first)
    keep1 = jnp.clip(capacity - total0 - before1, 0.0, second)
    keep = keep0 + keep1
    keep16 = keep.astype(BF16)
    er, ec = iota((experts, experts), 0), iota((experts, experts), 1)
    mate = er // local - ec // local + 2 * (ec // local % 2)
    same = er // local == ec // local
    load = jnp.dot(keep16, same.astype(BF16), preferred_element_type=F32)
    mate_load = jnp.dot(keep16, (mate == 1).astype(BF16), preferred_element_type=F32)
    inside = jnp.dot(keep16, (same & (er < ec)).astype(BF16), preferred_element_type=F32)
    rung = jnp.zeros((1, 1), F32)
    over = jnp.zeros_like(load)
    size = jnp.full((1, 1), float(sizes[-1]), F32)
    for cap in reversed(sizes[:-1]):
        spill = jnp.maximum(load - cap, 0.0)
        bad = (spill > TAIL) | ((spill > 0.0) & (mate_load + spill > cap))
        good = jnp.max(jnp.max(jnp.where(bad, 1.0, 0.0), axis=1, keepdims=True), axis=0, keepdims=True) == 0.0
        over = jnp.where(good, spill, over)
        size = jnp.where(good, float(cap), size)
        rung = jnp.where(good, rung, rung + 1.0)
    rung_ref[...] = rung.astype(I32)
    offset = TAIL - over + inside
    high = jnp.floor(offset * (1.0 / ALIGN))
    low = offset - high * ALIGN

    rows[0], rows[1], rows[2], rows[3] = high, low, keep0, keep1
    table = jnp.concatenate([rows[i, pl.ds(me, 1), :] for i in range(4)] + [jnp.zeros((4, experts), F32)], axis=0).astype(BF16)
    side = lax.rem(me, 2)

    @pl.loop(0, blocks)
    def _(b):
        cols = pl.ds(pl.multiple_of(b * TOKEN_BLOCK, TOKEN_BLOCK), TOKEN_BLOCK)
        for j in range(2):
            ids = ids_ref[j : j + 1, cols]
            hot16 = jnp.where(expert_rows == ids, 1.0, 0.0).astype(BF16)
            found = jnp.dot(table, hot16, preferred_element_type=F32)
            rk = rank[j : j + 1, cols]
            spot = found[0:1] * ALIGN + found[1:2] + rk
            if j == 1:
                spot = spot + found[2:3]
            owner = ids // local
            half = ((owner + side) % 2).astype(F32)
            direct = spot >= TAIL
            row = jnp.where(direct, half * size + spot - TAIL, (2.0 - half) * size + spot - TAIL)
            key = row.astype(I32) + (owner // 2) * (2 * stride)
            pos_ref[j : j + 1, cols] = jnp.where(rk < found[2 + j : 3 + j], key, -1)

    mine = (iota((local, experts), 1) == iota((local, experts), 0) + me * local).astype(BF16)

    def pick(values):
        return lax.dot_general(mine, values.astype(BF16), (((1,), (1,)), ((), ())), preferred_element_type=F32)

    from_step = (source_of(me, iota((groups, groups), 0), groups) == iota((groups, groups), 1)).astype(BF16)
    older, newer = iota((groups, groups), 1), iota((groups, groups), 0)
    ahead_of = ((older < newer) & ((older < near) == (newer < near))).astype(BF16)

    def by_step(values):
        return jnp.dot(from_step, values.astype(BF16), preferred_element_type=F32)

    kept = by_step(keep)
    ahead = pick(jnp.dot(ahead_of, kept.astype(BF16), preferred_element_type=F32))
    high, low, kept = pick(by_step(high)), pick(by_step(low)), pick(kept)
    start_ref[...] = high.astype(I32)
    lanes = groups * WIN
    spread = (iota((groups, lanes), 1) // WIN == iota((groups, lanes), 0)).astype(BF16)

    def widen(values):
        return jnp.dot(values.astype(BF16), spread, preferred_element_type=F32)

    wide_low, wide_kept, wide_ahead = widen(low), widen(kept), widen(ahead)
    lane = (iota((local, lanes), 1) % WIN).astype(F32)
    valid = (lane >= wide_low) & (lane < wide_low + wide_kept)
    slot_ref[...] = jnp.where(valid, wide_ahead + lane - wide_low, -1.0).astype(I32)
    seat = iota((local, capacity), 1).astype(F32)
    goals = [jnp.full((local, capacity), -1.0, F32) for _ in range(2)]
    for step in range(groups):
        begin, count = ahead[:, step : step + 1], kept[:, step : step + 1]
        spot = high[:, step : step + 1] * ALIGN + low[:, step : step + 1] + step * stride
        part = int(step >= near)
        goals[part] = jnp.where((seat >= begin) & (seat < begin + count), seat - begin + spot, goals[part])
    for part in range(2):
        place_ref[part] = goals[part].astype(I32)


def moe_kernel(groups, cap, stride, local, near, segment, start_ref, slot_ref, place_ref, pos_ref, gate_ref, x_hbm, w_in_hbm, w_out_hbm, out_ref, x_ref, buf, got_a, got_b, outs, tails, ret, w_in, w_out, win, obuf, spots, gates, acc, w_sem, send_sem, recv_sem, back_send, back_recv, tail_send, tail_recv, pass_send, pass_recv, own_sem):
    me = lax.axis_index("expert")
    tokens, dim = x_ref.shape
    depth = w_in.shape[0]
    x_copy = pltpu.make_async_copy(x_hbm, x_ref, own_sem.at[2])
    x_copy.start()
    full = cap + TAIL
    full_blocks, cap_blocks, tail_blocks = full // ALIGN, cap // ALIGN, TAIL // ALIGN
    token_blocks = tokens // TOKEN_BLOCK
    sibling = {"expert": me + 1 - 2 * lax.rem(me, 2)}
    barrier = announce(me, groups)

    def fetch(visit):
        e, place = lax.rem(visit, local), lax.rem(visit, depth)
        return (
            pltpu.make_async_copy(w_in_hbm.at[e], w_in.at[place], w_sem.at[0, place]),
            pltpu.make_async_copy(w_out_hbm.at[e], w_out.at[place], w_sem.at[1, place]),
        )

    for visit in range(depth):
        for copy in fetch(visit):
            copy.start()

    def mate_of(step):
        return step + 1 - 2 * lax.rem(step, 2)

    def push(step, got, first):
        return pltpu.make_async_remote_copy(src_ref=buf.at[step], dst_ref=got.at[pl.ds((step - first) * full_blocks + tail_blocks, cap_blocks)], send_sem=send_sem.at[step], recv_sem=recv_sem.at[step], device_id={"expert": peer(me, step, groups)}, device_id_type=MESH)

    def tail_over(step, got, first):
        return pltpu.make_async_remote_copy(src_ref=got.at[pl.ds((step - first) * full_blocks + cap_blocks, tail_blocks)], dst_ref=got.at[pl.ds((mate_of(step) - first) * full_blocks, tail_blocks)], send_sem=tail_send.at[step], recv_sem=tail_recv.at[mate_of(step)], device_id=sibling, device_id_type=MESH)

    def tail_in(step, got, first):
        return pltpu.make_async_remote_copy(src_ref=got.at[pl.ds((mate_of(step) - first) * full_blocks + cap_blocks, tail_blocks)], dst_ref=got.at[pl.ds((step - first) * full_blocks, tail_blocks)], send_sem=tail_send.at[mate_of(step)], recv_sem=tail_recv.at[step], device_id=sibling, device_id_type=MESH)

    def pass_over(step):
        return pltpu.make_async_remote_copy(src_ref=outs.at[step, pl.ds(0, TAIL)], dst_ref=tails.at[mate_of(step)], send_sem=pass_send.at[step], recv_sem=pass_recv.at[mate_of(step)], device_id=sibling, device_id_type=MESH)

    def pass_in(step):
        return pltpu.make_async_remote_copy(src_ref=outs.at[mate_of(step), pl.ds(0, TAIL)], dst_ref=tails.at[step], send_sem=pass_send.at[mate_of(step)], recv_sem=pass_recv.at[step], device_id=sibling, device_id_type=MESH)

    def berth(step):
        rest = step - (groups - 4)
        return step + step // (groups - 4) * (rest % 2 * 2 + rest // 2 - rest)

    def give(step):
        return pltpu.make_async_remote_copy(src_ref=outs.at[step, pl.ds(TAIL, cap)], dst_ref=ret.at[berth(step)], send_sem=back_send.at[step], recv_sem=back_recv.at[step], device_id={"expert": source_of(me, step, groups)}, device_id_type=MESH)

    def pack(step):
        base = peer(me, step, groups) // 2 * (2 * stride) + lax.rem(step, 2) * cap
        spot = pos_ref[...] - base
        line = iota((cap, tokens), 0)
        hot = (line == spot[0:1]) | (line == spot[1:2])
        rows = jnp.dot(jnp.where(hot, 1.0, 0.0).astype(BF16), x_ref[...], preferred_element_type=F32).astype(BF16)
        buf[step] = rows.reshape(cap_blocks, ALIGN, dim)

    def turn(index):
        third = index % 3
        early = 2 * (2 - third + 3 * (third * (third - 1) // 2)) + index // 3
        later = (index + groups - 6) // groups
        last = (index + 2) // groups
        return index + (1 - later) * (early - index) + 2 * later - groups * last

    x_copy.wait()
    pack(4)
    pl.semaphore_wait(barrier, groups - 1)
    push(4, got_a, 0).start()

    @pl.loop(1, groups)
    def _(index):
        step = turn(index)
        pack(step)

        @pl.when((step > 0) & (step < near))
        def _():
            push(step, got_a, 0).start()

        @pl.when(step >= near)
        def _():
            push(step, got_b, near).start()

    mine = pltpu.make_async_copy(buf.at[0], got_a.at[pl.ds(tail_blocks, cap_blocks)], own_sem.at[0])
    mine.start()
    pad = WIN // ALIGN
    got_a[pl.ds(near * full_blocks, pad)] = jnp.zeros((pad, ALIGN, dim), BF16)
    got_b[pl.ds((groups - near) * full_blocks, pad)] = jnp.zeros((pad, ALIGN, dim), BF16)

    @pl.loop(0, groups)
    def _(step):
        outs[step] = jnp.zeros((full, dim), BF16)

    @pl.loop(0, tokens // 128)
    def _(b):
        at = pl.ds(pl.multiple_of(b * 128, 128), 128)
        for j in range(2):
            spots[j, at, :] = jnp.broadcast_to(pos_ref[j : j + 1, at], (128, 128)).T
            gates[j, at, :] = jnp.broadcast_to(gate_ref[j : j + 1, at], (128, 128)).T
            acc[j, at, :] = jnp.zeros((128, dim), BF16)

    obuf[...] = jnp.zeros_like(obuf)

    def experts(got, first, last, done):
        lanes = (last - first) * WIN
        seats = (last - first) * segment

        quads = local // 4

        @pl.loop(0, quads)
        def _(quad):
            @pl.loop(0, 2)
            def _(twin):
                pair = quad * 2 + twin
                for k in range(2):
                    e = pair * 2 + k
                    for step in range(first, last):
                        row = (step - first) * full_blocks + start_ref[e, step]
                        for half in range(WIN // ALIGN):
                            at = (step - first) * WIN + half * ALIGN
                            win[k, at : at + ALIGN, :] = got[row + half]
                for k in range(2):
                    e = pair * 2 + k
                    visit = done + e
                    place = lax.rem(visit, depth)
                    for copy in fetch(visit):
                        copy.wait()
                    slot = slot_ref[pl.ds(e, 1), :][:, first * WIN : last * WIN]
                    hot = jnp.where(iota((seats, lanes), 0) == slot, 1.0, 0.0).astype(BF16)
                    x = jnp.dot(hot, win[k, :lanes, :], preferred_element_type=F32).astype(BF16)
                    h = jax.nn.gelu(jnp.dot(x, w_in[place], preferred_element_type=F32)).astype(BF16)
                    o = jnp.dot(h, w_out[place], preferred_element_type=F32).astype(BF16)
                    obuf[pl.ds(pl.multiple_of(twin * 256 + k * 128, 128), seats), :] = o
                for k in range(2):
                    visit = done + pair * 2 + k + depth

                    @pl.when(visit < 2 * local)
                    def _():
                        for copy in fetch(visit):
                            copy.start()

            part = 0 if first == 0 else 1
            goal = jnp.concatenate([place_ref[part, pl.ds(quad * 4 + k, 1), :] for k in range(4)], axis=1)

            def place_rows(low, high):
                @pl.loop(first, last)
                def _(step):
                    hot = jnp.where(iota((high - low, 512), 0) == goal - step * stride - low, 1.0, 0.0).astype(BF16)
                    outs[step, low:high] += jnp.dot(hot, obuf[...], preferred_element_type=F32).astype(BF16)

            quarter = TAIL + local // 4 * segment
            middle = TAIL + local // 2 * segment

            @pl.when(quad < quads // 4)
            def _():
                place_rows(0, quarter)

            @pl.when((quad >= quads // 4) & (quad < quads // 2))
            def _():
                place_rows(0, min(middle, full))

            @pl.when(quad >= quads // 2)
            def _():
                place_rows(TAIL, full)

            @pl.when(quad == quads // 2 - 1)
            def _():
                @pl.loop(first, last)
                def _(step):
                    pass_over(step).start()

    def join(first, last):
        @pl.loop(first, last)
        def _(step):
            pass_in(step).wait_recv()
            outs[step, cap:, :] += tails[step]

    def chip_base(step):
        return peer(me, step, groups) // 2 * (2 * stride)

    def picked(at, returned, lines):
        lane = iota((TOKEN_BLOCK, 128), 1)
        for j in range(2):
            line = lines(spots[j, at, :])
            hot = jnp.concatenate([jnp.where(line - k == lane, 1.0, 0.0).astype(BF16) for k in range(0, 2 * cap, 128)], axis=1)
            yield j, acc[j, at, :] + jnp.dot(hot[:, : 2 * cap], returned, preferred_element_type=F32).astype(BF16)

    def add(first, lines, finish):
        returned = ret[pl.ds(first, 2)].reshape(2 * cap, dim)

        @pl.loop(0, token_blocks)
        def _(b):
            at = pl.ds(pl.multiple_of(b * TOKEN_BLOCK, TOKEN_BLOCK), TOKEN_BLOCK)
            sums = [value for _, value in picked(at, returned, lines)]
            if not finish:
                for j in range(2):
                    acc[j, at, :] = sums[j]
                return
            for c in range(0, dim, 128):
                mixed = x_ref[at, c : c + 128].astype(F32) + gates[0, at, :] * sums[0][:, c : c + 128].astype(F32)
                out_ref[at, c : c + 128] = (mixed + gates[1, at, :] * sums[1][:, c : c + 128].astype(F32)).astype(BF16)

    mine.wait()
    tail_over(0, got_a, 0).start()

    @pl.loop(1, near)
    def _(step):
        push(step, got_a, 0).wait_recv()
        tail_over(step, got_a, 0).start()

    @pl.loop(0, near)
    def _(step):
        tail_in(step, got_a, 0).wait_recv()

    experts(got_a, 0, near, 0)
    join(0, near)
    back = pltpu.make_async_copy(outs.at[0, pl.ds(TAIL, cap)], ret.at[0], own_sem.at[1])
    back.start()

    @pl.loop(near, groups)
    def _(step):
        push(step, got_b, near).wait_recv()
        tail_over(step, got_b, near).start()

    @pl.loop(1, near)
    def _(step):
        give(step).start()

    @pl.loop(near, groups)
    def _(step):
        tail_in(step, got_b, near).wait_recv()

    experts(got_b, near, groups, local)
    join(near, groups)

    @pl.loop(near, groups)
    def _(step):
        give(step).start()

    back.wait()

    @pl.loop(0, groups // 2 - 2)
    def _(half):
        @pl.when(half > 0)
        def _():
            give(half * 2).wait_recv()

        give(half * 2 + 1).wait_recv()
        base = chip_base(half * 2)
        add(half * 2, lambda spot: spot - base, False)

    for core in range(2):
        steps = [groups - 4 + core, groups - 2 + core]
        for step in steps:
            give(step).wait_recv()
        bases = [chip_base(step) + core * cap for step in steps]

        def lines(spot):
            near_by, other = spot - bases[0], spot - bases[1]
            other = jnp.where((other >= 0) & (other < cap), other + cap, -1)
            return jnp.where((near_by >= 0) & (near_by < cap), near_by, other)

        add(groups - 4 + 2 * core, lines, core == 1)

    @pl.loop(1, near)
    def _(step):
        push(step, got_a, 0).wait_send()

    @pl.loop(near, groups)
    def _(step):
        push(step, got_b, near).wait_send()

    @pl.loop(0, near)
    def _(step):
        tail_over(step, got_a, 0).wait_send()

    @pl.loop(near, groups)
    def _(step):
        tail_over(step, got_b, near).wait_send()

    @pl.loop(0, groups)
    def _(step):
        pass_over(step).wait_send()

    @pl.loop(1, groups)
    def _(step):
        give(step).wait_send()


def solution(mesh):
    groups = mesh.shape["expert"]
    row_spec = P(("data", "expert"), None)
    weight_spec = P("expert", None, None)

    def device_step(token_rows, expert_ids, gate_weights, w_in, w_out):
        tokens, top_k = expert_ids.shape
        local, dim, hidden = w_in.shape
        experts = local * groups
        mean_load = tokens * top_k // experts
        capacity = groups * mean_load
        segment = 7 * mean_load // 4
        worst = local * segment
        sizes = [local * mean_load * 18 // 16, local * mean_load * 19 // 16, worst]
        stride = 2 * local * mean_load
        lanes = groups * WIN
        near = groups // 2
        vmem = pl.BlockSpec(memory_space=VMEM)
        anywhere = pl.BlockSpec(memory_space=pl.ANY)

        def params(collective_id):
            return pltpu.CompilerParams(collective_id=collective_id, has_side_effects=True, vmem_limit_bytes=61 * 1024 * 1024)

        pair_sems = [pltpu.SemaphoreType.DMA((groups,)), pltpu.SemaphoreType.DMA((groups,))]
        pos, slot, start, place, rung = pl.pallas_call(
            functools.partial(route_kernel, groups, capacity, sizes, stride, local, near),
            out_shape=[
                jax.ShapeDtypeStruct((top_k, tokens), I32),
                jax.ShapeDtypeStruct((local, lanes), I32),
                jax.ShapeDtypeStruct((local, groups), I32),
                jax.ShapeDtypeStruct((2, local, capacity), I32),
                jax.ShapeDtypeStruct((1, 1), I32),
            ],
            in_specs=[vmem],
            out_specs=[vmem] * 5,
            scratch_shapes=[
                VMEM((groups, top_k, experts), F32),
                VMEM((top_k, experts, 128), F32),
                VMEM((top_k, tokens), F32),
                VMEM((4, groups, experts), F32),
            ]
            + pair_sems,
            compiler_params=params(0),
            name="route",
        )(expert_ids.T)

        def exchange(cap, collective_id):
            depth = 4 if cap == worst else 10

            def run():
                return pl.pallas_call(
                    functools.partial(moe_kernel, groups, cap, stride, local, near, segment),
                    out_shape=jax.ShapeDtypeStruct((tokens, dim), BF16),
                    in_specs=[pl.BlockSpec(memory_space=pltpu.SMEM)] + [vmem] * 4 + [anywhere] * 3,
                    out_specs=vmem,
                    scratch_shapes=[
                        VMEM((tokens, dim), BF16),
                        VMEM((groups, cap // ALIGN, ALIGN, dim), BF16),
                        VMEM(((near * (cap + TAIL) + WIN) // ALIGN, ALIGN, dim), BF16),
                        VMEM((((groups - near) * (cap + TAIL) + WIN) // ALIGN, ALIGN, dim), BF16),
                        VMEM((groups, cap + TAIL, dim), BF16),
                        VMEM((groups, TAIL, dim), BF16),
                        VMEM((groups, cap, dim), BF16),
                        VMEM((depth, dim, hidden), BF16),
                        VMEM((depth, hidden, dim), BF16),
                        VMEM((2, near * WIN, dim), BF16),
                        VMEM((4 * capacity, dim), BF16),
                        VMEM((top_k, tokens, 128), I32),
                        VMEM((top_k, tokens, 128), F32),
                        VMEM((top_k, tokens, dim), BF16),
                        pltpu.SemaphoreType.DMA((2, depth)),
                    ]
                    + pair_sems * 4
                    + [pltpu.SemaphoreType.DMA((3,))],
                    compiler_params=params(collective_id),
                    name="experts",
                )(start, slot, place, pos, gate_weights.T, token_rows, w_in, w_out)

            return run

        return lax.switch(rung.reshape(()), [exchange(cap, 1 + i) for i, cap in enumerate(sizes)])

    return jax.shard_map(device_step, mesh=mesh, in_specs=(row_spec, row_spec, row_spec, weight_spec, weight_spec), out_specs=row_spec, check_vma=False)
```

```python
import functools

import jax
import jax.numpy as jnp
from jax import lax
from jax.experimental import pallas as pl
from jax.experimental.pallas import tpu as pltpu
from jax.sharding import PartitionSpec as P

MESH = pl.DeviceIdType.MESH
VMEM = pltpu.VMEM
F32, BF16, I32 = jnp.float32, jnp.bfloat16, jnp.int32
WIN = 32
ALIGN = 16
TAIL = 48
TOKEN_BLOCK = 256


def iota(shape, dim):
    return lax.broadcasted_iota(I32, shape, dim)


def chips_away(step, chips):
    half = step // 2
    return lax.rem(2 * half + 3 * (half // (chips // 2)), chips)


def peer(me, step, groups):
    chips = groups // 2
    chip = lax.rem(me // 2 + chips_away(step, chips), chips)
    return chip * 2 + lax.rem(me + step, 2)


def source_of(me, step, groups):
    chips = groups // 2
    chip = lax.rem(me // 2 - chips_away(step, chips) + chips, chips)
    return chip * 2 + lax.rem(me + step, 2)


def announce(me, groups):
    barrier = pltpu.get_barrier_semaphore()

    @pl.loop(1, groups)
    def _(step):
        pl.semaphore_signal(barrier, inc=1, device_id={"expert": lax.rem(me + step, groups)}, device_id_type=MESH)

    return barrier


def route_kernel(groups, capacity, sizes, stride, local, near, ids_ref, pos_ref, slot_ref, start_ref, place_ref, rung_ref, cnt, carry, rank, rows, send_sem, recv_sem):
    me = lax.axis_index("expert")
    tokens = ids_ref.shape[1]
    experts = local * groups
    blocks = tokens // TOKEN_BLOCK
    barrier = announce(me, groups)

    expert_rows = iota((experts, TOKEN_BLOCK), 0)
    upper = (iota((TOKEN_BLOCK, TOKEN_BLOCK), 0) <= iota((TOKEN_BLOCK, TOKEN_BLOCK), 1)).astype(BF16)
    carry[...] = jnp.zeros_like(carry)

    @pl.loop(0, blocks)
    def _(b):
        cols = pl.ds(pl.multiple_of(b * TOKEN_BLOCK, TOKEN_BLOCK), TOKEN_BLOCK)
        for j in range(2):
            hot = expert_rows == ids_ref[j : j + 1, cols]
            run = jnp.dot(jnp.where(hot, 1.0, 0.0).astype(BF16), upper, preferred_element_type=F32)
            run = run + jnp.concatenate([carry[j]] * (TOKEN_BLOCK // 128), axis=1)
            rank[j : j + 1, cols] = jnp.sum(jnp.where(hot, run, 0.0), axis=0, keepdims=True) - 1.0
            carry[j] = jnp.broadcast_to(run[:, TOKEN_BLOCK - 1 :], (experts, 128))

    for j in range(2):
        row = jnp.concatenate([carry[j, k : k + 128, :].T[:1] for k in range(0, experts, 128)], axis=1)
        cnt[me, j : j + 1, :] = row

    def send(step):
        to = lax.rem(me + step, groups)
        return pltpu.make_async_remote_copy(src_ref=cnt.at[me], dst_ref=cnt.at[me], send_sem=send_sem.at[step], recv_sem=recv_sem.at[step], device_id={"expert": to}, device_id_type=MESH)

    def arrive(step):
        origin = lax.rem(me - step + groups, groups)
        return pltpu.make_async_remote_copy(src_ref=cnt.at[origin], dst_ref=cnt.at[origin], send_sem=send_sem.at[step], recv_sem=recv_sem.at[step], device_id={"expert": origin}, device_id_type=MESH)

    pl.semaphore_wait(barrier, groups - 1)

    @pl.loop(1, groups)
    def _(step):
        send(step).start()

    @pl.loop(1, groups)
    def _(step):
        arrive(step).wait_recv()

    @pl.loop(1, groups)
    def _(step):
        send(step).wait_send()

    first, second = cnt[:, 0, :], cnt[:, 1, :]
    earlier = (iota((groups, groups), 1) < iota((groups, groups), 0)).astype(BF16)
    before0 = jnp.dot(earlier, first.astype(BF16), preferred_element_type=F32)
    before1 = jnp.dot(earlier, second.astype(BF16), preferred_element_type=F32)
    total0 = jnp.sum(first, axis=0, keepdims=True)
    keep0 = jnp.clip(capacity - before0, 0.0, first)
    keep1 = jnp.clip(capacity - total0 - before1, 0.0, second)
    keep = keep0 + keep1
    keep16 = keep.astype(BF16)
    er, ec = iota((experts, experts), 0), iota((experts, experts), 1)
    mate = er // local - ec // local + 2 * (ec // local % 2)
    same = er // local == ec // local
    load = jnp.dot(keep16, same.astype(BF16), preferred_element_type=F32)
    mate_load = jnp.dot(keep16, (mate == 1).astype(BF16), preferred_element_type=F32)
    inside = jnp.dot(keep16, (same & (er < ec)).astype(BF16), preferred_element_type=F32)
    rung = jnp.zeros((1, 1), F32)
    over = jnp.zeros_like(load)
    size = jnp.full((1, 1), float(sizes[-1]), F32)
    for cap in reversed(sizes[:-1]):
        spill = jnp.maximum(load - cap, 0.0)
        bad = (spill > TAIL) | ((spill > 0.0) & (mate_load + spill > cap))
        good = jnp.max(jnp.max(jnp.where(bad, 1.0, 0.0), axis=1, keepdims=True), axis=0, keepdims=True) == 0.0
        over = jnp.where(good, spill, over)
        size = jnp.where(good, float(cap), size)
        rung = jnp.where(good, rung, rung + 1.0)
    rung_ref[...] = rung.astype(I32)
    offset = TAIL - over + inside
    high = jnp.floor(offset * (1.0 / ALIGN))
    low = offset - high * ALIGN

    rows[0], rows[1], rows[2], rows[3] = high, low, keep0, keep1
    table = jnp.concatenate([rows[i, pl.ds(me, 1), :] for i in range(4)] + [jnp.zeros((4, experts), F32)], axis=0).astype(BF16)
    side = lax.rem(me, 2)

    @pl.loop(0, blocks)
    def _(b):
        cols = pl.ds(pl.multiple_of(b * TOKEN_BLOCK, TOKEN_BLOCK), TOKEN_BLOCK)
        for j in range(2):
            ids = ids_ref[j : j + 1, cols]
            hot16 = jnp.where(expert_rows == ids, 1.0, 0.0).astype(BF16)
            found = jnp.dot(table, hot16, preferred_element_type=F32)
            rk = rank[j : j + 1, cols]
            spot = found[0:1] * ALIGN + found[1:2] + rk
            if j == 1:
                spot = spot + found[2:3]
            owner = ids // local
            half = ((owner + side) % 2).astype(F32)
            direct = spot >= TAIL
            row = jnp.where(direct, half * size + spot - TAIL, (2.0 - half) * size + spot - TAIL)
            key = row.astype(I32) + (owner // 2) * (2 * stride)
            pos_ref[j : j + 1, cols] = jnp.where(rk < found[2 + j : 3 + j], key, -1)

    mine = (iota((local, experts), 1) == iota((local, experts), 0) + me * local).astype(BF16)

    def pick(values):
        return lax.dot_general(mine, values.astype(BF16), (((1,), (1,)), ((), ())), preferred_element_type=F32)

    from_step = (source_of(me, iota((groups, groups), 0), groups) == iota((groups, groups), 1)).astype(BF16)
    older, newer = iota((groups, groups), 1), iota((groups, groups), 0)
    ahead_of = ((older < newer) & ((older < near) == (newer < near))).astype(BF16)

    def by_step(values):
        return jnp.dot(from_step, values.astype(BF16), preferred_element_type=F32)

    kept = by_step(keep)
    ahead = pick(jnp.dot(ahead_of, kept.astype(BF16), preferred_element_type=F32))
    high, low, kept = pick(by_step(high)), pick(by_step(low)), pick(kept)
    start_ref[...] = high.astype(I32)
    lanes = groups * WIN
    spread = (iota((groups, lanes), 1) // WIN == iota((groups, lanes), 0)).astype(BF16)

    def widen(values):
        return jnp.dot(values.astype(BF16), spread, preferred_element_type=F32)

    wide_low, wide_kept, wide_ahead = widen(low), widen(kept), widen(ahead)
    lane = (iota((local, lanes), 1) % WIN).astype(F32)
    valid = (lane >= wide_low) & (lane < wide_low + wide_kept)
    slot_ref[...] = jnp.where(valid, wide_ahead + lane - wide_low, -1.0).astype(I32)
    seat = iota((local, capacity), 1).astype(F32)
    goals = [jnp.full((local, capacity), -1.0, F32) for _ in range(2)]
    for step in range(groups):
        begin, count = ahead[:, step : step + 1], kept[:, step : step + 1]
        spot = high[:, step : step + 1] * ALIGN + low[:, step : step + 1] + step * stride
        part = int(step >= near)
        goals[part] = jnp.where((seat >= begin) & (seat < begin + count), seat - begin + spot, goals[part])
    for part in range(2):
        place_ref[part] = goals[part].astype(I32)


def moe_kernel(groups, cap, stride, local, near, segment, start_ref, slot_ref, place_ref, pos_ref, gate_ref, x_hbm, w_in_hbm, w_out_hbm, out_ref, x_ref, buf, got_a, got_b, outs, tails, ret, w_in, w_out, win, obuf, spots, gates, acc, w_sem, send_sem, recv_sem, back_send, back_recv, tail_send, tail_recv, pass_send, pass_recv, own_sem):
    me = lax.axis_index("expert")
    tokens, dim = x_ref.shape
    depth = w_in.shape[0]
    x_copy = pltpu.make_async_copy(x_hbm, x_ref, own_sem.at[2])
    x_copy.start()
    full = cap + TAIL
    full_blocks, cap_blocks, tail_blocks = full // ALIGN, cap // ALIGN, TAIL // ALIGN
    token_blocks = tokens // TOKEN_BLOCK
    sibling = {"expert": me + 1 - 2 * lax.rem(me, 2)}
    barrier = announce(me, groups)

    def fetch(visit):
        e, place = lax.rem(visit, local), lax.rem(visit, depth)
        return (
            pltpu.make_async_copy(w_in_hbm.at[e], w_in.at[place], w_sem.at[0, place]),
            pltpu.make_async_copy(w_out_hbm.at[e], w_out.at[place], w_sem.at[1, place]),
        )

    for visit in range(depth):
        for copy in fetch(visit):
            copy.start()

    def mate_of(step):
        return step + 1 - 2 * lax.rem(step, 2)

    def push(step, got, first):
        return pltpu.make_async_remote_copy(src_ref=buf.at[step], dst_ref=got.at[pl.ds((step - first) * full_blocks + tail_blocks, cap_blocks)], send_sem=send_sem.at[step], recv_sem=recv_sem.at[step], device_id={"expert": peer(me, step, groups)}, device_id_type=MESH)

    def tail_over(step, got, first):
        return pltpu.make_async_remote_copy(src_ref=got.at[pl.ds((step - first) * full_blocks + cap_blocks, tail_blocks)], dst_ref=got.at[pl.ds((mate_of(step) - first) * full_blocks, tail_blocks)], send_sem=tail_send.at[step], recv_sem=tail_recv.at[mate_of(step)], device_id=sibling, device_id_type=MESH)

    def tail_in(step, got, first):
        return pltpu.make_async_remote_copy(src_ref=got.at[pl.ds((mate_of(step) - first) * full_blocks + cap_blocks, tail_blocks)], dst_ref=got.at[pl.ds((step - first) * full_blocks, tail_blocks)], send_sem=tail_send.at[mate_of(step)], recv_sem=tail_recv.at[step], device_id=sibling, device_id_type=MESH)

    def pass_over(step):
        return pltpu.make_async_remote_copy(src_ref=outs.at[step, pl.ds(0, TAIL)], dst_ref=tails.at[mate_of(step)], send_sem=pass_send.at[step], recv_sem=pass_recv.at[mate_of(step)], device_id=sibling, device_id_type=MESH)

    def pass_in(step):
        return pltpu.make_async_remote_copy(src_ref=outs.at[mate_of(step), pl.ds(0, TAIL)], dst_ref=tails.at[step], send_sem=pass_send.at[mate_of(step)], recv_sem=pass_recv.at[step], device_id=sibling, device_id_type=MESH)

    def berth(step):
        rest = step - (groups - 4)
        return step + step // (groups - 4) * (rest % 2 * 2 + rest // 2 - rest)

    def give(step):
        return pltpu.make_async_remote_copy(src_ref=outs.at[step, pl.ds(TAIL, cap)], dst_ref=ret.at[berth(step)], send_sem=back_send.at[step], recv_sem=back_recv.at[step], device_id={"expert": source_of(me, step, groups)}, device_id_type=MESH)

    def pack(step):
        base = peer(me, step, groups) // 2 * (2 * stride) + lax.rem(step, 2) * cap
        spot = pos_ref[...] - base
        line = iota((cap, tokens), 0)
        hot = (line == spot[0:1]) | (line == spot[1:2])
        rows = jnp.dot(jnp.where(hot, 1.0, 0.0).astype(BF16), x_ref[...], preferred_element_type=F32).astype(BF16)
        buf[step] = rows.reshape(cap_blocks, ALIGN, dim)

    def turn(index):
        third = index % 3
        early = 2 * (2 - third + 3 * (third * (third - 1) // 2)) + index // 3
        later = (index + groups - 6) // groups
        last = (index + 2) // groups
        return index + (1 - later) * (early - index) + 2 * later - groups * last

    x_copy.wait()
    pack(4)
    pl.semaphore_wait(barrier, groups - 1)
    push(4, got_a, 0).start()

    @pl.loop(1, groups)
    def _(index):
        step = turn(index)
        pack(step)

        @pl.when((step > 0) & (step < near))
        def _():
            push(step, got_a, 0).start()

        @pl.when(step >= near)
        def _():
            push(step, got_b, near).start()

    mine = pltpu.make_async_copy(buf.at[0], got_a.at[pl.ds(tail_blocks, cap_blocks)], own_sem.at[0])
    mine.start()
    pad = WIN // ALIGN
    got_a[pl.ds(near * full_blocks, pad)] = jnp.zeros((pad, ALIGN, dim), BF16)
    got_b[pl.ds((groups - near) * full_blocks, pad)] = jnp.zeros((pad, ALIGN, dim), BF16)

    @pl.loop(0, groups)
    def _(step):
        outs[step] = jnp.zeros((full, dim), BF16)

    @pl.loop(0, tokens // 128)
    def _(b):
        at = pl.ds(pl.multiple_of(b * 128, 128), 128)
        for j in range(2):
            spots[j, at, :] = jnp.broadcast_to(pos_ref[j : j + 1, at], (128, 128)).T
            gates[j, at, :] = jnp.broadcast_to(gate_ref[j : j + 1, at], (128, 128)).T
            acc[j, at, :] = jnp.zeros((128, dim), BF16)

    obuf[...] = jnp.zeros_like(obuf)

    def experts(got, first, last, done):
        lanes = (last - first) * WIN
        seats = (last - first) * segment

        quads = local // 4

        @pl.loop(0, quads)
        def _(quad):
            @pl.loop(0, 2)
            def _(twin):
                pair = quad * 2 + twin
                for k in range(2):
                    e = pair * 2 + k
                    for step in range(first, last):
                        row = (step - first) * full_blocks + start_ref[e, step]
                        for half in range(WIN // ALIGN):
                            at = (step - first) * WIN + half * ALIGN
                            win[k, at : at + ALIGN, :] = got[row + half]
                for k in range(2):
                    e = pair * 2 + k
                    visit = done + e
                    place = lax.rem(visit, depth)
                    for copy in fetch(visit):
                        copy.wait()
                    slot = slot_ref[pl.ds(e, 1), :][:, first * WIN : last * WIN]
                    hot = jnp.where(iota((seats, lanes), 0) == slot, 1.0, 0.0).astype(BF16)
                    x = jnp.dot(hot, win[k, :lanes, :], preferred_element_type=F32).astype(BF16)
                    h = jax.nn.gelu(jnp.dot(x, w_in[place], preferred_element_type=F32)).astype(BF16)
                    o = jnp.dot(h, w_out[place], preferred_element_type=F32).astype(BF16)
                    obuf[pl.ds(pl.multiple_of(twin * 256 + k * 128, 128), seats), :] = o
                for k in range(2):
                    visit = done + pair * 2 + k + depth

                    @pl.when(visit < 2 * local)
                    def _():
                        for copy in fetch(visit):
                            copy.start()

            part = 0 if first == 0 else 1
            goal = jnp.concatenate([place_ref[part, pl.ds(quad * 4 + k, 1), :] for k in range(4)], axis=1)

            def place_rows(low, high):
                @pl.loop(first, last)
                def _(step):
                    hot = jnp.where(iota((high - low, 512), 0) == goal - step * stride - low, 1.0, 0.0).astype(BF16)
                    outs[step, low:high] += jnp.dot(hot, obuf[...], preferred_element_type=F32).astype(BF16)

            quarter = TAIL + local // 4 * segment
            middle = TAIL + local // 2 * segment

            @pl.when(quad < quads // 4)
            def _():
                place_rows(0, quarter)

            @pl.when((quad >= quads // 4) & (quad < quads // 2))
            def _():
                place_rows(0, min(middle, full))

            @pl.when(quad >= quads // 2)
            def _():
                place_rows(TAIL, full)

            @pl.when(quad == quads // 2 - 1)
            def _():
                @pl.loop(first, last)
                def _(step):
                    pass_over(step).start()

    def join(first, last):
        @pl.loop(first, last)
        def _(step):
            pass_in(step).wait_recv()
            outs[step, cap:, :] += tails[step]

    def chip_base(step):
        return peer(me, step, groups) // 2 * (2 * stride)

    def picked(at, returned, lines):
        lane = iota((TOKEN_BLOCK, 128), 1)
        for j in range(2):
            line = lines(spots[j, at, :])
            hot = jnp.concatenate([jnp.where(line - k == lane, 1.0, 0.0).astype(BF16) for k in range(0, 2 * cap, 128)], axis=1)
            yield j, acc[j, at, :] + jnp.dot(hot[:, : 2 * cap], returned, preferred_element_type=F32).astype(BF16)

    def add(first, lines, finish):
        returned = ret[pl.ds(first, 2)].reshape(2 * cap, dim)

        @pl.loop(0, token_blocks)
        def _(b):
            at = pl.ds(pl.multiple_of(b * TOKEN_BLOCK, TOKEN_BLOCK), TOKEN_BLOCK)
            sums = [value for _, value in picked(at, returned, lines)]
            if not finish:
                for j in range(2):
                    acc[j, at, :] = sums[j]
                return
            for c in range(0, dim, 128):
                mixed = x_ref[at, c : c + 128].astype(F32) + gates[0, at, :] * sums[0][:, c : c + 128].astype(F32)
                out_ref[at, c : c + 128] = (mixed + gates[1, at, :] * sums[1][:, c : c + 128].astype(F32)).astype(BF16)

    mine.wait()
    tail_over(0, got_a, 0).start()

    @pl.loop(1, near)
    def _(step):
        push(step, got_a, 0).wait_recv()
        tail_over(step, got_a, 0).start()

    @pl.loop(0, near)
    def _(step):
        tail_in(step, got_a, 0).wait_recv()

    experts(got_a, 0, near, 0)
    join(0, near)
    back = pltpu.make_async_copy(outs.at[0, pl.ds(TAIL, cap)], ret.at[0], own_sem.at[1])
    back.start()

    def arrive(step):
        push(step, got_b, near).wait_recv()
        tail_over(step, got_b, near).start()

    @pl.loop(near, groups - 4)
    def _(step):
        arrive(step)

    arrive(groups - 4)
    arrive(groups - 2)

    @pl.loop(1, near)
    def _(step):
        give(step).start()

    arrive(groups - 3)
    arrive(groups - 1)

    @pl.loop(near, groups)
    def _(step):
        tail_in(step, got_b, near).wait_recv()

    experts(got_b, near, groups, local)
    join(near, groups)

    @pl.loop(near, groups)
    def _(step):
        give(step).start()

    back.wait()

    @pl.loop(0, groups // 2 - 2)
    def _(half):
        @pl.when(half > 0)
        def _():
            give(half * 2).wait_recv()

        give(half * 2 + 1).wait_recv()
        base = chip_base(half * 2)
        add(half * 2, lambda spot: spot - base, False)

    for core in range(2):
        steps = [groups - 4 + core, groups - 2 + core]
        for step in steps:
            give(step).wait_recv()
        bases = [chip_base(step) + core * cap for step in steps]

        def lines(spot):
            near_by, other = spot - bases[0], spot - bases[1]
            other = jnp.where((other >= 0) & (other < cap), other + cap, -1)
            return jnp.where((near_by >= 0) & (near_by < cap), near_by, other)

        add(groups - 4 + 2 * core, lines, core == 1)

    @pl.loop(1, near)
    def _(step):
        push(step, got_a, 0).wait_send()

    @pl.loop(near, groups)
    def _(step):
        push(step, got_b, near).wait_send()

    @pl.loop(0, near)
    def _(step):
        tail_over(step, got_a, 0).wait_send()

    @pl.loop(near, groups)
    def _(step):
        tail_over(step, got_b, near).wait_send()

    @pl.loop(0, groups)
    def _(step):
        pass_over(step).wait_send()

    @pl.loop(1, groups)
    def _(step):
        give(step).wait_send()


def solution(mesh):
    groups = mesh.shape["expert"]
    row_spec = P(("data", "expert"), None)
    weight_spec = P("expert", None, None)

    def device_step(token_rows, expert_ids, gate_weights, w_in, w_out):
        tokens, top_k = expert_ids.shape
        local, dim, hidden = w_in.shape
        experts = local * groups
        mean_load = tokens * top_k // experts
        capacity = groups * mean_load
        segment = 7 * mean_load // 4
        worst = local * segment
        sizes = [local * mean_load * 18 // 16, local * mean_load * 19 // 16, worst]
        stride = 2 * local * mean_load
        lanes = groups * WIN
        near = groups // 2
        vmem = pl.BlockSpec(memory_space=VMEM)
        anywhere = pl.BlockSpec(memory_space=pl.ANY)

        def params(collective_id):
            return pltpu.CompilerParams(collective_id=collective_id, has_side_effects=True, vmem_limit_bytes=61 * 1024 * 1024)

        pair_sems = [pltpu.SemaphoreType.DMA((groups,)), pltpu.SemaphoreType.DMA((groups,))]
        pos, slot, start, place, rung = pl.pallas_call(
            functools.partial(route_kernel, groups, capacity, sizes, stride, local, near),
            out_shape=[
                jax.ShapeDtypeStruct((top_k, tokens), I32),
                jax.ShapeDtypeStruct((local, lanes), I32),
                jax.ShapeDtypeStruct((local, groups), I32),
                jax.ShapeDtypeStruct((2, local, capacity), I32),
                jax.ShapeDtypeStruct((1, 1), I32),
            ],
            in_specs=[vmem],
            out_specs=[vmem] * 5,
            scratch_shapes=[
                VMEM((groups, top_k, experts), F32),
                VMEM((top_k, experts, 128), F32),
                VMEM((top_k, tokens), F32),
                VMEM((4, groups, experts), F32),
            ]
            + pair_sems,
            compiler_params=params(0),
            name="route",
        )(expert_ids.T)

        def exchange(cap, collective_id):
            depth = 4 if cap == worst else 10

            def run():
                return pl.pallas_call(
                    functools.partial(moe_kernel, groups, cap, stride, local, near, segment),
                    out_shape=jax.ShapeDtypeStruct((tokens, dim), BF16),
                    in_specs=[pl.BlockSpec(memory_space=pltpu.SMEM)] + [vmem] * 4 + [anywhere] * 3,
                    out_specs=vmem,
                    scratch_shapes=[
                        VMEM((tokens, dim), BF16),
                        VMEM((groups, cap // ALIGN, ALIGN, dim), BF16),
                        VMEM(((near * (cap + TAIL) + WIN) // ALIGN, ALIGN, dim), BF16),
                        VMEM((((groups - near) * (cap + TAIL) + WIN) // ALIGN, ALIGN, dim), BF16),
                        VMEM((groups, cap + TAIL, dim), BF16),
                        VMEM((groups, TAIL, dim), BF16),
                        VMEM((groups, cap, dim), BF16),
                        VMEM((depth, dim, hidden), BF16),
                        VMEM((depth, hidden, dim), BF16),
                        VMEM((2, near * WIN, dim), BF16),
                        VMEM((4 * capacity, dim), BF16),
                        VMEM((top_k, tokens, 128), I32),
                        VMEM((top_k, tokens, 128), F32),
                        VMEM((top_k, tokens, dim), BF16),
                        pltpu.SemaphoreType.DMA((2, depth)),
                    ]
                    + pair_sems * 4
                    + [pltpu.SemaphoreType.DMA((3,))],
                    compiler_params=params(collective_id),
                    name="experts",
                )(start, slot, place, pos, gate_weights.T, token_rows, w_in, w_out)

            return run

        return lax.switch(rung.reshape(()), [exchange(cap, 1 + i) for i, cap in enumerate(sizes)])

    return jax.shard_map(device_step, mesh=mesh, in_specs=(row_spec, row_spec, row_spec, weight_spec, weight_spec), out_specs=row_spec, check_vma=False)
```

```python
import functools

import jax
import jax.numpy as jnp
from jax import lax
from jax.experimental import pallas as pl
from jax.experimental.pallas import tpu as pltpu
from jax.sharding import PartitionSpec as P

MESH = pl.DeviceIdType.MESH
VMEM = pltpu.VMEM
F32, BF16, I32 = jnp.float32, jnp.bfloat16, jnp.int32
WIN = 32
ALIGN = 16
TAIL = 48
TOKEN_BLOCK = 256


def iota(shape, dim):
    return lax.broadcasted_iota(I32, shape, dim)


def chips_away(step, chips):
    half = step // 2
    return lax.rem(2 * half + 3 * (half // (chips // 2)), chips)


def peer(me, step, groups):
    chips = groups // 2
    chip = lax.rem(me // 2 + chips_away(step, chips), chips)
    return chip * 2 + lax.rem(me + step, 2)


def source_of(me, step, groups):
    chips = groups // 2
    chip = lax.rem(me // 2 - chips_away(step, chips) + chips, chips)
    return chip * 2 + lax.rem(me + step, 2)


def announce(me, groups):
    barrier = pltpu.get_barrier_semaphore()

    @pl.loop(1, groups)
    def _(step):
        pl.semaphore_signal(barrier, inc=1, device_id={"expert": lax.rem(me + step, groups)}, device_id_type=MESH)

    return barrier


def route_kernel(groups, capacity, sizes, stride, local, near, ids_ref, pos_ref, slot_ref, start_ref, place_ref, rung_ref, cnt, carry, rank, rows, send_sem, recv_sem):
    me = lax.axis_index("expert")
    tokens = ids_ref.shape[1]
    experts = local * groups
    blocks = tokens // TOKEN_BLOCK
    barrier = announce(me, groups)

    expert_rows = iota((experts, TOKEN_BLOCK), 0)
    upper = (iota((TOKEN_BLOCK, TOKEN_BLOCK), 0) <= iota((TOKEN_BLOCK, TOKEN_BLOCK), 1)).astype(BF16)
    carry[...] = jnp.zeros_like(carry)

    @pl.loop(0, blocks)
    def _(b):
        cols = pl.ds(pl.multiple_of(b * TOKEN_BLOCK, TOKEN_BLOCK), TOKEN_BLOCK)
        for j in range(2):
            hot = expert_rows == ids_ref[j : j + 1, cols]
            run = jnp.dot(jnp.where(hot, 1.0, 0.0).astype(BF16), upper, preferred_element_type=F32)
            run = run + jnp.concatenate([carry[j]] * (TOKEN_BLOCK // 128), axis=1)
            rank[j : j + 1, cols] = jnp.sum(jnp.where(hot, run, 0.0), axis=0, keepdims=True) - 1.0
            carry[j] = jnp.broadcast_to(run[:, TOKEN_BLOCK - 1 :], (experts, 128))

    for j in range(2):
        row = jnp.concatenate([carry[j, k : k + 128, :].T[:1] for k in range(0, experts, 128)], axis=1)
        cnt[me, j : j + 1, :] = row

    def send(step):
        to = lax.rem(me + step, groups)
        return pltpu.make_async_remote_copy(src_ref=cnt.at[me], dst_ref=cnt.at[me], send_sem=send_sem.at[step], recv_sem=recv_sem.at[step], device_id={"expert": to}, device_id_type=MESH)

    def arrive(step):
        origin = lax.rem(me - step + groups, groups)
        return pltpu.make_async_remote_copy(src_ref=cnt.at[origin], dst_ref=cnt.at[origin], send_sem=send_sem.at[step], recv_sem=recv_sem.at[step], device_id={"expert": origin}, device_id_type=MESH)

    pl.semaphore_wait(barrier, groups - 1)

    @pl.loop(1, groups)
    def _(step):
        send(step).start()

    @pl.loop(1, groups)
    def _(step):
        arrive(step).wait_recv()

    @pl.loop(1, groups)
    def _(step):
        send(step).wait_send()

    first, second = cnt[:, 0, :], cnt[:, 1, :]
    earlier = (iota((groups, groups), 1) < iota((groups, groups), 0)).astype(BF16)
    before0 = jnp.dot(earlier, first.astype(BF16), preferred_element_type=F32)
    before1 = jnp.dot(earlier, second.astype(BF16), preferred_element_type=F32)
    total0 = jnp.sum(first, axis=0, keepdims=True)
    keep0 = jnp.clip(capacity - before0, 0.0, first)
    keep1 = jnp.clip(capacity - total0 - before1, 0.0, second)
    keep = keep0 + keep1
    keep16 = keep.astype(BF16)
    er, ec = iota((experts, experts), 0), iota((experts, experts), 1)
    mate = er // local - ec // local + 2 * (ec // local % 2)
    same = er // local == ec // local
    load = jnp.dot(keep16, same.astype(BF16), preferred_element_type=F32)
    mate_load = jnp.dot(keep16, (mate == 1).astype(BF16), preferred_element_type=F32)
    inside = jnp.dot(keep16, (same & (er < ec)).astype(BF16), preferred_element_type=F32)
    rung = jnp.zeros((1, 1), F32)
    over = jnp.zeros_like(load)
    size = jnp.full((1, 1), float(sizes[-1]), F32)
    for cap in reversed(sizes[:-1]):
        spill = jnp.maximum(load - cap, 0.0)
        bad = (spill > TAIL) | ((spill > 0.0) & (mate_load + spill > cap))
        good = jnp.max(jnp.max(jnp.where(bad, 1.0, 0.0), axis=1, keepdims=True), axis=0, keepdims=True) == 0.0
        over = jnp.where(good, spill, over)
        size = jnp.where(good, float(cap), size)
        rung = jnp.where(good, rung, rung + 1.0)
    rung_ref[...] = rung.astype(I32)
    offset = TAIL - over + inside
    high = jnp.floor(offset * (1.0 / ALIGN))
    low = offset - high * ALIGN

    rows[0], rows[1], rows[2], rows[3] = high, low, keep0, keep1
    table = jnp.concatenate([rows[i, pl.ds(me, 1), :] for i in range(4)] + [jnp.zeros((4, experts), F32)], axis=0).astype(BF16)
    side = lax.rem(me, 2)

    @pl.loop(0, blocks)
    def _(b):
        cols = pl.ds(pl.multiple_of(b * TOKEN_BLOCK, TOKEN_BLOCK), TOKEN_BLOCK)
        for j in range(2):
            ids = ids_ref[j : j + 1, cols]
            hot16 = jnp.where(expert_rows == ids, 1.0, 0.0).astype(BF16)
            found = jnp.dot(table, hot16, preferred_element_type=F32)
            rk = rank[j : j + 1, cols]
            spot = found[0:1] * ALIGN + found[1:2] + rk
            if j == 1:
                spot = spot + found[2:3]
            owner = ids // local
            half = ((owner + side) % 2).astype(F32)
            direct = spot >= TAIL
            row = jnp.where(direct, half * size + spot - TAIL, (2.0 - half) * size + spot - TAIL)
            key = row.astype(I32) + (owner // 2) * (2 * stride)
            pos_ref[j : j + 1, cols] = jnp.where(rk < found[2 + j : 3 + j], key, -1)

    mine = (iota((local, experts), 1) == iota((local, experts), 0) + me * local).astype(BF16)

    def pick(values):
        return lax.dot_general(mine, values.astype(BF16), (((1,), (1,)), ((), ())), preferred_element_type=F32)

    from_step = (source_of(me, iota((groups, groups), 0), groups) == iota((groups, groups), 1)).astype(BF16)
    older, newer = iota((groups, groups), 1), iota((groups, groups), 0)
    ahead_of = ((older < newer) & ((older < near) == (newer < near))).astype(BF16)

    def by_step(values):
        return jnp.dot(from_step, values.astype(BF16), preferred_element_type=F32)

    kept = by_step(keep)
    ahead = pick(jnp.dot(ahead_of, kept.astype(BF16), preferred_element_type=F32))
    high, low, kept = pick(by_step(high)), pick(by_step(low)), pick(kept)
    start_ref[...] = high.astype(I32)
    lanes = groups * WIN
    spread = (iota((groups, lanes), 1) // WIN == iota((groups, lanes), 0)).astype(BF16)

    def widen(values):
        return jnp.dot(values.astype(BF16), spread, preferred_element_type=F32)

    wide_low, wide_kept, wide_ahead = widen(low), widen(kept), widen(ahead)
    lane = (iota((local, lanes), 1) % WIN).astype(F32)
    valid = (lane >= wide_low) & (lane < wide_low + wide_kept)
    slot_ref[...] = jnp.where(valid, wide_ahead + lane - wide_low, -1.0).astype(I32)
    seat = iota((local, capacity), 1).astype(F32)
    goals = [jnp.full((local, capacity), -1.0, F32) for _ in range(2)]
    for step in range(groups):
        begin, count = ahead[:, step : step + 1], kept[:, step : step + 1]
        spot = high[:, step : step + 1] * ALIGN + low[:, step : step + 1] + step * stride
        part = int(step >= near)
        goals[part] = jnp.where((seat >= begin) & (seat < begin + count), seat - begin + spot, goals[part])
    for part in range(2):
        place_ref[part] = goals[part].astype(I32)


def moe_kernel(groups, cap, stride, local, near, segment, start_ref, slot_ref, place_ref, pos_ref, gate_ref, x_hbm, w_in_hbm, w_out_hbm, out_ref, x_ref, buf, got_a, got_b, outs, tails, ret, w_in, w_out, win, obuf, spots, gates, acc, w_sem, send_sem, recv_sem, back_send, back_recv, tail_send, tail_recv, pass_send, pass_recv, own_sem):
    me = lax.axis_index("expert")
    tokens, dim = x_ref.shape
    depth = w_in.shape[0]
    x_copy = pltpu.make_async_copy(x_hbm, x_ref, own_sem.at[2])
    x_copy.start()
    full = cap + TAIL
    full_blocks, cap_blocks, tail_blocks = full // ALIGN, cap // ALIGN, TAIL // ALIGN
    token_blocks = tokens // TOKEN_BLOCK
    sibling = {"expert": me + 1 - 2 * lax.rem(me, 2)}
    barrier = announce(me, groups)

    def fetch(visit):
        e, place = lax.rem(visit, local), lax.rem(visit, depth)
        return (
            pltpu.make_async_copy(w_in_hbm.at[e], w_in.at[place], w_sem.at[0, place]),
            pltpu.make_async_copy(w_out_hbm.at[e], w_out.at[place], w_sem.at[1, place]),
        )

    for visit in range(depth):
        for copy in fetch(visit):
            copy.start()

    def mate_of(step):
        return step + 1 - 2 * lax.rem(step, 2)

    def push(step, got, first):
        return pltpu.make_async_remote_copy(src_ref=buf.at[step], dst_ref=got.at[pl.ds((step - first) * full_blocks + tail_blocks, cap_blocks)], send_sem=send_sem.at[step], recv_sem=recv_sem.at[step], device_id={"expert": peer(me, step, groups)}, device_id_type=MESH)

    def tail_over(step, got, first):
        return pltpu.make_async_remote_copy(src_ref=got.at[pl.ds((step - first) * full_blocks + cap_blocks, tail_blocks)], dst_ref=got.at[pl.ds((mate_of(step) - first) * full_blocks, tail_blocks)], send_sem=tail_send.at[step], recv_sem=tail_recv.at[mate_of(step)], device_id=sibling, device_id_type=MESH)

    def tail_in(step, got, first):
        return pltpu.make_async_remote_copy(src_ref=got.at[pl.ds((mate_of(step) - first) * full_blocks + cap_blocks, tail_blocks)], dst_ref=got.at[pl.ds((step - first) * full_blocks, tail_blocks)], send_sem=tail_send.at[mate_of(step)], recv_sem=tail_recv.at[step], device_id=sibling, device_id_type=MESH)

    def pass_over(step):
        return pltpu.make_async_remote_copy(src_ref=outs.at[step, pl.ds(0, TAIL)], dst_ref=tails.at[mate_of(step)], send_sem=pass_send.at[step], recv_sem=pass_recv.at[mate_of(step)], device_id=sibling, device_id_type=MESH)

    def pass_in(step):
        return pltpu.make_async_remote_copy(src_ref=outs.at[mate_of(step), pl.ds(0, TAIL)], dst_ref=tails.at[step], send_sem=pass_send.at[mate_of(step)], recv_sem=pass_recv.at[step], device_id=sibling, device_id_type=MESH)

    def berth(step):
        rest = step - (groups - 4)
        return step + step // (groups - 4) * (rest % 2 * 2 + rest // 2 - rest)

    def give(step):
        return pltpu.make_async_remote_copy(src_ref=outs.at[step, pl.ds(TAIL, cap)], dst_ref=ret.at[berth(step)], send_sem=back_send.at[step], recv_sem=back_recv.at[step], device_id={"expert": source_of(me, step, groups)}, device_id_type=MESH)

    def pack(step):
        base = peer(me, step, groups) // 2 * (2 * stride) + lax.rem(step, 2) * cap
        spot = pos_ref[...] - base
        line = iota((cap, tokens), 0)
        hot = (line == spot[0:1]) | (line == spot[1:2])
        rows = jnp.dot(jnp.where(hot, 1.0, 0.0).astype(BF16), x_ref[...], preferred_element_type=F32).astype(BF16)
        buf[step] = rows.reshape(cap_blocks, ALIGN, dim)

    def turn(index):
        third = index % 3
        early = 2 * (2 - third + 3 * (third * (third - 1) // 2)) + index // 3
        later = (index + groups - 6) // groups
        last = (index + 2) // groups
        return index + (1 - later) * (early - index) + 2 * later - groups * last

    x_copy.wait()
    pack(4)
    pl.semaphore_wait(barrier, groups - 1)
    push(4, got_a, 0).start()

    @pl.loop(1, groups)
    def _(index):
        step = turn(index)
        pack(step)

        @pl.when((step > 0) & (step < near))
        def _():
            push(step, got_a, 0).start()

        @pl.when(step >= near)
        def _():
            push(step, got_b, near).start()

    mine = pltpu.make_async_copy(buf.at[0], got_a.at[pl.ds(tail_blocks, cap_blocks)], own_sem.at[0])
    mine.start()
    pad = WIN // ALIGN
    got_a[pl.ds(near * full_blocks, pad)] = jnp.zeros((pad, ALIGN, dim), BF16)
    got_b[pl.ds((groups - near) * full_blocks, pad)] = jnp.zeros((pad, ALIGN, dim), BF16)

    @pl.loop(0, groups)
    def _(step):
        outs[step] = jnp.zeros((full, dim), BF16)

    @pl.loop(0, tokens // 128)
    def _(b):
        at = pl.ds(pl.multiple_of(b * 128, 128), 128)
        for j in range(2):
            spots[j, at, :] = jnp.broadcast_to(pos_ref[j : j + 1, at], (128, 128)).T
            gates[j, at, :] = jnp.broadcast_to(gate_ref[j : j + 1, at], (128, 128)).T
            acc[j, at, :] = jnp.zeros((128, dim), BF16)

    obuf[...] = jnp.zeros_like(obuf)

    def experts(got, first, last, done):
        lanes = (last - first) * WIN
        seats = (last - first) * segment

        quads = local // 4

        @pl.loop(0, quads)
        def _(quad):
            @pl.loop(0, 2)
            def _(twin):
                pair = quad * 2 + twin
                for k in range(2):
                    e = pair * 2 + k
                    for step in range(first, last):
                        row = (step - first) * full_blocks + start_ref[e, step]
                        for half in range(WIN // ALIGN):
                            at = (step - first) * WIN + half * ALIGN
                            win[k, at : at + ALIGN, :] = got[row + half]
                for k in range(2):
                    e = pair * 2 + k
                    visit = done + e
                    place = lax.rem(visit, depth)
                    for copy in fetch(visit):
                        copy.wait()
                    slot = slot_ref[pl.ds(e, 1), :][:, first * WIN : last * WIN]
                    hot = jnp.where(iota((seats, lanes), 0) == slot, 1.0, 0.0).astype(BF16)
                    x = jnp.dot(hot, win[k, :lanes, :], preferred_element_type=F32).astype(BF16)
                    h = jax.nn.gelu(jnp.dot(x, w_in[place], preferred_element_type=F32)).astype(BF16)
                    o = jnp.dot(h, w_out[place], preferred_element_type=F32).astype(BF16)
                    obuf[pl.ds(pl.multiple_of(twin * 256 + k * 128, 128), seats), :] = o
                for k in range(2):
                    visit = done + pair * 2 + k + depth

                    @pl.when(visit < 2 * local)
                    def _():
                        for copy in fetch(visit):
                            copy.start()

            part = 0 if first == 0 else 1
            goal = jnp.concatenate([place_ref[part, pl.ds(quad * 4 + k, 1), :] for k in range(4)], axis=1)

            def place_rows(low, high):
                @pl.loop(first, last)
                def _(step):
                    hot = jnp.where(iota((high - low, 512), 0) == goal - step * stride - low, 1.0, 0.0).astype(BF16)
                    outs[step, low:high] += jnp.dot(hot, obuf[...], preferred_element_type=F32).astype(BF16)

            quarter = TAIL + local // 4 * segment
            middle = TAIL + local // 2 * segment

            @pl.when(quad < quads // 4)
            def _():
                place_rows(0, quarter)

            @pl.when((quad >= quads // 4) & (quad < quads // 2))
            def _():
                place_rows(0, min(middle, full))

            @pl.when(quad >= quads // 2)
            def _():
                place_rows(TAIL, full)

            @pl.when(quad == quads // 2 - 1)
            def _():
                @pl.loop(first, last)
                def _(step):
                    pass_over(step).start()

    def join(first, last):
        @pl.loop(first, last)
        def _(step):
            pass_in(step).wait_recv()
            outs[step, cap:, :] += tails[step]

    def chip_base(step):
        return peer(me, step, groups) // 2 * (2 * stride)

    def picked(at, returned, lines):
        lane = iota((TOKEN_BLOCK, 128), 1)
        for j in range(2):
            line = lines(spots[j, at, :])
            hot = jnp.concatenate([jnp.where(line - k == lane, 1.0, 0.0).astype(BF16) for k in range(0, 2 * cap, 128)], axis=1)
            yield j, acc[j, at, :] + jnp.dot(hot[:, : 2 * cap], returned, preferred_element_type=F32).astype(BF16)

    def add(first, lines, finish):
        returned = ret[pl.ds(first, 2)].reshape(2 * cap, dim)

        @pl.loop(0, token_blocks)
        def _(b):
            at = pl.ds(pl.multiple_of(b * TOKEN_BLOCK, TOKEN_BLOCK), TOKEN_BLOCK)
            sums = [value for _, value in picked(at, returned, lines)]
            if not finish:
                for j in range(2):
                    acc[j, at, :] = sums[j]
                return
            for c in range(0, dim, 128):
                mixed = x_ref[at, c : c + 128].astype(F32) + gates[0, at, :] * sums[0][:, c : c + 128].astype(F32)
                out_ref[at, c : c + 128] = (mixed + gates[1, at, :] * sums[1][:, c : c + 128].astype(F32)).astype(BF16)

    mine.wait()
    tail_over(0, got_a, 0).start()

    @pl.loop(1, near)
    def _(step):
        push(step, got_a, 0).wait_recv()
        tail_over(step, got_a, 0).start()

    @pl.loop(0, near)
    def _(step):
        tail_in(step, got_a, 0).wait_recv()

    experts(got_a, 0, near, 0)
    join(0, near)
    back = pltpu.make_async_copy(outs.at[0, pl.ds(TAIL, cap)], ret.at[0], own_sem.at[1])
    back.start()

    @pl.loop(near, groups)
    def _(step):
        push(step, got_b, near).wait_recv()
        tail_over(step, got_b, near).start()

    @pl.loop(1, near)
    def _(step):
        give(step).start()

    @pl.loop(near, groups)
    def _(step):
        tail_in(step, got_b, near).wait_recv()

    experts(got_b, near, groups, local)
    join(near, groups)

    @pl.loop(1, near)
    def _(step):
        give(step).wait_recv()

    @pl.loop(near, groups)
    def _(step):
        give(step).start()

    back.wait()

    @pl.loop(0, groups // 2 - 2)
    def _(half):
        @pl.when(half >= near // 2)
        def _():
            give(half * 2).wait_recv()
            give(half * 2 + 1).wait_recv()

        base = chip_base(half * 2)
        add(half * 2, lambda spot: spot - base, False)

    for core in range(2):
        steps = [groups - 4 + core, groups - 2 + core]
        for step in steps:
            give(step).wait_recv()
        bases = [chip_base(step) + core * cap for step in steps]

        def lines(spot):
            near_by, other = spot - bases[0], spot - bases[1]
            other = jnp.where((other >= 0) & (other < cap), other + cap, -1)
            return jnp.where((near_by >= 0) & (near_by < cap), near_by, other)

        add(groups - 4 + 2 * core, lines, core == 1)

    @pl.loop(1, near)
    def _(step):
        push(step, got_a, 0).wait_send()

    @pl.loop(near, groups)
    def _(step):
        push(step, got_b, near).wait_send()

    @pl.loop(0, near)
    def _(step):
        tail_over(step, got_a, 0).wait_send()

    @pl.loop(near, groups)
    def _(step):
        tail_over(step, got_b, near).wait_send()

    @pl.loop(0, groups)
    def _(step):
        pass_over(step).wait_send()

    @pl.loop(1, groups)
    def _(step):
        give(step).wait_send()


def solution(mesh):
    groups = mesh.shape["expert"]
    row_spec = P(("data", "expert"), None)
    weight_spec = P("expert", None, None)

    def device_step(token_rows, expert_ids, gate_weights, w_in, w_out):
        tokens, top_k = expert_ids.shape
        local, dim, hidden = w_in.shape
        experts = local * groups
        mean_load = tokens * top_k // experts
        capacity = groups * mean_load
        segment = 7 * mean_load // 4
        worst = local * segment
        sizes = [local * mean_load * 18 // 16, local * mean_load * 19 // 16, worst]
        stride = 2 * local * mean_load
        lanes = groups * WIN
        near = groups // 2
        vmem = pl.BlockSpec(memory_space=VMEM)
        anywhere = pl.BlockSpec(memory_space=pl.ANY)

        def params(collective_id):
            return pltpu.CompilerParams(collective_id=collective_id, has_side_effects=True, vmem_limit_bytes=61 * 1024 * 1024)

        pair_sems = [pltpu.SemaphoreType.DMA((groups,)), pltpu.SemaphoreType.DMA((groups,))]
        pos, slot, start, place, rung = pl.pallas_call(
            functools.partial(route_kernel, groups, capacity, sizes, stride, local, near),
            out_shape=[
                jax.ShapeDtypeStruct((top_k, tokens), I32),
                jax.ShapeDtypeStruct((local, lanes), I32),
                jax.ShapeDtypeStruct((local, groups), I32),
                jax.ShapeDtypeStruct((2, local, capacity), I32),
                jax.ShapeDtypeStruct((1, 1), I32),
            ],
            in_specs=[vmem],
            out_specs=[vmem] * 5,
            scratch_shapes=[
                VMEM((groups, top_k, experts), F32),
                VMEM((top_k, experts, 128), F32),
                VMEM((top_k, tokens), F32),
                VMEM((4, groups, experts), F32),
            ]
            + pair_sems,
            compiler_params=params(0),
            name="route",
        )(expert_ids.T)

        def exchange(cap, collective_id):
            depth = 4 if cap == worst else 10

            def run():
                return pl.pallas_call(
                    functools.partial(moe_kernel, groups, cap, stride, local, near, segment),
                    out_shape=jax.ShapeDtypeStruct((tokens, dim), BF16),
                    in_specs=[pl.BlockSpec(memory_space=pltpu.SMEM)] + [vmem] * 4 + [anywhere] * 3,
                    out_specs=vmem,
                    scratch_shapes=[
                        VMEM((tokens, dim), BF16),
                        VMEM((groups, cap // ALIGN, ALIGN, dim), BF16),
                        VMEM(((near * (cap + TAIL) + WIN) // ALIGN, ALIGN, dim), BF16),
                        VMEM((((groups - near) * (cap + TAIL) + WIN) // ALIGN, ALIGN, dim), BF16),
                        VMEM((groups, cap + TAIL, dim), BF16),
                        VMEM((groups, TAIL, dim), BF16),
                        VMEM((groups, cap, dim), BF16),
                        VMEM((depth, dim, hidden), BF16),
                        VMEM((depth, hidden, dim), BF16),
                        VMEM((2, near * WIN, dim), BF16),
                        VMEM((4 * capacity, dim), BF16),
                        VMEM((top_k, tokens, 128), I32),
                        VMEM((top_k, tokens, 128), F32),
                        VMEM((top_k, tokens, dim), BF16),
                        pltpu.SemaphoreType.DMA((2, depth)),
                    ]
                    + pair_sems * 4
                    + [pltpu.SemaphoreType.DMA((3,))],
                    compiler_params=params(collective_id),
                    name="experts",
                )(start, slot, place, pos, gate_weights.T, token_rows, w_in, w_out)

            return run

        return lax.switch(rung.reshape(()), [exchange(cap, 1 + i) for i, cap in enumerate(sizes)])

    return jax.shard_map(device_step, mesh=mesh, in_specs=(row_spec, row_spec, row_spec, weight_spec, weight_spec), out_specs=row_spec, check_vma=False)
```
